16 devices in a mesh: kv: 2 (over y, z), dup: 8 (over x, core).
Axes of the slice: x: 4, y: 2, z: 1, core: 2. Of those that a mesh axis runs over, the one named last changes fastest.
The devices are a block of a 4x4x8 slice.
Arguments:
- queries: bfloat16 [512, 24, 128], P('kv', 'dup'), parts along dimension 0
- key_cache: bfloat16 [512, 4096, 128], P('kv', 'dup'), parts along dimension 0
- value_cache: bfloat16 [512, 4096, 128], P('kv', 'dup'), parts along dimension 0
- lengths: int32 [512], P('kv'), parts along dimension 0
Outputs:
- output: bfloat16 [512, 24, 128], P('kv', 'dup'), parts along dimension 0
There are 2 independent parts. The reference program is written for one: setup_inputs(seed, part) draws one part's arguments, and reference() takes and returns one part's arrays. A program takes and returns all parts, laid end to end along the dimension named above; each array names one.
All inputs are finite; a program needn't handle non-finite values.
Results may differ from the reference program's by a relative error of at most 0.00823596.
Values are sent between devices in bfloat16 or wider.
A program may use at most 768 MiB of HBM per device.

```python
import math
import jax
import jax.numpy as jnp
from jax import lax

BATCH = 256
SEQ = 4096
HEADS = 48
KV_HEADS = 8
HEAD_DIM = 128
DRAFT = 4

GROUP_HEADS = HEADS // KV_HEADS
QUERY_ROWS = GROUP_HEADS * DRAFT


def wave_field(k_freq, k_phase, k_dir, strength):
    spot_frac = jnp.arange(SEQ, dtype=jnp.float32) / SEQ
    freq_row = jax.random.randint(k_freq, (BATCH, 3), 1, 17, jnp.int32).astype(jnp.float32)
    phases = jax.random.uniform(k_phase, (BATCH, 3), jnp.float32) * (2.0 * math.pi)
    directions = jax.random.normal(k_dir, (BATCH, 3, HEAD_DIM), jnp.float32)
    wave_vals = jnp.cos(2.0 * math.pi * freq_row[:, None, :] * spot_frac[None, :, None] + phases[:, None, :])
    return strength * jnp.einsum("bsk,bkd->bsd", wave_vals, directions)


def setup_inputs(seed: int = 0, part: int = 0) -> dict:
    part_key = jax.random.fold_in(jax.random.key(seed), part)
    key_list = jax.random.split(part_key, 11)
    queries = jax.random.normal(key_list[0], (BATCH, QUERY_ROWS, HEAD_DIM), jnp.float32)
    k_noise = jax.random.normal(key_list[1], (BATCH, SEQ, HEAD_DIM), jnp.float32)
    key_cache = k_noise + wave_field(key_list[2], key_list[3], key_list[4], 1.5)
    v_noise = jax.random.normal(key_list[5], (BATCH, SEQ, HEAD_DIM), jnp.float32)
    value_cache = v_noise + wave_field(key_list[6], key_list[7], key_list[8], 1.0)
    low_len = max(DRAFT, SEQ // 8)
    lengths = jax.random.randint(key_list[9], (BATCH,), low_len, SEQ + 1, jnp.int32)
    full_row = jax.random.randint(key_list[10], (), 0, BATCH, jnp.int32)
    lengths = jnp.where(jnp.arange(BATCH) == full_row, SEQ, lengths).astype(jnp.int32)
    return {"queries": queries.astype(jnp.bfloat16), "key_cache": key_cache.astype(jnp.bfloat16), "value_cache": value_cache.astype(jnp.bfloat16), "lengths": lengths}


def reference(queries, key_cache, value_cache, lengths):
    score_scale = 1.0 / math.sqrt(HEAD_DIM)
    draft_pos = jnp.arange(QUERY_ROWS) % DRAFT
    seq_pos = jnp.arange(SEQ)

    def one_sequence(operands):
        q_rows, k_rows, v_rows, length = operands
        scores = jnp.dot(q_rows, k_rows.T, preferred_element_type=jnp.float32) * score_scale
        last_pos = length - DRAFT + draft_pos
        allowed = seq_pos[None, :] <= last_pos[:, None]
        scores = jnp.where(allowed, scores, -jnp.inf)
        row_peak = jnp.max(scores, axis=1, keepdims=True)
        prob_vals = jnp.exp(scores - row_peak)
        row_mass = jnp.sum(prob_vals, axis=1, keepdims=True)
        weighted = jnp.dot(prob_vals.astype(jnp.bfloat16), v_rows, preferred_element_type=jnp.float32)
        return (weighted / row_mass).astype(jnp.bfloat16)

    return lax.map(one_sequence, (queries, key_cache, value_cache, lengths))
```

```python
import functools

import jax
import jax.numpy as jnp
from jax import lax
from jax.experimental import pallas as pl
from jax.experimental.pallas import tpu as pltpu
from jax.sharding import PartitionSpec as P

DRAFT = 4
NEG_BIG = -3e38
LOG2E = 1.4426950408889634
MESH = pl.DeviceIdType.MESH

CHUNK = 32
GROUP = 8
SLOTS = 20
PITCH = CHUNK + 4


def attend(q_ref, len_ref, k_hbm, v_hbm, o_ref,
           kbuf, vbuf, q_all, q_wide, pos_rel, part_o, part_l,
           pair_so, pair_sl, pair_ro, pair_rl,
           chip_so, chip_sl, chip_ro, chip_rl, keep_o, keep_l,
           k_sem, v_sem, qs_sem, qr_sem, ps_sem, pr_sem, cs_sem, cr_sem):
    own, num_batch, head_dim = q_ref.shape
    span = k_hbm.shape[1]
    rows = 8 * own
    half = 4 * own
    chunks = num_batch // CHUNK
    groups = num_batch // GROUP
    scale = (head_dim ** -0.5) * LOG2E

    me = lax.axis_index("dup")
    chip = me // 2
    core = me % 2
    turn = 1 - 2 * core
    partner = chip * 2 + (1 - core)
    ahead = ((chip + turn + 4) % 4) * 2 + core
    behind = ((chip - turn + 4) % 4) * 2 + core
    across = ((chip + 2) % 4) * 2 + core

    def cache_copies(group):
        slot = group % SLOTS
        part = pl.ds(group * GROUP, GROUP)
        return (pltpu.make_async_copy(k_hbm.at[part], kbuf.at[slot], k_sem.at[slot]),
                pltpu.make_async_copy(v_hbm.at[part], vbuf.at[slot], v_sem.at[slot]))

    def start_cache(group, carry=0):
        for copy in cache_copies(group):
            copy.start()
        return carry

    lax.fori_loop(0, min(SLOTS, groups), start_cache, 0)

    barrier = pltpu.get_barrier_semaphore()
    for peer in (partner, ahead, behind, across):
        pl.semaphore_signal(barrier, inc=1, device_id={"dup": peer}, device_id_type=MESH)

    def q_copy(kind, c):
        part = pl.ds(pl.multiple_of(c * CHUNK, CHUNK), CHUNK)
        src, dst, peer = (
            (q_ref.at[:, part], q_all.at[2, :, part], behind),
            (q_ref.at[:, part], q_all.at[1, :, part], ahead),
            (q_ref.at[:, part], q_all.at[4, :, part], partner),
            (q_all.at[1, :, part], q_all.at[3, :, part], ahead),
            (q_all.at[1, :, part], q_all.at[5, :, part], partner),
            (q_all.at[2, :, part], q_all.at[6, :, part], partner),
            (q_all.at[3, :, part], q_all.at[7, :, part], partner),
        )[kind]
        return pltpu.make_async_remote_copy(
            src_ref=src, dst_ref=dst, send_sem=qs_sem.at[kind, c], recv_sem=qr_sem.at[kind, c],
            device_id={"dup": peer}, device_id_type=MESH)

    def q_own(c):
        for kind in (0, 1, 2):
            q_copy(kind, c).start()

    def q_pass_near(c):
        q_copy(1, c).wait_recv()
        q_copy(3, c).start()
        q_copy(4, c).start()
        q_copy(0, c).wait_recv()
        q_copy(5, c).start()

    def q_pass_far(c):
        q_copy(3, c).wait_recv()
        q_copy(6, c).start()

    span_start = me * span
    chip_disp = (0, 4 - turn, 4 + turn, 2)
    pair_disp = (0, 4 + turn, 4 - turn, 2)
    row_id = lax.broadcasted_iota(jnp.int32, (rows, span), 0)
    token = jnp.zeros((rows, span), jnp.int32)
    for h in range(2):
        for s in range(4):
            disp = (chip_disp, pair_disp)[h][s]
            device = ((chip + disp) % 4) * 2 + (core if h == 0 else 1 - core)
            for i in range(own):
                token = jnp.where(row_id == h * half + s * own + i, (own * device + i) % DRAFT, token)
    pos_rel[...] = lax.broadcasted_iota(jnp.int32, (rows, span), 1) + span_start - token

    pl.semaphore_wait(barrier, 4)
    q_own(0)
    q_own(1)
    q_pass_near(0)
    q_pass_far(0)

    def widen_queries(c):
        part = pl.ds(pl.multiple_of(c * CHUNK, CHUNK), CHUNK)
        for kind in (2, 4, 5, 6):
            q_copy(kind, c).wait_recv()
        for s in range(8):
            for i in range(own):
                block = q_ref[i, part, :] if s == 0 else q_all[s, i, part, :]
                q_wide[pl.ds((s * own + i) * PITCH, CHUNK), :] = block.astype(jnp.float32)

    def attend_pair(c, slot, first, j):
        zeros = jnp.zeros((rows, head_dim), jnp.float32)
        q0 = q_wide[pl.ds(first + j, rows, stride=PITCH), :]
        q1 = q_wide[pl.ds(first + j + 1, rows, stride=PITCH), :]
        q2 = jnp.concatenate([jnp.concatenate([q0, zeros], 1), jnp.concatenate([zeros, q1], 1)], 0).astype(jnp.bfloat16)
        k2 = jnp.concatenate([kbuf[slot, j], kbuf[slot, j + 1]], 1)
        s = lax.dot_general(q2, k2, (((1,), (1,)), ((), ())), preferred_element_type=jnp.float32)
        rel = pos_rel[...]
        base = c * CHUNK + first + j
        s = jnp.concatenate([
            jnp.where(rel <= len_ref[base] - DRAFT, s[:rows], NEG_BIG),
            jnp.where(rel <= len_ref[base + 1] - DRAFT, s[rows:], NEG_BIG)], 0)
        peak = jnp.max(s, axis=1, keepdims=True)
        p = jnp.exp2((s - peak) * scale)
        mass = jnp.sum(p, axis=1, keepdims=True)
        v2 = jnp.concatenate([vbuf[slot, j], vbuf[slot, j + 1]], 1)
        o2 = jnp.dot(p.astype(jnp.bfloat16), v2, preferred_element_type=jnp.float32)
        inv = 1.0 / mass
        log_mass = jnp.broadcast_to(peak * scale + jnp.log2(mass), (2 * rows, head_dim))
        par = c % 2
        for n in range(2):
            o = o2[n * rows:(n + 1) * rows, n * head_dim:(n + 1) * head_dim] * inv[n * rows:(n + 1) * rows]
            at = pl.ds(first + j + n, rows, stride=PITCH)
            part_o.at[par][at, :] = o
            part_l.at[par][at, :] = log_mass[n * rows:(n + 1) * rows]

    lane = lax.broadcasted_iota(jnp.int32, (CHUNK, head_dim), 1)
    seq = lax.broadcasted_iota(jnp.int32, (CHUNK, head_dim), 0)

    def to_lanes(values):
        total = jnp.zeros((CHUNK, head_dim), jnp.float32)
        for i, value in enumerate(values):
            total = jnp.where(lane == seq + i * CHUNK, value, total)
        return jnp.sum(total, axis=0, keepdims=True)

    def from_lanes(line, i):
        return jnp.sum(jnp.where(lane == seq + i * CHUNK, line, 0.0), axis=1, keepdims=True)

    def pair_copies(c):
        return tuple(pltpu.make_async_remote_copy(
            src_ref=src.at[c], dst_ref=dst.at[c], send_sem=ps_sem.at[n, c], recv_sem=pr_sem.at[n, c],
            device_id={"dup": partner}, device_id_type=MESH) for n, (src, dst) in enumerate(((pair_so, pair_ro), (pair_sl, pair_rl))))

    def chip_copies(c):
        copies = []
        for s, (there, peer) in enumerate(((1, behind), (0, ahead), (2, across))):
            for n, (src, dst) in enumerate(((chip_so, chip_ro), (chip_sl, chip_rl))):
                copies.append(pltpu.make_async_remote_copy(
                    src_ref=src.at[c, s], dst_ref=dst.at[c, there],
                    send_sem=cs_sem.at[n, s, c], recv_sem=cr_sem.at[n, there, c],
                    device_id={"dup": peer}, device_id_type=MESH))
        return copies

    def chip_arrivals(c):
        return [pltpu.make_async_remote_copy(
            src_ref=(chip_so, chip_sl)[n].at[c, s], dst_ref=(chip_ro, chip_rl)[n].at[c, s],
            send_sem=cs_sem.at[n, s, c], recv_sem=cr_sem.at[n, s, c],
            device_id={"dup": partner}, device_id_type=MESH) for s in range(3) for n in range(2)]

    def slab(ref, par, row):
        return ref.at[par][pl.ds(row * PITCH, CHUNK), :]

    def give_partner(c):
        par = c % 2
        for s in range(4):
            for i in range(own):
                pair_so[c, s, i * CHUNK:(i + 1) * CHUNK, :] = slab(part_o, par, half + s * own + i).astype(jnp.bfloat16)
        for s in range(4):
            pair_sl[c, s] = to_lanes([slab(part_l, par, half + s * own + i) for i in range(own)])
        for copy in pair_copies(c):
            copy.start()

    def merge_chip(c):
        par = c % 2
        for copy in pair_copies(c):
            copy.wait_recv()
        for s in (3, 1, 2, 0):
            logs = []
            line = pair_rl[c, s]
            for i in range(own):
                mine = slab(part_l, par, s * own + i)
                theirs = from_lanes(line, i)
                top = jnp.maximum(mine, theirs)
                w_mine, w_theirs = jnp.exp2(mine - top), jnp.exp2(theirs - top)
                total = w_mine + w_theirs
                o = (w_mine * slab(part_o, par, s * own + i)
                     + w_theirs * pair_ro[c, s, i * CHUNK:(i + 1) * CHUNK, :].astype(jnp.float32)) / total
                log_total = top + jnp.log2(total)
                if s == 0:
                    keep_o[par, i] = o
                    keep_l[par, i] = log_total
                else:
                    chip_so[c, s - 1, i * CHUNK:(i + 1) * CHUNK, :] = o.astype(jnp.bfloat16)
                    logs.append(log_total)
            if s:
                chip_sl[c, s - 1] = to_lanes(logs)
        for copy in chip_copies(c):
            copy.start()

    def merge_group(c):
        par = c % 2
        for copy in chip_arrivals(c):
            copy.wait_recv()
        lines = [chip_rl[c, s] for s in range(3)]
        for i in range(own):
            logs = [keep_l[par, i]] + [from_lanes(line, i) for line in lines]
            top = functools.reduce(jnp.maximum, logs)
            weights = [jnp.exp2(log - top) for log in logs]
            total = functools.reduce(jnp.add, weights)
            merged = weights[0] * keep_o[par, i]
            for s in range(3):
                merged = merged + weights[s + 1] * chip_ro[c, s, i * CHUNK:(i + 1) * CHUNK, :].astype(jnp.float32)
            o_ref[i, pl.ds(pl.multiple_of(c * CHUNK, CHUNK), CHUNK), :] = (merged / total).astype(jnp.bfloat16)

    def chunk_step(c, carry):
        @pl.when(c + 2 < chunks)
        def _():
            q_own(c + 2)

        @pl.when(c + 1 < chunks)
        def _():
            q_pass_near(c + 1)

        widen_queries(c)

        def group_step(g, inner):
            group = c * (CHUNK // GROUP) + g
            slot = group % SLOTS
            for copy in cache_copies(group):
                copy.wait()
            for j in range(0, GROUP, 2):
                attend_pair(c, slot, g * GROUP, j)

            @pl.when(group + SLOTS < groups)
            def _():
                start_cache(group + SLOTS)
            return inner

        lax.fori_loop(0, CHUNK // GROUP, group_step, 0)

        @pl.when(c + 1 < chunks)
        def _():
            q_pass_far(c + 1)

        give_partner(c)

        @pl.when(c >= 2)
        def _():
            merge_group(c - 2)

        @pl.when(c >= 1)
        def _():
            merge_chip(c - 1)
        return carry

    lax.fori_loop(0, chunks, chunk_step, 0)
    merge_group(chunks - 2)
    merge_chip(chunks - 1)
    merge_group(chunks - 1)

    def drain(c, carry):
        for kind in range(7):
            q_copy(kind, c).wait_send()
        for copy in pair_copies(c) + tuple(chip_copies(c)):
            copy.wait_send()
        return carry

    lax.fori_loop(0, chunks, drain, 0)


def solution(mesh):
    def group_step(q_local, k_span, v_span, len_local):
        num_batch, own, head_dim = q_local.shape
        span = k_span.shape[1]
        chunks = num_batch // CHUNK
        rows = 8 * own
        vmem = functools.partial(pl.BlockSpec, memory_space=pltpu.VMEM)
        hbm = functools.partial(pl.BlockSpec, memory_space=pl.ANY)
        bf16, f32 = jnp.bfloat16, jnp.float32
        dma = pltpu.SemaphoreType.DMA
        out = pl.pallas_call(
            attend,
            out_shape=jax.ShapeDtypeStruct((own, num_batch, head_dim), bf16),
            in_specs=[vmem(), pl.BlockSpec(memory_space=pltpu.SMEM), hbm(), hbm()],
            out_specs=vmem(),
            scratch_shapes=[
                pltpu.VMEM((SLOTS, GROUP, span, head_dim), bf16),
                pltpu.VMEM((SLOTS, GROUP, span, head_dim), bf16),
                pltpu.VMEM((8, own, num_batch, head_dim), bf16),
                pltpu.VMEM((rows * PITCH, head_dim), f32),
                pltpu.VMEM((rows, span), jnp.int32),
                pltpu.VMEM((2, rows * PITCH, head_dim), f32),
                pltpu.VMEM((2, rows * PITCH, head_dim), f32),
                pltpu.VMEM((chunks, 4, own * CHUNK, head_dim), bf16),
                pltpu.VMEM((chunks, 4, 1, head_dim), f32),
                pltpu.VMEM((chunks, 4, own * CHUNK, head_dim), bf16),
                pltpu.VMEM((chunks, 4, 1, head_dim), f32),
                pltpu.VMEM((chunks, 3, own * CHUNK, head_dim), bf16),
                pltpu.VMEM((chunks, 3, 1, head_dim), f32),
                pltpu.VMEM((chunks, 3, own * CHUNK, head_dim), bf16),
                pltpu.VMEM((chunks, 3, 1, head_dim), f32),
                pltpu.VMEM((2, own, CHUNK, head_dim), f32),
                pltpu.VMEM((2, own, CHUNK, head_dim), f32),
                dma((SLOTS,)), dma((SLOTS,)),
                dma((7, chunks)), dma((7, chunks)),
                dma((2, chunks)), dma((2, chunks)),
                dma((2, 3, chunks)), dma((2, 3, chunks)),
            ],
            compiler_params=pltpu.CompilerParams(
                collective_id=0, has_side_effects=True, vmem_limit_bytes=60 * 1024 * 1024),
            cost_estimate=pl.CostEstimate(
                flops=4 * num_batch * rows * span * head_dim,
                bytes_accessed=4 * num_batch * span * head_dim,
                transcendentals=num_batch * rows * span),
        )(q_local.transpose(1, 0, 2), len_local, k_span, v_span)
        return out.transpose(1, 0, 2)

    return jax.shard_map(
        group_step, mesh=mesh,
        in_specs=(P("kv", "dup", None), P("kv", "dup", None), P("kv", "dup", None), P("kv")),
        out_specs=P("kv", "dup", None), check_vma=False)
```

```python
import functools

import jax
import jax.numpy as jnp
from jax import lax
from jax.experimental import pallas as pl
from jax.experimental.pallas import tpu as pltpu
from jax.sharding import PartitionSpec as P

DRAFT = 4
NEG_BIG = -3e38
LOG2E = 1.4426950408889634
MESH = pl.DeviceIdType.MESH

CHUNK = 64
GROUP = 8
SLOTS = 20
PITCH = CHUNK + 4


def attend(q_ref, len_ref, k_hbm, v_hbm, o_ref,
           kbuf, vbuf, q_all, q_wide, pos_rel, part_o, part_l,
           pair_so, pair_sl, pair_ro, pair_rl,
           chip_so, chip_sl, chip_ro, chip_rl, keep_o, keep_l,
           k_sem, v_sem, qs_sem, qr_sem, ps_sem, pr_sem, cs_sem, cr_sem):
    own, num_batch, head_dim = q_ref.shape
    span = k_hbm.shape[1]
    rows = 8 * own
    half = 4 * own
    chunks = num_batch // CHUNK
    groups = num_batch // GROUP
    scale = (head_dim ** -0.5) * LOG2E

    me = lax.axis_index("dup")
    chip = me // 2
    core = me % 2
    turn = 1 - 2 * core
    partner = chip * 2 + (1 - core)
    ahead = ((chip + turn + 4) % 4) * 2 + core
    behind = ((chip - turn + 4) % 4) * 2 + core
    across = ((chip + 2) % 4) * 2 + core

    def cache_copies(group):
        slot = group % SLOTS
        part = pl.ds(group * GROUP, GROUP)
        return (pltpu.make_async_copy(k_hbm.at[part], kbuf.at[slot], k_sem.at[slot]),
                pltpu.make_async_copy(v_hbm.at[part], vbuf.at[slot], v_sem.at[slot]))

    def start_cache(group, carry=0):
        for copy in cache_copies(group):
            copy.start()
        return carry

    lax.fori_loop(0, min(SLOTS, groups), start_cache, 0)

    barrier = pltpu.get_barrier_semaphore()
    for peer in (partner, ahead, behind, across):
        pl.semaphore_signal(barrier, inc=1, device_id={"dup": peer}, device_id_type=MESH)

    def q_copy(kind, c):
        part = pl.ds(pl.multiple_of(c * CHUNK, CHUNK), CHUNK)
        src, dst, peer = (
            (q_ref.at[:, part], q_all.at[2, :, part], behind),
            (q_ref.at[:, part], q_all.at[1, :, part], ahead),
            (q_ref.at[:, part], q_all.at[4, :, part], partner),
            (q_all.at[1, :, part], q_all.at[3, :, part], ahead),
            (q_all.at[1, :, part], q_all.at[5, :, part], partner),
            (q_all.at[2, :, part], q_all.at[6, :, part], partner),
            (q_all.at[3, :, part], q_all.at[7, :, part], partner),
        )[kind]
        return pltpu.make_async_remote_copy(
            src_ref=src, dst_ref=dst, send_sem=qs_sem.at[kind, c], recv_sem=qr_sem.at[kind, c],
            device_id={"dup": peer}, device_id_type=MESH)

    def q_own(c):
        for kind in (0, 1, 2):
            q_copy(kind, c).start()

    def q_pass_near(c):
        q_copy(1, c).wait_recv()
        q_copy(3, c).start()
        q_copy(4, c).start()
        q_copy(0, c).wait_recv()
        q_copy(5, c).start()

    def q_pass_far(c):
        q_copy(3, c).wait_recv()
        q_copy(6, c).start()

    span_start = me * span
    chip_disp = (0, 4 - turn, 4 + turn, 2)
    pair_disp = (0, 4 + turn, 4 - turn, 2)
    row_id = lax.broadcasted_iota(jnp.int32, (rows, span), 0)
    token = jnp.zeros((rows, span), jnp.int32)
    for h in range(2):
        for s in range(4):
            disp = (chip_disp, pair_disp)[h][s]
            device = ((chip + disp) % 4) * 2 + (core if h == 0 else 1 - core)
            for i in range(own):
                token = jnp.where(row_id == h * half + s * own + i, (own * device + i) % DRAFT, token)
    pos_rel[...] = lax.broadcasted_iota(jnp.int32, (rows, span), 1) + span_start - token

    pl.semaphore_wait(barrier, 4)
    q_own(0)
    q_own(1)
    q_pass_near(0)
    q_pass_far(0)

    def widen_queries(c):
        part = pl.ds(pl.multiple_of(c * CHUNK, CHUNK), CHUNK)
        for kind in (2, 4, 5, 6):
            q_copy(kind, c).wait_recv()
        for s in range(8):
            for i in range(own):
                block = q_ref[i, part, :] if s == 0 else q_all[s, i, part, :]
                q_wide[pl.ds((s * own + i) * PITCH, CHUNK), :] = block.astype(jnp.float32)

    def attend_pair(c, slot, first, j):
        zeros = jnp.zeros((rows, head_dim), jnp.float32)
        q0 = q_wide[pl.ds(first + j, rows, stride=PITCH), :]
        q1 = q_wide[pl.ds(first + j + 1, rows, stride=PITCH), :]
        q2 = jnp.concatenate([jnp.concatenate([q0, zeros], 1), jnp.concatenate([zeros, q1], 1)], 0).astype(jnp.bfloat16)
        k2 = jnp.concatenate([kbuf[slot, j], kbuf[slot, j + 1]], 1)
        s = lax.dot_general(q2, k2, (((1,), (1,)), ((), ())), preferred_element_type=jnp.float32)
        rel = pos_rel[...]
        base = c * CHUNK + first + j
        s = jnp.concatenate([
            jnp.where(rel <= len_ref[base] - DRAFT, s[:rows], NEG_BIG),
            jnp.where(rel <= len_ref[base + 1] - DRAFT, s[rows:], NEG_BIG)], 0)
        peak = jnp.max(s, axis=1, keepdims=True)
        p = jnp.exp2((s - peak) * scale)
        mass = jnp.sum(p, axis=1, keepdims=True)
        v2 = jnp.concatenate([vbuf[slot, j], vbuf[slot, j + 1]], 1)
        o2 = jnp.dot(p.astype(jnp.bfloat16), v2, preferred_element_type=jnp.float32)
        inv = 1.0 / mass
        log_mass = jnp.broadcast_to(peak * scale + jnp.log2(mass), (2 * rows, head_dim))
        par = c % 2
        for n in range(2):
            o = o2[n * rows:(n + 1) * rows, n * head_dim:(n + 1) * head_dim] * inv[n * rows:(n + 1) * rows]
            at = pl.ds(first + j + n, rows, stride=PITCH)
            part_o.at[par][at, :] = o
            part_l.at[par][at, :] = log_mass[n * rows:(n + 1) * rows]

    lane = lax.broadcasted_iota(jnp.int32, (CHUNK, head_dim), 1)
    seq = lax.broadcasted_iota(jnp.int32, (CHUNK, head_dim), 0)

    def to_lanes(value):
        return jnp.sum(jnp.where(lane == seq, value, 0.0), axis=0, keepdims=True)

    def from_lanes(line):
        return jnp.sum(jnp.where(lane == seq, line, 0.0), axis=1, keepdims=True)

    def pair_copies(c):
        return tuple(pltpu.make_async_remote_copy(
            src_ref=src.at[c], dst_ref=dst.at[c], send_sem=ps_sem.at[n, c], recv_sem=pr_sem.at[n, c],
            device_id={"dup": partner}, device_id_type=MESH) for n, (src, dst) in enumerate(((pair_so, pair_ro), (pair_sl, pair_rl))))

    def chip_copies(c):
        copies = []
        for s, (there, peer) in enumerate(((1, behind), (0, ahead), (2, across))):
            for n, (src, dst) in enumerate(((chip_so, chip_ro), (chip_sl, chip_rl))):
                copies.append(pltpu.make_async_remote_copy(
                    src_ref=src.at[c, s], dst_ref=dst.at[c, there],
                    send_sem=cs_sem.at[n, s, c], recv_sem=cr_sem.at[n, there, c],
                    device_id={"dup": peer}, device_id_type=MESH))
        return copies

    def chip_arrivals(c):
        return [pltpu.make_async_remote_copy(
            src_ref=(chip_so, chip_sl)[n].at[c, s], dst_ref=(chip_ro, chip_rl)[n].at[c, s],
            send_sem=cs_sem.at[n, s, c], recv_sem=cr_sem.at[n, s, c],
            device_id={"dup": partner}, device_id_type=MESH) for s in range(3) for n in range(2)]

    def slab(ref, par, row):
        return ref.at[par][pl.ds(row * PITCH, CHUNK), :]

    def give_partner(c):
        par = c % 2
        for s in range(4):
            for i in range(own):
                pair_so[c, s, i * CHUNK:(i + 1) * CHUNK, :] = slab(part_o, par, half + s * own + i).astype(jnp.bfloat16)
        for s in range(4):
            for i in range(own):
                pair_sl[c, s, i:i + 1, :] = to_lanes(slab(part_l, par, half + s * own + i))
        for copy in pair_copies(c):
            copy.start()

    def merge_chip(c):
        par = c % 2
        for copy in pair_copies(c):
            copy.wait_recv()
        for s in (3, 1, 2, 0):
            for i in range(own):
                mine = slab(part_l, par, s * own + i)
                theirs = from_lanes(pair_rl[c, s, i:i + 1, :])
                top = jnp.maximum(mine, theirs)
                w_mine, w_theirs = jnp.exp2(mine - top), jnp.exp2(theirs - top)
                total = w_mine + w_theirs
                o = (w_mine * slab(part_o, par, s * own + i)
                     + w_theirs * pair_ro[c, s, i * CHUNK:(i + 1) * CHUNK, :].astype(jnp.float32)) / total
                log_total = top + jnp.log2(total)
                if s == 0:
                    keep_o[par, i] = o
                    keep_l[par, i] = log_total
                else:
                    chip_so[c, s - 1, i * CHUNK:(i + 1) * CHUNK, :] = o.astype(jnp.bfloat16)
                    chip_sl[c, s - 1, i:i + 1, :] = to_lanes(log_total)
        for copy in chip_copies(c):
            copy.start()

    def merge_group(c):
        par = c % 2
        for copy in chip_arrivals(c):
            copy.wait_recv()
        for i in range(own):
            logs = [keep_l[par, i]] + [from_lanes(chip_rl[c, s, i:i + 1, :]) for s in range(3)]
            top = functools.reduce(jnp.maximum, logs)
            weights = [jnp.exp2(log - top) for log in logs]
            total = functools.reduce(jnp.add, weights)
            merged = weights[0] * keep_o[par, i]
            for s in range(3):
                merged = merged + weights[s + 1] * chip_ro[c, s, i * CHUNK:(i + 1) * CHUNK, :].astype(jnp.float32)
            o_ref[i, pl.ds(pl.multiple_of(c * CHUNK, CHUNK), CHUNK), :] = (merged / total).astype(jnp.bfloat16)

    def chunk_step(c, carry):
        @pl.when(c + 2 < chunks)
        def _():
            q_own(c + 2)

        @pl.when(c + 1 < chunks)
        def _():
            q_pass_near(c + 1)

        widen_queries(c)

        def group_step(g, inner):
            group = c * (CHUNK // GROUP) + g
            slot = group % SLOTS
            for copy in cache_copies(group):
                copy.wait()
            for j in range(0, GROUP, 2):
                attend_pair(c, slot, g * GROUP, j)

            @pl.when(group + SLOTS < groups)
            def _():
                start_cache(group + SLOTS)
            return inner

        lax.fori_loop(0, CHUNK // GROUP, group_step, 0)

        @pl.when(c + 1 < chunks)
        def _():
            q_pass_far(c + 1)

        give_partner(c)

        @pl.when(c >= 2)
        def _():
            merge_group(c - 2)

        @pl.when(c >= 1)
        def _():
            merge_chip(c - 1)
        return carry

    lax.fori_loop(0, chunks, chunk_step, 0)
    merge_group(chunks - 2)
    merge_chip(chunks - 1)
    merge_group(chunks - 1)

    def drain(c, carry):
        for kind in range(7):
            q_copy(kind, c).wait_send()
        for copy in pair_copies(c) + tuple(chip_copies(c)):
            copy.wait_send()
        return carry

    lax.fori_loop(0, chunks, drain, 0)


def solution(mesh):
    def group_step(q_local, k_span, v_span, len_local):
        num_batch, own, head_dim = q_local.shape
        span = k_span.shape[1]
        chunks = num_batch // CHUNK
        rows = 8 * own
        vmem = functools.partial(pl.BlockSpec, memory_space=pltpu.VMEM)
        hbm = functools.partial(pl.BlockSpec, memory_space=pl.ANY)
        bf16, f32 = jnp.bfloat16, jnp.float32
        dma = pltpu.SemaphoreType.DMA
        out = pl.pallas_call(
            attend,
            out_shape=jax.ShapeDtypeStruct((own, num_batch, head_dim), bf16),
            in_specs=[vmem(), pl.BlockSpec(memory_space=pltpu.SMEM), hbm(), hbm()],
            out_specs=vmem(),
            scratch_shapes=[
                pltpu.VMEM((SLOTS, GROUP, span, head_dim), bf16),
                pltpu.VMEM((SLOTS, GROUP, span, head_dim), bf16),
                pltpu.VMEM((8, own, num_batch, head_dim), bf16),
                pltpu.VMEM((rows * PITCH, head_dim), f32),
                pltpu.VMEM((rows, span), jnp.int32),
                pltpu.VMEM((2, rows * PITCH, head_dim), f32),
                pltpu.VMEM((2, rows * PITCH, head_dim), f32),
                pltpu.VMEM((chunks, 4, own * CHUNK, head_dim), bf16),
                pltpu.VMEM((chunks, 4, own, head_dim), f32),
                pltpu.VMEM((chunks, 4, own * CHUNK, head_dim), bf16),
                pltpu.VMEM((chunks, 4, own, head_dim), f32),
                pltpu.VMEM((chunks, 3, own * CHUNK, head_dim), bf16),
                pltpu.VMEM((chunks, 3, own, head_dim), f32),
                pltpu.VMEM((chunks, 3, own * CHUNK, head_dim), bf16),
                pltpu.VMEM((chunks, 3, own, head_dim), f32),
                pltpu.VMEM((2, own, CHUNK, head_dim), f32),
                pltpu.VMEM((2, own, CHUNK, head_dim), f32),
                dma((SLOTS,)), dma((SLOTS,)),
                dma((7, chunks)), dma((7, chunks)),
                dma((2, chunks)), dma((2, chunks)),
                dma((2, 3, chunks)), dma((2, 3, chunks)),
            ],
            compiler_params=pltpu.CompilerParams(
                collective_id=0, has_side_effects=True, vmem_limit_bytes=60 * 1024 * 1024),
            cost_estimate=pl.CostEstimate(
                flops=4 * num_batch * rows * span * head_dim,
                bytes_accessed=4 * num_batch * span * head_dim,
                transcendentals=num_batch * rows * span),
        )(q_local.transpose(1, 0, 2), len_local, k_span, v_span)
        return out.transpose(1, 0, 2)

    return jax.shard_map(
        group_step, mesh=mesh,
        in_specs=(P("kv", "dup", None), P("kv", "dup", None), P("kv", "dup", None), P("kv")),
        out_specs=P("kv", "dup", None), check_vma=False)
```

```python
import functools

import jax
import jax.numpy as jnp
from jax import lax
from jax.experimental import pallas as pl
from jax.experimental.pallas import tpu as pltpu
from jax.sharding import PartitionSpec as P

DRAFT = 4
NEG_BIG = -3e38
LOG2E = 1.4426950408889634
MESH = pl.DeviceIdType.MESH

CHUNK = 64
GROUP = 8
SLOTS = 20
TIMES = (1, 1, 1)
PITCH = CHUNK + 4


def attend(q_ref, len_ref, k_hbm, v_hbm, o_ref,
           kbuf, vbuf, q_all, q_wide, pos_rel, part_o, part_l,
           pair_so, pair_sl, pair_ro, pair_rl,
           chip_so, chip_sl, chip_ro, chip_rl, keep_o, keep_l,
           k_sem, v_sem, qs_sem, qr_sem, ps_sem, pr_sem, cs_sem, cr_sem, s_buf, p_buf, i_buf):
    own, num_batch, head_dim = q_ref.shape
    span = k_hbm.shape[1]
    rows = 8 * own
    half = 4 * own
    chunks = num_batch // CHUNK
    groups = num_batch // GROUP
    scale = (head_dim ** -0.5) * LOG2E

    me = lax.axis_index("dup")
    chip = me // 2
    core = me % 2
    turn = 1 - 2 * core
    partner = chip * 2 + (1 - core)
    ahead = ((chip + turn + 4) % 4) * 2 + core
    behind = ((chip - turn + 4) % 4) * 2 + core
    across = ((chip + 2) % 4) * 2 + core

    def cache_copies(group):
        slot = group % SLOTS
        part = pl.ds(group * GROUP, GROUP)
        return (pltpu.make_async_copy(k_hbm.at[part], kbuf.at[slot], k_sem.at[slot]),
                pltpu.make_async_copy(v_hbm.at[part], vbuf.at[slot], v_sem.at[slot]))

    def start_cache(group, carry=0):
        for copy in cache_copies(group):
            copy.start()
        return carry

    lax.fori_loop(0, min(SLOTS, groups), start_cache, 0)

    barrier = pltpu.get_barrier_semaphore()
    for peer in (partner, ahead, behind, across):
        pl.semaphore_signal(barrier, inc=1, device_id={"dup": peer}, device_id_type=MESH)

    def q_copy(kind, c):
        part = pl.ds(pl.multiple_of(c * CHUNK, CHUNK), CHUNK)
        src, dst, peer = (
            (q_ref.at[:, part], q_all.at[2, :, part], behind),
            (q_ref.at[:, part], q_all.at[1, :, part], ahead),
            (q_ref.at[:, part], q_all.at[4, :, part], partner),
            (q_all.at[1, :, part], q_all.at[3, :, part], ahead),
            (q_all.at[1, :, part], q_all.at[5, :, part], partner),
            (q_all.at[2, :, part], q_all.at[6, :, part], partner),
            (q_all.at[3, :, part], q_all.at[7, :, part], partner),
        )[kind]
        return pltpu.make_async_remote_copy(
            src_ref=src, dst_ref=dst, send_sem=qs_sem.at[kind, c], recv_sem=qr_sem.at[kind, c],
            device_id={"dup": peer}, device_id_type=MESH)

    def q_own(c):
        for kind in (0, 1, 2):
            q_copy(kind, c).start()

    def q_pass_near(c):
        q_copy(1, c).wait_recv()
        q_copy(3, c).start()
        q_copy(4, c).start()
        q_copy(0, c).wait_recv()
        q_copy(5, c).start()

    def q_pass_far(c):
        q_copy(3, c).wait_recv()
        q_copy(6, c).start()

    span_start = me * span
    chip_disp = (0, 4 - turn, 4 + turn, 2)
    pair_disp = (0, 4 + turn, 4 - turn, 2)
    row_id = lax.broadcasted_iota(jnp.int32, (rows, span), 0)
    token = jnp.zeros((rows, span), jnp.int32)
    for h in range(2):
        for s in range(4):
            disp = (chip_disp, pair_disp)[h][s]
            device = ((chip + disp) % 4) * 2 + (core if h == 0 else 1 - core)
            for i in range(own):
                token = jnp.where(row_id == h * half + s * own + i, (own * device + i) % DRAFT, token)
    pos_rel[...] = lax.broadcasted_iota(jnp.int32, (rows, span), 1) + span_start - token

    pl.semaphore_wait(barrier, 4)
    q_own(0)
    q_own(1)
    q_pass_near(0)
    q_pass_far(0)

    def widen_queries(c):
        part = pl.ds(pl.multiple_of(c * CHUNK, CHUNK), CHUNK)
        for kind in (2, 4, 5, 6):
            q_copy(kind, c).wait_recv()
        for s in range(8):
            for i in range(own):
                block = q_ref[i, part, :] if s == 0 else q_all[s, i, part, :]
                q_wide[pl.ds((s * own + i) * PITCH, CHUNK), :] = block.astype(jnp.float32)

    def score_pair(c, slot, first, j):
        zeros = jnp.zeros((rows, head_dim), jnp.float32)
        q0 = q_wide[pl.ds(first + j, rows, stride=PITCH), :]
        q1 = q_wide[pl.ds(first + j + 1, rows, stride=PITCH), :]
        q2 = jnp.concatenate([jnp.concatenate([q0, zeros], 1), jnp.concatenate([zeros, q1], 1)], 0).astype(jnp.bfloat16)
        k2 = jnp.concatenate([kbuf[slot, j], kbuf[slot, j + 1]], 1)
        s_buf[j // 2] = lax.dot_general(q2, k2, (((1,), (1,)), ((), ())), preferred_element_type=jnp.float32)

    def soft_pair(c, slot, first, j):
        s = s_buf[j // 2]
        rel = pos_rel[...]
        base = c * CHUNK + first + j
        s = jnp.concatenate([
            jnp.where(rel <= len_ref[base] - DRAFT, s[:rows], NEG_BIG),
            jnp.where(rel <= len_ref[base + 1] - DRAFT, s[rows:], NEG_BIG)], 0)
        peak = jnp.max(s, axis=1, keepdims=True)
        p = jnp.exp2((s - peak) * scale)
        mass = jnp.sum(p, axis=1, keepdims=True)
        p_buf[j // 2] = p.astype(jnp.bfloat16)
        i_buf[j // 2] = jnp.broadcast_to(1.0 / mass, (2 * rows, head_dim))
        log_mass = jnp.broadcast_to(peak * scale + jnp.log2(mass), (2 * rows, head_dim))
        par = c % 2
        for n in range(2):
            at = pl.ds(first + j + n, rows, stride=PITCH)
            part_l.at[par][at, :] = log_mass[n * rows:(n + 1) * rows]

    def mix_pair(c, slot, first, j):
        v2 = jnp.concatenate([vbuf[slot, j], vbuf[slot, j + 1]], 1)
        o2 = jnp.dot(p_buf[j // 2], v2, preferred_element_type=jnp.float32)
        inv = i_buf[j // 2]
        par = c % 2
        for n in range(2):
            o = o2[n * rows:(n + 1) * rows, n * head_dim:(n + 1) * head_dim] * inv[n * rows:(n + 1) * rows]
            at = pl.ds(first + j + n, rows, stride=PITCH)
            part_o.at[par][at, :] = o

    lane = lax.broadcasted_iota(jnp.int32, (CHUNK, head_dim), 1)
    seq = lax.broadcasted_iota(jnp.int32, (CHUNK, head_dim), 0)

    def to_lanes(value):
        return jnp.sum(jnp.where(lane == seq, value, 0.0), axis=0, keepdims=True)

    def from_lanes(line):
        return jnp.sum(jnp.where(lane == seq, line, 0.0), axis=1, keepdims=True)

    def pair_copies(c):
        return tuple(pltpu.make_async_remote_copy(
            src_ref=src.at[c], dst_ref=dst.at[c], send_sem=ps_sem.at[n, c], recv_sem=pr_sem.at[n, c],
            device_id={"dup": partner}, device_id_type=MESH) for n, (src, dst) in enumerate(((pair_so, pair_ro), (pair_sl, pair_rl))))

    def chip_copies(c):
        copies = []
        for s, (there, peer) in enumerate(((1, behind), (0, ahead), (2, across))):
            for n, (src, dst) in enumerate(((chip_so, chip_ro), (chip_sl, chip_rl))):
                copies.append(pltpu.make_async_remote_copy(
                    src_ref=src.at[c, s], dst_ref=dst.at[c, there],
                    send_sem=cs_sem.at[n, s, c], recv_sem=cr_sem.at[n, there, c],
                    device_id={"dup": peer}, device_id_type=MESH))
        return copies

    def chip_arrivals(c):
        return [pltpu.make_async_remote_copy(
            src_ref=(chip_so, chip_sl)[n].at[c, s], dst_ref=(chip_ro, chip_rl)[n].at[c, s],
            send_sem=cs_sem.at[n, s, c], recv_sem=cr_sem.at[n, s, c],
            device_id={"dup": partner}, device_id_type=MESH) for s in range(3) for n in range(2)]

    def slab(ref, par, row):
        return ref.at[par][pl.ds(row * PITCH, CHUNK), :]

    def give_partner(c):
        par = c % 2
        for s in range(4):
            for i in range(own):
                pair_so[c, s, i * CHUNK:(i + 1) * CHUNK, :] = slab(part_o, par, half + s * own + i).astype(jnp.bfloat16)
        for s in range(4):
            for i in range(own):
                pair_sl[c, s, i:i + 1, :] = to_lanes(slab(part_l, par, half + s * own + i))
        for copy in pair_copies(c):
            copy.start()

    def merge_chip(c):
        par = c % 2
        for copy in pair_copies(c):
            copy.wait_recv()
        for s in (3, 1, 2, 0):
            for i in range(own):
                mine = slab(part_l, par, s * own + i)
                theirs = from_lanes(pair_rl[c, s, i:i + 1, :])
                top = jnp.maximum(mine, theirs)
                w_mine, w_theirs = jnp.exp2(mine - top), jnp.exp2(theirs - top)
                total = w_mine + w_theirs
                o = (w_mine * slab(part_o, par, s * own + i)
                     + w_theirs * pair_ro[c, s, i * CHUNK:(i + 1) * CHUNK, :].astype(jnp.float32)) / total
                log_total = top + jnp.log2(total)
                if s == 0:
                    keep_o[par, i] = o
                    keep_l[par, i] = log_total
                else:
                    chip_so[c, s - 1, i * CHUNK:(i + 1) * CHUNK, :] = o.astype(jnp.bfloat16)
                    chip_sl[c, s - 1, i:i + 1, :] = to_lanes(log_total)
        for copy in chip_copies(c):
            copy.start()

    def merge_group(c):
        par = c % 2
        for copy in chip_arrivals(c):
            copy.wait_recv()
        for i in range(own):
            logs = [keep_l[par, i]] + [from_lanes(chip_rl[c, s, i:i + 1, :]) for s in range(3)]
            top = functools.reduce(jnp.maximum, logs)
            weights = [jnp.exp2(log - top) for log in logs]
            total = functools.reduce(jnp.add, weights)
            merged = weights[0] * keep_o[par, i]
            for s in range(3):
                merged = merged + weights[s + 1] * chip_ro[c, s, i * CHUNK:(i + 1) * CHUNK, :].astype(jnp.float32)
            o_ref[i, pl.ds(pl.multiple_of(c * CHUNK, CHUNK), CHUNK), :] = (merged / total).astype(jnp.bfloat16)

    def chunk_step(c, carry):
        @pl.when(c + 2 < chunks)
        def _():
            q_own(c + 2)

        @pl.when(c + 1 < chunks)
        def _():
            q_pass_near(c + 1)

        widen_queries(c)

        def group_step(g, inner):
            group = c * (CHUNK // GROUP) + g
            slot = group % SLOTS
            for copy in cache_copies(group):
                copy.wait()
            for phase, times in ((score_pair, TIMES[0]), (soft_pair, TIMES[1]), (mix_pair, TIMES[2])):
                def again(_, x):
                    for j in range(0, GROUP, 2):
                        phase(c, slot, g * GROUP, j)
                    return x
                lax.fori_loop(0, times, again, 0)

            @pl.when(group + SLOTS < groups)
            def _():
                start_cache(group + SLOTS)
            return inner

        lax.fori_loop(0, CHUNK // GROUP, group_step, 0)

        @pl.when(c + 1 < chunks)
        def _():
            q_pass_far(c + 1)

        give_partner(c)

        @pl.when(c >= 2)
        def _():
            merge_group(c - 2)

        @pl.when(c >= 1)
        def _():
            merge_chip(c - 1)
        return carry

    lax.fori_loop(0, chunks, chunk_step, 0)
    merge_group(chunks - 2)
    merge_chip(chunks - 1)
    merge_group(chunks - 1)

    def drain(c, carry):
        for kind in range(7):
            q_copy(kind, c).wait_send()
        for copy in pair_copies(c) + tuple(chip_copies(c)):
            copy.wait_send()
        return carry

    lax.fori_loop(0, chunks, drain, 0)


def solution(mesh):
    def group_step(q_local, k_span, v_span, len_local):
        num_batch, own, head_dim = q_local.shape
        span = k_span.shape[1]
        chunks = num_batch // CHUNK
        rows = 8 * own
        vmem = functools.partial(pl.BlockSpec, memory_space=pltpu.VMEM)
        hbm = functools.partial(pl.BlockSpec, memory_space=pl.ANY)
        bf16, f32 = jnp.bfloat16, jnp.float32
        dma = pltpu.SemaphoreType.DMA
        out = pl.pallas_call(
            attend,
            out_shape=jax.ShapeDtypeStruct((own, num_batch, head_dim), bf16),
            in_specs=[vmem(), pl.BlockSpec(memory_space=pltpu.SMEM), hbm(), hbm()],
            out_specs=vmem(),
            scratch_shapes=[
                pltpu.VMEM((SLOTS, GROUP, span, head_dim), bf16),
                pltpu.VMEM((SLOTS, GROUP, span, head_dim), bf16),
                pltpu.VMEM((8, own, num_batch, head_dim), bf16),
                pltpu.VMEM((rows * PITCH, head_dim), f32),
                pltpu.VMEM((rows, span), jnp.int32),
                pltpu.VMEM((2, rows * PITCH, head_dim), f32),
                pltpu.VMEM((2, rows * PITCH, head_dim), f32),
                pltpu.VMEM((chunks, 4, own * CHUNK, head_dim), bf16),
                pltpu.VMEM((chunks, 4, own, head_dim), f32),
                pltpu.VMEM((chunks, 4, own * CHUNK, head_dim), bf16),
                pltpu.VMEM((chunks, 4, own, head_dim), f32),
                pltpu.VMEM((chunks, 3, own * CHUNK, head_dim), bf16),
                pltpu.VMEM((chunks, 3, own, head_dim), f32),
                pltpu.VMEM((chunks, 3, own * CHUNK, head_dim), bf16),
                pltpu.VMEM((chunks, 3, own, head_dim), f32),
                pltpu.VMEM((2, own, CHUNK, head_dim), f32),
                pltpu.VMEM((2, own, CHUNK, head_dim), f32),
                dma((SLOTS,)), dma((SLOTS,)),
                dma((7, chunks)), dma((7, chunks)),
                dma((2, chunks)), dma((2, chunks)),
                dma((2, 3, chunks)), dma((2, 3, chunks)),
                pltpu.VMEM((GROUP // 2, 2 * rows, span), f32), pltpu.VMEM((GROUP // 2, 2 * rows, span), bf16), pltpu.VMEM((GROUP // 2, 2 * rows, head_dim), f32),
            ],
            compiler_params=pltpu.CompilerParams(
                collective_id=0, has_side_effects=True, vmem_limit_bytes=60 * 1024 * 1024),
            cost_estimate=pl.CostEstimate(
                flops=4 * num_batch * rows * span * head_dim,
                bytes_accessed=4 * num_batch * span * head_dim,
                transcendentals=num_batch * rows * span),
        )(q_local.transpose(1, 0, 2), len_local, k_span, v_span)
        return out.transpose(1, 0, 2)

    return jax.shard_map(
        group_step, mesh=mesh,
        in_specs=(P("kv", "dup", None), P("kv", "dup", None), P("kv", "dup", None), P("kv")),
        out_specs=P("kv", "dup", None), check_vma=False)
```

```python
import functools

import jax
import jax.numpy as jnp
from jax import lax
from jax.experimental import pallas as pl
from jax.experimental.pallas import tpu as pltpu
from jax.sharding import PartitionSpec as P

DRAFT = 4
NEG_BIG = -3e38
LOG2E = 1.4426950408889634
MESH = pl.DeviceIdType.MESH

GROUP = 16
KEYS = 10
VALUES = 11
PITCH = GROUP + 4
RING = 8
KEEP = 16
ASK = 2
GIVE, MERGE, FINAL = 3, 5, 9


def attend(q_ref, len_ref, k_hbm, v_hbm, o_ref,
           kbuf, vbuf, q_all, q_wide, pos_rel, s_buf, p_buf, i_buf, part_o, part_l,
           pair_so, pair_sl, pair_ro, pair_rl,
           chip_so, chip_sl, chip_ro, chip_rl, keep_o, keep_l,
           k_sem, v_sem, qs_sem, qr_sem, ps_sem, pr_sem, cs_sem, cr_sem):
    own, num_batch, head_dim = q_ref.shape
    span = k_hbm.shape[1]
    rows = 8 * own
    half = 4 * own
    steps = num_batch // GROUP
    asks = steps // ASK
    scale = (head_dim ** -0.5) * LOG2E

    me = lax.axis_index("dup")
    chip = me // 2
    core = me % 2
    turn = 1 - 2 * core
    partner = chip * 2 + (1 - core)
    ahead = ((chip + turn + 4) % 4) * 2 + core
    behind = ((chip - turn + 4) % 4) * 2 + core
    across = ((chip + 2) % 4) * 2 + core

    def key_copy(g):
        return pltpu.make_async_copy(k_hbm.at[pl.ds(g * GROUP, GROUP)], kbuf.at[g % KEYS], k_sem.at[g % KEYS])

    def value_copy(g):
        return pltpu.make_async_copy(v_hbm.at[pl.ds(g * GROUP, GROUP)], vbuf.at[g % VALUES], v_sem.at[g % VALUES])

    key_copy(0).start()
    key_copy(1).start()

    def start_cache(g, carry):
        key_copy(g + 2).start()
        value_copy(g).start()
        return carry

    lax.fori_loop(0, KEYS - 2, start_cache, 0)
    for g in range(KEYS - 2, VALUES):
        value_copy(g).start()

    barrier = pltpu.get_barrier_semaphore()
    for peer in (partner, ahead, behind, across):
        pl.semaphore_signal(barrier, inc=1, device_id={"dup": peer}, device_id_type=MESH)

    def q_copy(kind, c):
        part = pl.ds(pl.multiple_of(c * ASK * GROUP, ASK * GROUP), ASK * GROUP)
        src, dst, peer = (
            (q_ref.at[:, part], q_all.at[2, :, part], behind),
            (q_ref.at[:, part], q_all.at[1, :, part], ahead),
            (q_ref.at[:, part], q_all.at[4, :, part], partner),
            (q_all.at[1, :, part], q_all.at[3, :, part], ahead),
            (q_all.at[1, :, part], q_all.at[5, :, part], partner),
            (q_all.at[2, :, part], q_all.at[6, :, part], partner),
            (q_all.at[3, :, part], q_all.at[7, :, part], partner),
        )[kind]
        return pltpu.make_async_remote_copy(
            src_ref=src, dst_ref=dst, send_sem=qs_sem.at[kind, c], recv_sem=qr_sem.at[kind, c],
            device_id={"dup": peer}, device_id_type=MESH)

    def q_own(c):
        for kind in (0, 1, 2):
            q_copy(kind, c).start()

    def q_pass_near(c):
        q_copy(1, c).wait_recv()
        q_copy(3, c).start()
        q_copy(4, c).start()
        q_copy(0, c).wait_recv()
        q_copy(5, c).start()

    def q_pass_far(c):
        q_copy(3, c).wait_recv()
        q_copy(6, c).start()

    span_start = me * span
    chip_disp = (0, 4 - turn, 4 + turn, 2)
    pair_disp = (0, 4 + turn, 4 - turn, 2)
    row_id = lax.broadcasted_iota(jnp.int32, (rows, span), 0)
    token = jnp.zeros((rows, span), jnp.int32)
    for h in range(2):
        for s in range(4):
            disp = (chip_disp, pair_disp)[h][s]
            device = ((chip + disp) % 4) * 2 + (core if h == 0 else 1 - core)
            for i in range(own):
                token = jnp.where(row_id == h * half + s * own + i, (own * device + i) % DRAFT, token)
    pos_rel[...] = lax.broadcasted_iota(jnp.int32, (rows, span), 1) + span_start - token

    pl.semaphore_wait(barrier, 4)
    q_own(0)
    q_own(1)
    q_pass_near(0)
    q_pass_far(0)
    q_pass_near(1)
    q_own(2)
    q_own(3)

    def q_arrive(c):
        for kind in (2, 4, 5, 6):
            q_copy(kind, c).wait_recv()

    lane = lax.broadcasted_iota(jnp.int32, (GROUP, head_dim), 1)
    seq = lax.broadcasted_iota(jnp.int32, (GROUP, head_dim), 0)

    def score(g):
        part = pl.ds(pl.multiple_of(g * GROUP, GROUP), GROUP)
        for s in range(8):
            for i in range(own):
                block = q_ref[i, part, :] if s == 0 else q_all[s, i, part, :]
                q_wide[pl.ds((s * own + i) * PITCH, GROUP), :] = block.astype(jnp.float32)
        slot = g % KEYS
        zeros = jnp.zeros((rows, head_dim), jnp.float32)
        for j in range(0, GROUP, 2):
            q0 = q_wide[pl.ds(j, rows, stride=PITCH), :]
            q1 = q_wide[pl.ds(j + 1, rows, stride=PITCH), :]
            q2 = jnp.concatenate([jnp.concatenate([q0, zeros], 1), jnp.concatenate([zeros, q1], 1)], 0).astype(jnp.bfloat16)
            k2 = jnp.concatenate([kbuf[slot, j], kbuf[slot, j + 1]], 1)
            s_buf[j // 2] = lax.dot_general(q2, k2, (((1,), (1,)), ((), ())), preferred_element_type=jnp.float32)

    def soften(g):
        slab_l = part_l.at[g % RING]
        for j in range(0, GROUP, 2):
            s = s_buf[j // 2]
            rel = pos_rel[...]
            base = g * GROUP + j
            s = jnp.concatenate([
                jnp.where(rel <= len_ref[base] - DRAFT, s[:rows], NEG_BIG),
                jnp.where(rel <= len_ref[base + 1] - DRAFT, s[rows:], NEG_BIG)], 0)
            peak = jnp.max(s, axis=1, keepdims=True)
            p = jnp.exp2((s - peak) * scale)
            mass = jnp.sum(p, axis=1, keepdims=True)
            p_buf[j // 2] = p.astype(jnp.bfloat16)
            i_buf[j // 2] = jnp.broadcast_to(1.0 / mass, (2 * rows, head_dim))
            log_mass = jnp.broadcast_to(peak * scale + jnp.log2(mass), (2 * rows, head_dim))
            for n in range(2):
                slab_l[pl.ds(j + n, rows, stride=PITCH), :] = log_mass[n * rows:(n + 1) * rows]

    def mix(g):
        slot = g % VALUES
        slab_o = part_o.at[g % RING]
        for j in range(0, GROUP, 2):
            v2 = jnp.concatenate([vbuf[slot, j], vbuf[slot, j + 1]], 1)
            o2 = jnp.dot(p_buf[j // 2], v2, preferred_element_type=jnp.float32)
            inv = i_buf[j // 2]
            for n in range(2):
                o = o2[n * rows:(n + 1) * rows, n * head_dim:(n + 1) * head_dim] * inv[n * rows:(n + 1) * rows]
                slab_o[pl.ds(j + n, rows, stride=PITCH), :] = o

    def to_lanes(values):
        total = jnp.zeros((GROUP, head_dim), jnp.float32)
        for i, value in enumerate(values):
            total = jnp.where(lane == seq + i * GROUP, value, total)
        return jnp.sum(total, axis=0, keepdims=True)

    def from_lanes(line, i):
        return jnp.sum(jnp.where(lane == seq + i * GROUP, line, 0.0), axis=1, keepdims=True)

    def pair_copies(c):
        return tuple(pltpu.make_async_remote_copy(
            src_ref=src.at[c], dst_ref=dst.at[c], send_sem=ps_sem.at[n, c], recv_sem=pr_sem.at[n, c],
            device_id={"dup": partner}, device_id_type=MESH) for n, (src, dst) in enumerate(((pair_so, pair_ro), (pair_sl, pair_rl))))

    def chip_copies(c):
        copies = []
        for s, (there, peer) in enumerate(((1, behind), (0, ahead), (2, across))):
            for n, (src, dst) in enumerate(((chip_so, chip_ro), (chip_sl, chip_rl))):
                copies.append(pltpu.make_async_remote_copy(
                    src_ref=src.at[c, s], dst_ref=dst.at[c, there],
                    send_sem=cs_sem.at[n, s, c], recv_sem=cr_sem.at[n, there, c],
                    device_id={"dup": peer}, device_id_type=MESH))
        return copies

    def chip_arrivals(c):
        return [pltpu.make_async_remote_copy(
            src_ref=(chip_so, chip_sl)[n].at[c, s], dst_ref=(chip_ro, chip_rl)[n].at[c, s],
            send_sem=cs_sem.at[n, s, c], recv_sem=cr_sem.at[n, s, c],
            device_id={"dup": partner}, device_id_type=MESH) for s in range(3) for n in range(2)]

    def slab(ref, g, row):
        return ref.at[g % RING][pl.ds(row * PITCH, GROUP), :]

    spare = FINAL

    def place(g):
        return (g + steps + spare) % (steps + spare)

    def give(g):
        c, r = place(g), g + KEEP
        for s in range(4):
            for i in range(own):
                pair_so[c, s, i * GROUP:(i + 1) * GROUP, :] = slab(part_o, r, half + s * own + i).astype(jnp.bfloat16)
        for s in range(4):
            pair_sl[c, s] = to_lanes([slab(part_l, r, half + s * own + i) for i in range(own)])

    def merge(g):
        c, r = place(g), g + KEEP
        for s in (3, 1, 2, 0):
            logs = []
            line = pair_rl[c, s]
            for i in range(own):
                mine = slab(part_l, r, s * own + i)
                theirs = from_lanes(line, i)
                top = jnp.maximum(mine, theirs)
                w_mine, w_theirs = jnp.exp2(mine - top), jnp.exp2(theirs - top)
                total = w_mine + w_theirs
                o = (w_mine * slab(part_o, r, s * own + i)
                     + w_theirs * pair_ro[c, s, i * GROUP:(i + 1) * GROUP, :].astype(jnp.float32)) / total
                log_total = top + jnp.log2(total)
                if s == 0:
                    keep_o[r % KEEP, i] = o
                    keep_l[r % KEEP, i] = log_total
                else:
                    chip_so[c, s - 1, i * GROUP:(i + 1) * GROUP, :] = o.astype(jnp.bfloat16)
                    logs.append(log_total)
            if s:
                chip_sl[c, s - 1] = to_lanes(logs)

    def final(g):
        c, r = place(g), g + KEEP
        to = pl.ds(pl.multiple_of(((g + steps) % steps) * GROUP, GROUP), GROUP)
        lines = [chip_rl[c, s] for s in range(3)]
        for i in range(own):
            logs = [keep_l[r % KEEP, i]] + [from_lanes(line, i) for line in lines]
            top = functools.reduce(jnp.maximum, logs)
            weights = [jnp.exp2(log - top) for log in logs]
            total = functools.reduce(jnp.add, weights)
            merged = weights[0] * keep_o[r % KEEP, i]
            for s in range(3):
                merged = merged + weights[s + 1] * chip_ro[c, s, i * GROUP:(i + 1) * GROUP, :].astype(jnp.float32)
            o_ref[i, to, :] = (merged / total).astype(jnp.bfloat16)

    def start_all(copies):
        for copy in copies:
            copy.start()

    def arrive_all(copies):
        for copy in copies:
            copy.wait_recv()

    q_arrive(0)
    key_copy(0).wait()
    score(0)
    key_copy(KEYS).start()
    key_copy(1).wait()
    soften(0)
    score(1)
    key_copy(KEYS + 1).start()
    q_pass_far(1)
    q_pass_near(2)

    def step(t, carry):
        c = t // ASK

        @pl.when(t % ASK == 0)
        def _():
            @pl.when(c + 3 < asks)
            def _():
                q_own(c + 3)

            @pl.when(c + 2 < asks)
            def _():
                q_pass_near(c + 2)

            @pl.when(c + 1 < asks)
            def _():
                q_pass_far(c + 1)

            q_arrive(c)

        key_copy(t).wait()
        value_copy(t - 2).wait()

        @pl.when(t >= MERGE)
        def _():
            arrive_all(pair_copies(t - MERGE))

        @pl.when(t >= FINAL)
        def _():
            arrive_all(chip_arrivals(t - FINAL))

        final(t - FINAL)
        merge(t - MERGE)
        give(t - GIVE)
        mix(t - 2)
        soften(t - 1)
        score(t)

        @pl.when(t + KEYS < steps)
        def _():
            key_copy(t + KEYS).start()

        @pl.when(t - 2 + VALUES < steps)
        def _():
            value_copy(t - 2 + VALUES).start()

        @pl.when(t >= GIVE)
        def _():
            start_all(pair_copies(t - GIVE))

        @pl.when(t >= MERGE)
        def _():
            start_all(chip_copies(t - MERGE))
        return carry

    lax.fori_loop(2, steps, step, 0)

    value_copy(steps - 2).wait()
    value_copy(steps - 1).wait()
    give(steps - GIVE)
    mix(steps - 2)
    soften(steps - 1)
    start_all(pair_copies(steps - GIVE))
    give(steps - 2)
    mix(steps - 1)
    start_all(pair_copies(steps - 2))
    give(steps - 1)
    start_all(pair_copies(steps - 1))

    def last_merge(g, carry):
        arrive_all(pair_copies(g))
        merge(g)
        start_all(chip_copies(g))
        return carry

    lax.fori_loop(steps - MERGE, steps, last_merge, 0)

    def last_final(g, carry):
        arrive_all(chip_arrivals(g))
        final(g)
        return carry

    lax.fori_loop(steps - FINAL, steps, last_final, 0)

    def drain_asks(c, carry):
        for kind in range(7):
            q_copy(kind, c).wait_send()
        return carry

    lax.fori_loop(0, asks, drain_asks, 0)

    def drain(c, carry):
        for copy in pair_copies(c) + tuple(chip_copies(c)):
            copy.wait_send()
        return carry

    lax.fori_loop(0, steps, drain, 0)


def solution(mesh):
    def group_step(q_local, k_span, v_span, len_local):
        num_batch, own, head_dim = q_local.shape
        span = k_span.shape[1]
        steps = num_batch // GROUP
        asks = steps // ASK
        places = steps + FINAL
        rows = 8 * own
        vmem = functools.partial(pl.BlockSpec, memory_space=pltpu.VMEM)
        hbm = functools.partial(pl.BlockSpec, memory_space=pl.ANY)
        bf16, f32 = jnp.bfloat16, jnp.float32
        dma = pltpu.SemaphoreType.DMA
        out = pl.pallas_call(
            attend,
            out_shape=jax.ShapeDtypeStruct((own, num_batch, head_dim), bf16),
            in_specs=[vmem(), pl.BlockSpec(memory_space=pltpu.SMEM), hbm(), hbm()],
            out_specs=vmem(),
            scratch_shapes=[
                pltpu.VMEM((KEYS, GROUP, span, head_dim), bf16),
                pltpu.VMEM((VALUES, GROUP, span, head_dim), bf16),
                pltpu.VMEM((8, own, num_batch, head_dim), bf16),
                pltpu.VMEM((rows * PITCH, head_dim), f32),
                pltpu.VMEM((rows, span), jnp.int32),
                pltpu.VMEM((GROUP // 2, 2 * rows, span), f32),
                pltpu.VMEM((GROUP // 2, 2 * rows, span), bf16),
                pltpu.VMEM((GROUP // 2, 2 * rows, head_dim), f32),
                pltpu.VMEM((RING, rows * PITCH, head_dim), f32),
                pltpu.VMEM((RING, rows * PITCH, head_dim), f32),
                pltpu.VMEM((places, 4, own * GROUP, head_dim), bf16),
                pltpu.VMEM((places, 4, 1, head_dim), f32),
                pltpu.VMEM((places, 4, own * GROUP, head_dim), bf16),
                pltpu.VMEM((places, 4, 1, head_dim), f32),
                pltpu.VMEM((places, 3, own * GROUP, head_dim), bf16),
                pltpu.VMEM((places, 3, 1, head_dim), f32),
                pltpu.VMEM((places, 3, own * GROUP, head_dim), bf16),
                pltpu.VMEM((places, 3, 1, head_dim), f32),
                pltpu.VMEM((KEEP, own, GROUP, head_dim), f32),
                pltpu.VMEM((KEEP, own, GROUP, head_dim), f32),
                dma((KEYS,)), dma((VALUES,)),
                dma((7, asks)), dma((7, asks)),
                dma((2, steps)), dma((2, steps)),
                dma((2, 3, steps)), dma((2, 3, steps)),
            ],
            compiler_params=pltpu.CompilerParams(
                collective_id=0, has_side_effects=True, vmem_limit_bytes=60 * 1024 * 1024),
            cost_estimate=pl.CostEstimate(
                flops=4 * num_batch * rows * span * head_dim,
                bytes_accessed=4 * num_batch * span * head_dim,
                transcendentals=num_batch * rows * span),
        )(q_local.transpose(1, 0, 2), len_local, k_span, v_span)
        return out.transpose(1, 0, 2)

    return jax.shard_map(
        group_step, mesh=mesh,
        in_specs=(P("kv", "dup", None), P("kv", "dup", None), P("kv", "dup", None), P("kv")),
        out_specs=P("kv", "dup", None), check_vma=False)
```

```python
import functools

import jax
import jax.numpy as jnp
from jax import lax
from jax.experimental import pallas as pl
from jax.experimental.pallas import tpu as pltpu
from jax.sharding import PartitionSpec as P

DRAFT = 4
NEG_BIG = -3e38
LOG2E = 1.4426950408889634
MESH = pl.DeviceIdType.MESH

GROUP = 16
KEYS = 10
VALUES = 11
PITCH = GROUP + 4
RING = 8
KEEP = 16
ASK = 2
GIVE, MERGE, RELAY, FINAL = 3, 5, 7, 9


def attend(q_ref, len_ref, k_hbm, v_hbm, o_ref,
           kbuf, vbuf, q_all, q_wide, pos_rel, s_buf, p_buf, i_buf, part_o, part_l,
           pair_so, pair_sl, pair_ro, pair_rl,
           chip_so, chip_sl, chip_ro, chip_rl, relay_o, relay_l, keep_o, keep_l,
           k_sem, v_sem, qs_sem, qr_sem, ps_sem, pr_sem, cs_sem, cr_sem, rs_sem, rr_sem):
    own, num_batch, head_dim = q_ref.shape
    span = k_hbm.shape[1]
    rows = 8 * own
    half = 4 * own
    steps = num_batch // GROUP
    asks = steps // ASK
    scale = (head_dim ** -0.5) * LOG2E

    me = lax.axis_index("dup")
    chip = me // 2
    core = me % 2
    turn = 1 - 2 * core
    partner = chip * 2 + (1 - core)
    ahead = ((chip + turn + 4) % 4) * 2 + core
    behind = ((chip - turn + 4) % 4) * 2 + core

    def key_copy(g):
        return pltpu.make_async_copy(k_hbm.at[pl.ds(g * GROUP, GROUP)], kbuf.at[g % KEYS], k_sem.at[g % KEYS])

    def value_copy(g):
        return pltpu.make_async_copy(v_hbm.at[pl.ds(g * GROUP, GROUP)], vbuf.at[g % VALUES], v_sem.at[g % VALUES])

    key_copy(0).start()
    key_copy(1).start()

    def start_cache(g, carry):
        key_copy(g + 2).start()
        value_copy(g).start()
        return carry

    lax.fori_loop(0, KEYS - 2, start_cache, 0)
    for g in range(KEYS - 2, VALUES):
        value_copy(g).start()

    barrier = pltpu.get_barrier_semaphore()
    for peer in (partner, ahead, behind):
        pl.semaphore_signal(barrier, inc=1, device_id={"dup": peer}, device_id_type=MESH)

    def q_copy(kind, c):
        part = pl.ds(pl.multiple_of(c * ASK * GROUP, ASK * GROUP), ASK * GROUP)
        src, dst, peer = (
            (q_ref.at[:, part], q_all.at[2, :, part], behind),
            (q_ref.at[:, part], q_all.at[1, :, part], ahead),
            (q_ref.at[:, part], q_all.at[4, :, part], partner),
            (q_all.at[1, :, part], q_all.at[3, :, part], ahead),
            (q_all.at[1, :, part], q_all.at[5, :, part], partner),
            (q_all.at[2, :, part], q_all.at[6, :, part], partner),
            (q_all.at[3, :, part], q_all.at[7, :, part], partner),
        )[kind]
        return pltpu.make_async_remote_copy(
            src_ref=src, dst_ref=dst, send_sem=qs_sem.at[kind, c], recv_sem=qr_sem.at[kind, c],
            device_id={"dup": peer}, device_id_type=MESH)

    def q_own(c):
        for kind in (0, 1, 2):
            q_copy(kind, c).start()

    def q_pass_near(c):
        q_copy(1, c).wait_recv()
        q_copy(3, c).start()
        q_copy(4, c).start()
        q_copy(0, c).wait_recv()
        q_copy(5, c).start()

    def q_pass_far(c):
        q_copy(3, c).wait_recv()
        q_copy(6, c).start()

    span_start = me * span
    chip_disp = (0, 4 - turn, 4 + turn, 2)
    pair_disp = (0, 4 + turn, 4 - turn, 2)
    row_id = lax.broadcasted_iota(jnp.int32, (rows, span), 0)
    token = jnp.zeros((rows, span), jnp.int32)
    for h in range(2):
        for s in range(4):
            disp = (chip_disp, pair_disp)[h][s]
            device = ((chip + disp) % 4) * 2 + (core if h == 0 else 1 - core)
            for i in range(own):
                token = jnp.where(row_id == h * half + s * own + i, (own * device + i) % DRAFT, token)
    pos_rel[...] = lax.broadcasted_iota(jnp.int32, (rows, span), 1) + span_start - token

    pl.semaphore_wait(barrier, 3)
    q_own(0)
    q_own(1)
    q_pass_near(0)
    q_pass_far(0)
    q_pass_near(1)
    q_own(2)
    q_own(3)

    def q_arrive(c):
        for kind in (2, 4, 5, 6):
            q_copy(kind, c).wait_recv()

    lane = lax.broadcasted_iota(jnp.int32, (GROUP, head_dim), 1)
    seq = lax.broadcasted_iota(jnp.int32, (GROUP, head_dim), 0)

    def score(g):
        part = pl.ds(pl.multiple_of(g * GROUP, GROUP), GROUP)
        for s in range(8):
            for i in range(own):
                block = q_ref[i, part, :] if s == 0 else q_all[s, i, part, :]
                q_wide[pl.ds((s * own + i) * PITCH, GROUP), :] = block.astype(jnp.float32)
        slot = g % KEYS
        zeros = jnp.zeros((rows, head_dim), jnp.float32)
        for j in range(0, GROUP, 2):
            q0 = q_wide[pl.ds(j, rows, stride=PITCH), :]
            q1 = q_wide[pl.ds(j + 1, rows, stride=PITCH), :]
            q2 = jnp.concatenate([jnp.concatenate([q0, zeros], 1), jnp.concatenate([zeros, q1], 1)], 0).astype(jnp.bfloat16)
            k2 = jnp.concatenate([kbuf[slot, j], kbuf[slot, j + 1]], 1)
            s_buf[j // 2] = lax.dot_general(q2, k2, (((1,), (1,)), ((), ())), preferred_element_type=jnp.float32)

    def soften(g):
        slab_l = part_l.at[g % RING]
        for j in range(0, GROUP, 2):
            s = s_buf[j // 2]
            rel = pos_rel[...]
            base = g * GROUP + j
            s = jnp.concatenate([
                jnp.where(rel <= len_ref[base] - DRAFT, s[:rows], NEG_BIG),
                jnp.where(rel <= len_ref[base + 1] - DRAFT, s[rows:], NEG_BIG)], 0)
            peak = jnp.max(s, axis=1, keepdims=True)
            p = jnp.exp2((s - peak) * scale)
            mass = jnp.sum(p, axis=1, keepdims=True)
            p_buf[j // 2] = p.astype(jnp.bfloat16)
            i_buf[j // 2] = jnp.broadcast_to(1.0 / mass, (2 * rows, head_dim))
            log_mass = jnp.broadcast_to(peak * scale + jnp.log2(mass), (2 * rows, head_dim))
            for n in range(2):
                slab_l[pl.ds(j + n, rows, stride=PITCH), :] = log_mass[n * rows:(n + 1) * rows]

    def mix(g):
        slot = g % VALUES
        slab_o = part_o.at[g % RING]
        for j in range(0, GROUP, 2):
            v2 = jnp.concatenate([vbuf[slot, j], vbuf[slot, j + 1]], 1)
            o2 = jnp.dot(p_buf[j // 2], v2, preferred_element_type=jnp.float32)
            inv = i_buf[j // 2]
            for n in range(2):
                o = o2[n * rows:(n + 1) * rows, n * head_dim:(n + 1) * head_dim] * inv[n * rows:(n + 1) * rows]
                slab_o[pl.ds(j + n, rows, stride=PITCH), :] = o

    def to_lanes(values):
        total = jnp.zeros((GROUP, head_dim), jnp.float32)
        for i, value in enumerate(values):
            total = jnp.where(lane == seq + i * GROUP, value, total)
        return jnp.sum(total, axis=0, keepdims=True)

    def from_lanes(line, i):
        return jnp.sum(jnp.where(lane == seq + i * GROUP, line, 0.0), axis=1, keepdims=True)

    def pair_copies(c):
        return tuple(pltpu.make_async_remote_copy(
            src_ref=src.at[c], dst_ref=dst.at[c], send_sem=ps_sem.at[n, c], recv_sem=pr_sem.at[n, c],
            device_id={"dup": partner}, device_id_type=MESH) for n, (src, dst) in enumerate(((pair_so, pair_ro), (pair_sl, pair_rl))))

    def chip_copies(c):
        copies = []
        for n, (src, dst, via) in enumerate(((chip_so, chip_ro, relay_o), (chip_sl, chip_rl, relay_l))):
            for s, to, sem, peer in ((2, via.at[c], rr_sem.at[n, c], ahead),
                                     (1, dst.at[c, 0], cr_sem.at[n, 0, c], ahead),
                                     (0, dst.at[c, 1], cr_sem.at[n, 1, c], behind)):
                copies.append(pltpu.make_async_remote_copy(
                    src_ref=src.at[c, s], dst_ref=to, send_sem=cs_sem.at[n, s, c], recv_sem=sem,
                    device_id={"dup": peer}, device_id_type=MESH))
        return copies

    def relay_copies(c):
        return [pltpu.make_async_remote_copy(
            src_ref=via.at[c], dst_ref=dst.at[c, 2], send_sem=rs_sem.at[n, c], recv_sem=cr_sem.at[n, 2, c],
            device_id={"dup": ahead}, device_id_type=MESH) for n, (via, dst) in enumerate(((relay_o, chip_ro), (relay_l, chip_rl)))]

    def pass_on(c):
        for n, via in enumerate((relay_o, relay_l)):
            pltpu.make_async_remote_copy(
                src_ref=via.at[c], dst_ref=via.at[c], send_sem=rs_sem.at[n, c], recv_sem=rr_sem.at[n, c],
                device_id={"dup": ahead}, device_id_type=MESH).wait_recv()
        for copy in relay_copies(c):
            copy.start()

    def chip_arrivals(c):
        return [pltpu.make_async_remote_copy(
            src_ref=(chip_so, chip_sl)[n].at[c, s], dst_ref=(chip_ro, chip_rl)[n].at[c, s],
            send_sem=cs_sem.at[n, s, c], recv_sem=cr_sem.at[n, s, c],
            device_id={"dup": partner}, device_id_type=MESH) for s in range(3) for n in range(2)]

    def slab(ref, g, row):
        return ref.at[g % RING][pl.ds(row * PITCH, GROUP), :]

    spare = FINAL

    def place(g):
        return (g + steps + spare) % (steps + spare)

    def give(g):
        c, r = place(g), g + KEEP
        for s in range(4):
            for i in range(own):
                pair_so[c, s, i * GROUP:(i + 1) * GROUP, :] = slab(part_o, r, half + s * own + i).astype(jnp.bfloat16)
        for s in range(4):
            pair_sl[c, s] = to_lanes([slab(part_l, r, half + s * own + i) for i in range(own)])

    def merge(g):
        c, r = place(g), g + KEEP
        for s in (3, 1, 2, 0):
            logs = []
            line = pair_rl[c, s]
            for i in range(own):
                mine = slab(part_l, r, s * own + i)
                theirs = from_lanes(line, i)
                top = jnp.maximum(mine, theirs)
                w_mine, w_theirs = jnp.exp2(mine - top), jnp.exp2(theirs - top)
                total = w_mine + w_theirs
                o = (w_mine * slab(part_o, r, s * own + i)
                     + w_theirs * pair_ro[c, s, i * GROUP:(i + 1) * GROUP, :].astype(jnp.float32)) / total
                log_total = top + jnp.log2(total)
                if s == 0:
                    keep_o[r % KEEP, i] = o
                    keep_l[r % KEEP, i] = log_total
                else:
                    chip_so[c, s - 1, i * GROUP:(i + 1) * GROUP, :] = o.astype(jnp.bfloat16)
                    logs.append(log_total)
            if s:
                chip_sl[c, s - 1] = to_lanes(logs)

    def final(g):
        c, r = place(g), g + KEEP
        to = pl.ds(pl.multiple_of(((g + steps) % steps) * GROUP, GROUP), GROUP)
        lines = [chip_rl[c, s] for s in range(3)]
        for i in range(own):
            logs = [keep_l[r % KEEP, i]] + [from_lanes(line, i) for line in lines]
            top = functools.reduce(jnp.maximum, logs)
            weights = [jnp.exp2(log - top) for log in logs]
            total = functools.reduce(jnp.add, weights)
            merged = weights[0] * keep_o[r % KEEP, i]
            for s in range(3):
                merged = merged + weights[s + 1] * chip_ro[c, s, i * GROUP:(i + 1) * GROUP, :].astype(jnp.float32)
            o_ref[i, to, :] = (merged / total).astype(jnp.bfloat16)

    def start_all(copies):
        for copy in copies:
            copy.start()

    def arrive_all(copies):
        for copy in copies:
            copy.wait_recv()

    q_arrive(0)
    key_copy(0).wait()
    score(0)
    key_copy(KEYS).start()
    key_copy(1).wait()
    soften(0)
    score(1)
    key_copy(KEYS + 1).start()
    q_pass_far(1)
    q_pass_near(2)

    def step(t, carry):
        c = t // ASK

        @pl.when(t % ASK == 0)
        def _():
            @pl.when(c + 3 < asks)
            def _():
                q_own(c + 3)

            @pl.when(c + 2 < asks)
            def _():
                q_pass_near(c + 2)

            @pl.when(c + 1 < asks)
            def _():
                q_pass_far(c + 1)

            q_arrive(c)

        key_copy(t).wait()
        value_copy(t - 2).wait()

        @pl.when(t >= MERGE)
        def _():
            arrive_all(pair_copies(t - MERGE))

        @pl.when(t >= RELAY)
        def _():
            pass_on(t - RELAY)

        @pl.when(t >= FINAL)
        def _():
            arrive_all(chip_arrivals(t - FINAL))

        final(t - FINAL)
        merge(t - MERGE)
        give(t - GIVE)
        mix(t - 2)
        soften(t - 1)
        score(t)

        @pl.when(t + KEYS < steps)
        def _():
            key_copy(t + KEYS).start()

        @pl.when(t - 2 + VALUES < steps)
        def _():
            value_copy(t - 2 + VALUES).start()

        @pl.when(t >= GIVE)
        def _():
            start_all(pair_copies(t - GIVE))

        @pl.when(t >= MERGE)
        def _():
            start_all(chip_copies(t - MERGE))
        return carry

    lax.fori_loop(2, steps, step, 0)

    value_copy(steps - 2).wait()
    value_copy(steps - 1).wait()
    give(steps - GIVE)
    mix(steps - 2)
    soften(steps - 1)
    start_all(pair_copies(steps - GIVE))
    give(steps - 2)
    mix(steps - 1)
    start_all(pair_copies(steps - 2))
    give(steps - 1)
    start_all(pair_copies(steps - 1))

    def last_merge(g, carry):
        arrive_all(pair_copies(g))
        merge(g)
        start_all(chip_copies(g))
        pass_on(g - 2)
        return carry

    def last_final(g, carry):
        arrive_all(chip_arrivals(g))
        final(g)
        return carry

    lax.fori_loop(steps - MERGE, steps, last_merge, 0)
    lax.fori_loop(steps - FINAL, steps - 5, last_final, 0)
    pass_on(steps - 2)
    pass_on(steps - 1)
    lax.fori_loop(steps - 5, steps, last_final, 0)

    def drain_asks(c, carry):
        for kind in range(7):
            q_copy(kind, c).wait_send()
        return carry

    lax.fori_loop(0, asks, drain_asks, 0)

    def drain(c, carry):
        for copy in list(pair_copies(c)) + chip_copies(c) + relay_copies(c):
            copy.wait_send()
        return carry

    lax.fori_loop(0, steps, drain, 0)


def solution(mesh):
    def group_step(q_local, k_span, v_span, len_local):
        num_batch, own, head_dim = q_local.shape
        span = k_span.shape[1]
        steps = num_batch // GROUP
        asks = steps // ASK
        places = steps + FINAL
        rows = 8 * own
        vmem = functools.partial(pl.BlockSpec, memory_space=pltpu.VMEM)
        hbm = functools.partial(pl.BlockSpec, memory_space=pl.ANY)
        bf16, f32 = jnp.bfloat16, jnp.float32
        dma = pltpu.SemaphoreType.DMA
        out = pl.pallas_call(
            attend,
            out_shape=jax.ShapeDtypeStruct((own, num_batch, head_dim), bf16),
            in_specs=[vmem(), pl.BlockSpec(memory_space=pltpu.SMEM), hbm(), hbm()],
            out_specs=vmem(),
            scratch_shapes=[
                pltpu.VMEM((KEYS, GROUP, span, head_dim), bf16),
                pltpu.VMEM((VALUES, GROUP, span, head_dim), bf16),
                pltpu.VMEM((8, own, num_batch, head_dim), bf16),
                pltpu.VMEM((rows * PITCH, head_dim), f32),
                pltpu.VMEM((rows, span), jnp.int32),
                pltpu.VMEM((GROUP // 2, 2 * rows, span), f32),
                pltpu.VMEM((GROUP // 2, 2 * rows, span), bf16),
                pltpu.VMEM((GROUP // 2, 2 * rows, head_dim), f32),
                pltpu.VMEM((RING, rows * PITCH, head_dim), f32),
                pltpu.VMEM((RING, rows * PITCH, head_dim), f32),
                pltpu.VMEM((places, 4, own * GROUP, head_dim), bf16),
                pltpu.VMEM((places, 4, 1, head_dim), f32),
                pltpu.VMEM((places, 4, own * GROUP, head_dim), bf16),
                pltpu.VMEM((places, 4, 1, head_dim), f32),
                pltpu.VMEM((places, 3, own * GROUP, head_dim), bf16),
                pltpu.VMEM((places, 3, 1, head_dim), f32),
                pltpu.VMEM((places, 3, own * GROUP, head_dim), bf16),
                pltpu.VMEM((places, 3, 1, head_dim), f32),
                pltpu.VMEM((steps, own * GROUP, head_dim), bf16),
                pltpu.VMEM((steps, 1, head_dim), f32),
                pltpu.VMEM((KEEP, own, GROUP, head_dim), f32),
                pltpu.VMEM((KEEP, own, GROUP, head_dim), f32),
                dma((KEYS,)), dma((VALUES,)),
                dma((7, asks)), dma((7, asks)),
                dma((2, steps)), dma((2, steps)),
                dma((2, 3, steps)), dma((2, 3, steps)),
                dma((2, steps)), dma((2, steps)),
            ],
            compiler_params=pltpu.CompilerParams(
                collective_id=0, has_side_effects=True, vmem_limit_bytes=60 * 1024 * 1024),
            cost_estimate=pl.CostEstimate(
                flops=4 * num_batch * rows * span * head_dim,
                bytes_accessed=4 * num_batch * span * head_dim,
                transcendentals=num_batch * rows * span),
        )(q_local.transpose(1, 0, 2), len_local, k_span, v_span)
        return out.transpose(1, 0, 2)

    return jax.shard_map(
        group_step, mesh=mesh,
        in_specs=(P("kv", "dup", None), P("kv", "dup", None), P("kv", "dup", None), P("kv")),
        out_specs=P("kv", "dup", None), check_vma=False)
```

```python
import functools

import jax
import jax.numpy as jnp
from jax import lax
from jax.experimental import pallas as pl
from jax.experimental.pallas import tpu as pltpu
from jax.sharding import PartitionSpec as P

DRAFT = 4
NEG_BIG = -3e38
LOG2E = 1.4426950408889634
MESH = pl.DeviceIdType.MESH

GROUP = 16
KEYS = 10
VALUES = 11
PITCH = GROUP + 4
RING = 8
KEEP = 16
ASK = 2
GIVE, MERGE, FINAL = 3, 6, 12
SPARE = 12


def attend(q_ref, len_ref, k_hbm, v_hbm, o_ref,
           kbuf, vbuf, q_all, q_wide, pos_rel, s_buf, p_buf, i_buf, part_o, part_l,
           pair_so, pair_ro, chip_so, chip_ro, pair_held, chip_held, keep_o, keep_l,
           k_sem, v_sem, qs_sem, qr_sem, ps_sem, pr_sem, cs_sem, cr_sem):
    own, num_batch, head_dim = q_ref.shape
    span = k_hbm.shape[1]
    rows = 8 * own
    half = 4 * own
    data = 2 * own * GROUP
    steps = num_batch // GROUP
    asks = steps // ASK
    scale = (head_dim ** -0.5) * LOG2E

    me = lax.axis_index("dup")
    chip = me // 2
    core = me % 2
    turn = 1 - 2 * core
    partner = chip * 2 + (1 - core)
    ahead = ((chip + turn + 4) % 4) * 2 + core
    behind = ((chip - turn + 4) % 4) * 2 + core
    across = ((chip + 2) % 4) * 2 + core

    def key_copy(g):
        return pltpu.make_async_copy(k_hbm.at[pl.ds(g * GROUP, GROUP)], kbuf.at[g % KEYS], k_sem.at[g % KEYS])

    def value_copy(g):
        return pltpu.make_async_copy(v_hbm.at[pl.ds(g * GROUP, GROUP)], vbuf.at[g % VALUES], v_sem.at[g % VALUES])

    key_copy(0).start()
    key_copy(1).start()

    def start_cache(g, carry):
        key_copy(g + 2).start()
        value_copy(g).start()
        return carry

    lax.fori_loop(0, KEYS - 2, start_cache, 0)
    for g in range(KEYS - 2, VALUES):
        value_copy(g).start()

    barrier = pltpu.get_barrier_semaphore()
    for peer in (partner, ahead, behind, across):
        pl.semaphore_signal(barrier, inc=1, device_id={"dup": peer}, device_id_type=MESH)

    def q_copy(kind, c):
        part = pl.ds(pl.multiple_of(c * ASK * GROUP, ASK * GROUP), ASK * GROUP)
        src, dst, peer = (
            (q_ref.at[:, part], q_all.at[2, :, part], behind),
            (q_ref.at[:, part], q_all.at[1, :, part], ahead),
            (q_ref.at[:, part], q_all.at[4, :, part], partner),
            (q_all.at[1, :, part], q_all.at[3, :, part], ahead),
            (q_all.at[1:4, :, part], q_all.at[5:8, :, part], partner),
        )[kind]
        return pltpu.make_async_remote_copy(
            src_ref=src, dst_ref=dst, send_sem=qs_sem.at[kind, c], recv_sem=qr_sem.at[kind, c],
            device_id={"dup": peer}, device_id_type=MESH)

    def q_own(c):
        for kind in (0, 1, 2):
            q_copy(kind, c).start()

    def q_pass_near(c):
        q_copy(1, c).wait_recv()
        q_copy(3, c).start()

    def q_pass_far(c):
        q_copy(0, c).wait_recv()
        q_copy(3, c).wait_recv()
        q_copy(4, c).start()

    span_start = me * span
    chip_disp = (0, 4 - turn, 4 + turn, 2)
    pair_disp = (0, 4 + turn, 4 - turn, 2)
    row_id = lax.broadcasted_iota(jnp.int32, (rows, span), 0)
    token = jnp.zeros((rows, span), jnp.int32)
    for h in range(2):
        for s in range(4):
            disp = (chip_disp, pair_disp)[h][s]
            device = ((chip + disp) % 4) * 2 + (core if h == 0 else 1 - core)
            for i in range(own):
                token = jnp.where(row_id == h * half + s * own + i, (own * device + i) % DRAFT, token)
    pos_rel[...] = lax.broadcasted_iota(jnp.int32, (rows, span), 1) + span_start - token

    pl.semaphore_wait(barrier, 4)
    q_own(0)
    q_own(1)
    q_pass_near(0)
    q_pass_far(0)
    q_pass_near(1)
    q_own(2)
    q_own(3)

    def q_arrive(c):
        for kind in (2, 4):
            q_copy(kind, c).wait_recv()

    lane = lax.broadcasted_iota(jnp.int32, (GROUP, head_dim), 1)
    seq = lax.broadcasted_iota(jnp.int32, (GROUP, head_dim), 0)

    def score(g):
        part = pl.ds(pl.multiple_of(g * GROUP, GROUP), GROUP)
        for s in range(8):
            for i in range(own):
                block = q_ref[i, part, :] if s == 0 else q_all[s, i, part, :]
                q_wide[pl.ds((s * own + i) * PITCH, GROUP), :] = block.astype(jnp.float32)
        slot = g % KEYS
        zeros = jnp.zeros((rows, head_dim), jnp.float32)
        for j in range(0, GROUP, 2):
            q0 = q_wide[pl.ds(j, rows, stride=PITCH), :]
            q1 = q_wide[pl.ds(j + 1, rows, stride=PITCH), :]
            q2 = jnp.concatenate([jnp.concatenate([q0, zeros], 1), jnp.concatenate([zeros, q1], 1)], 0).astype(jnp.bfloat16)
            k2 = jnp.concatenate([kbuf[slot, j], kbuf[slot, j + 1]], 1)
            s_buf[j // 2] = lax.dot_general(q2, k2, (((1,), (1,)), ((), ())), preferred_element_type=jnp.float32)

    def soften(g):
        slab_l = part_l.at[g % RING]
        for j in range(0, GROUP, 2):
            s = s_buf[j // 2]
            rel = pos_rel[...]
            base = g * GROUP + j
            s = jnp.concatenate([
                jnp.where(rel <= len_ref[base] - DRAFT, s[:rows], NEG_BIG),
                jnp.where(rel <= len_ref[base + 1] - DRAFT, s[rows:], NEG_BIG)], 0)
            peak = jnp.max(s, axis=1, keepdims=True)
            p = jnp.exp2((s - peak) * scale)
            mass = jnp.sum(p, axis=1, keepdims=True)
            p_buf[j // 2] = p.astype(jnp.bfloat16)
            i_buf[j // 2] = jnp.broadcast_to(1.0 / mass, (2 * rows, head_dim))
            log_mass = jnp.broadcast_to(peak * scale + jnp.log2(mass), (2 * rows, head_dim))
            for n in range(2):
                slab_l[pl.ds(j + n, rows, stride=PITCH), :] = log_mass[n * rows:(n + 1) * rows]

    def mix(g):
        slot = g % VALUES
        slab_o = part_o.at[g % RING]
        for j in range(0, GROUP, 2):
            v2 = jnp.concatenate([vbuf[slot, j], vbuf[slot, j + 1]], 1)
            o2 = jnp.dot(p_buf[j // 2], v2, preferred_element_type=jnp.float32)
            inv = i_buf[j // 2]
            for n in range(2):
                o = o2[n * rows:(n + 1) * rows, n * head_dim:(n + 1) * head_dim] * inv[n * rows:(n + 1) * rows]
                slab_o[pl.ds(j + n, rows, stride=PITCH), :] = o

    def to_lanes(values, h, held):
        total = jnp.zeros((GROUP, head_dim), jnp.float32)
        for i, value in enumerate(values):
            total = jnp.where(lane == seq + (h * own + i) * GROUP, value, total)
        line = jnp.sum(total, axis=0, keepdims=True)
        line = jnp.where(lane[:1] >= h * own * GROUP, line, held[...])
        held[...] = line
        high = line.astype(jnp.bfloat16).astype(jnp.float32)
        mid = (line - high).astype(jnp.bfloat16).astype(jnp.float32)
        low = line - high - mid
        part = seq[:8]
        return jnp.where(part == 0, high, jnp.where(part == 1, mid, jnp.where(part == 2, low, 0.0))).astype(jnp.bfloat16)

    def from_lanes(line, h, i):
        return jnp.sum(jnp.where(lane == seq + (h * own + i) * GROUP, line, 0.0), axis=1, keepdims=True)

    def joined(ref, *at):
        return jnp.sum(ref[(*at, pl.ds(data, 8), slice(None))].astype(jnp.float32), axis=0, keepdims=True)

    def pair_copy(k):
        return pltpu.make_async_remote_copy(
            src_ref=pair_so.at[k], dst_ref=pair_ro.at[k], send_sem=ps_sem.at[k], recv_sem=pr_sem.at[k],
            device_id={"dup": partner}, device_id_type=MESH)

    def chip_copies(k):
        return [pltpu.make_async_remote_copy(
            src_ref=chip_so.at[k, s], dst_ref=chip_ro.at[k, there], send_sem=cs_sem.at[s, k], recv_sem=cr_sem.at[there, k],
            device_id={"dup": peer}, device_id_type=MESH) for s, there, peer in ((2, 2, across), (1, 0, ahead), (0, 1, behind))]

    def chip_arrivals(k):
        return [pltpu.make_async_remote_copy(
            src_ref=chip_so.at[k, s], dst_ref=chip_ro.at[k, s], send_sem=cs_sem.at[s, k], recv_sem=cr_sem.at[s, k],
            device_id={"dup": partner}, device_id_type=MESH) for s in range(3)]

    def slab(ref, g, row):
        return ref.at[g % RING][pl.ds(row * PITCH, GROUP), :]

    def place(g):
        at = (g + steps + SPARE) % (steps + SPARE)
        return at // 2, at % 2

    def rows_of(h, i):
        return pl.ds(pl.multiple_of((h * own + i) * GROUP, GROUP), GROUP)

    def give(g):
        (k, h), r = place(g), g + KEEP
        for s in range(4):
            for i in range(own):
                pair_so[k, s, rows_of(h, i), :] = slab(part_o, r, half + s * own + i).astype(jnp.bfloat16)
        for s in range(4):
            pair_so[k, s, pl.ds(data, 8), :] = to_lanes(
                [slab(part_l, r, half + s * own + i) for i in range(own)], h, pair_held.at[s])

    def merge(g):
        (k, h), r = place(g), g + KEEP
        for s in (3, 1, 2, 0):
            logs = []
            line = joined(pair_ro, k, s)
            for i in range(own):
                mine = slab(part_l, r, s * own + i)
                theirs = from_lanes(line, h, i)
                top = jnp.maximum(mine, theirs)
                w_mine, w_theirs = jnp.exp2(mine - top), jnp.exp2(theirs - top)
                total = w_mine + w_theirs
                o = (w_mine * slab(part_o, r, s * own + i)
                     + w_theirs * pair_ro[k, s, rows_of(h, i), :].astype(jnp.float32)) / total
                log_total = top + jnp.log2(total)
                if s == 0:
                    keep_o[r % KEEP, i] = o
                    keep_l[r % KEEP, i] = log_total
                else:
                    chip_so[k, s - 1, rows_of(h, i), :] = o.astype(jnp.bfloat16)
                    logs.append(log_total)
            if s:
                chip_so[k, s - 1, pl.ds(data, 8), :] = to_lanes(logs, h, chip_held.at[s - 1])

    def final(g):
        (k, h), r = place(g), g + KEEP
        to = pl.ds(pl.multiple_of(((g + steps) % steps) * GROUP, GROUP), GROUP)
        lines = [joined(chip_ro, k, s) for s in range(3)]
        for i in range(own):
            logs = [keep_l[r % KEEP, i]] + [from_lanes(line, h, i) for line in lines]
            top = functools.reduce(jnp.maximum, logs)
            weights = [jnp.exp2(log - top) for log in logs]
            total = functools.reduce(jnp.add, weights)
            merged = weights[0] * keep_o[r % KEEP, i]
            for s in range(3):
                merged = merged + weights[s + 1] * chip_ro[k, s, rows_of(h, i), :].astype(jnp.float32)
            o_ref[i, to, :] = (merged / total).astype(jnp.bfloat16)

    def start_all(copies):
        for copy in copies:
            copy.start()

    def arrive_all(copies):
        for copy in copies:
            copy.wait_recv()

    q_arrive(0)
    key_copy(0).wait()
    score(0)
    key_copy(KEYS).start()
    key_copy(1).wait()
    soften(0)
    score(1)
    key_copy(KEYS + 1).start()
    q_pass_far(1)
    q_pass_near(2)

    def step(t, carry):
        c = t // ASK

        @pl.when(t % ASK == 0)
        def _():
            @pl.when(c + 3 < asks)
            def _():
                q_own(c + 3)

            @pl.when(c + 2 < asks)
            def _():
                q_pass_near(c + 2)

            @pl.when(c + 1 < asks)
            def _():
                q_pass_far(c + 1)

            q_arrive(c)

        key_copy(t).wait()
        value_copy(t - 2).wait()

        @pl.when((t >= MERGE) & ((t - MERGE) % 2 == 0))
        def _():
            pair_copy((t - MERGE) // 2).wait_recv()

        @pl.when((t >= FINAL) & ((t + FINAL) % 2 == 0))
        def _():
            arrive_all(chip_arrivals((t - FINAL) // 2))

        final(t - FINAL)
        merge(t - MERGE)
        give(t - GIVE)
        mix(t - 2)
        soften(t - 1)
        score(t)

        @pl.when(t + KEYS < steps)
        def _():
            key_copy(t + KEYS).start()

        @pl.when(t - 2 + VALUES < steps)
        def _():
            value_copy(t - 2 + VALUES).start()

        @pl.when((t >= GIVE) & ((t - GIVE) % 2 == 1))
        def _():
            pair_copy((t - GIVE) // 2).start()

        @pl.when((t >= MERGE) & ((t - MERGE) % 2 == 1))
        def _():
            start_all(chip_copies((t - MERGE) // 2))
        return carry

    lax.fori_loop(2, steps, step, 0)

    value_copy(steps - 2).wait()
    value_copy(steps - 1).wait()
    give(steps - GIVE)
    mix(steps - 2)
    soften(steps - 1)
    pair_copy(steps // 2 - 2).start()
    give(steps - 2)
    mix(steps - 1)
    give(steps - 1)
    pair_copy(steps // 2 - 1).start()

    def last_merge(k, carry):
        pair_copy(k).wait_recv()
        merge(2 * k)
        merge(2 * k + 1)
        start_all(chip_copies(k))
        return carry

    def last_final(k, carry):
        arrive_all(chip_arrivals(k))
        final(2 * k)
        final(2 * k + 1)
        return carry

    lax.fori_loop((steps - MERGE) // 2, steps // 2, last_merge, 0)
    lax.fori_loop((steps - FINAL) // 2, steps // 2, last_final, 0)

    def drain_asks(c, carry):
        for kind in range(5):
            q_copy(kind, c).wait_send()
        return carry

    lax.fori_loop(0, asks, drain_asks, 0)

    def drain(k, carry):
        for copy in [pair_copy(k)] + chip_copies(k):
            copy.wait_send()
        return carry

    lax.fori_loop(0, steps // 2, drain, 0)


def solution(mesh):
    def group_step(q_local, k_span, v_span, len_local):
        num_batch, own, head_dim = q_local.shape
        span = k_span.shape[1]
        steps = num_batch // GROUP
        asks = steps // ASK
        places = (steps + SPARE) // 2
        block = 2 * own * GROUP + 8
        rows = 8 * own
        vmem = functools.partial(pl.BlockSpec, memory_space=pltpu.VMEM)
        hbm = functools.partial(pl.BlockSpec, memory_space=pl.ANY)
        bf16, f32 = jnp.bfloat16, jnp.float32
        dma = pltpu.SemaphoreType.DMA
        out = pl.pallas_call(
            attend,
            out_shape=jax.ShapeDtypeStruct((own, num_batch, head_dim), bf16),
            in_specs=[vmem(), pl.BlockSpec(memory_space=pltpu.SMEM), hbm(), hbm()],
            out_specs=vmem(),
            scratch_shapes=[
                pltpu.VMEM((KEYS, GROUP, span, head_dim), bf16),
                pltpu.VMEM((VALUES, GROUP, span, head_dim), bf16),
                pltpu.VMEM((8, own, num_batch, head_dim), bf16),
                pltpu.VMEM((rows * PITCH, head_dim), f32),
                pltpu.VMEM((rows, span), jnp.int32),
                pltpu.VMEM((GROUP // 2, 2 * rows, span), f32),
                pltpu.VMEM((GROUP // 2, 2 * rows, span), bf16),
                pltpu.VMEM((GROUP // 2, 2 * rows, head_dim), f32),
                pltpu.VMEM((RING, rows * PITCH, head_dim), f32),
                pltpu.VMEM((RING, rows * PITCH, head_dim), f32),
                pltpu.VMEM((places, 4, block, head_dim), bf16),
                pltpu.VMEM((places, 4, block, head_dim), bf16),
                pltpu.VMEM((places, 3, block, head_dim), bf16),
                pltpu.VMEM((places, 3, block, head_dim), bf16),
                pltpu.VMEM((4, 1, head_dim), f32),
                pltpu.VMEM((3, 1, head_dim), f32),
                pltpu.VMEM((KEEP, own, GROUP, head_dim), f32),
                pltpu.VMEM((KEEP, own, GROUP, head_dim), f32),
                dma((KEYS,)), dma((VALUES,)),
                dma((5, asks)), dma((5, asks)),
                dma((steps // 2,)), dma((steps // 2,)),
                dma((3, steps // 2)), dma((3, steps // 2)),
            ],
            compiler_params=pltpu.CompilerParams(
                collective_id=0, has_side_effects=True, vmem_limit_bytes=60 * 1024 * 1024),
            cost_estimate=pl.CostEstimate(
                flops=4 * num_batch * rows * span * head_dim,
                bytes_accessed=4 * num_batch * span * head_dim,
                transcendentals=num_batch * rows * span),
        )(q_local.transpose(1, 0, 2), len_local, k_span, v_span)
        return out.transpose(1, 0, 2)

    return jax.shard_map(
        group_step, mesh=mesh,
        in_specs=(P("kv", "dup", None), P("kv", "dup", None), P("kv", "dup", None), P("kv")),
        out_specs=P("kv", "dup", None), check_vma=False)
```

```python
import functools

import jax
import jax.numpy as jnp
from jax import lax
from jax.experimental import pallas as pl
from jax.experimental.pallas import tpu as pltpu
from jax.sharding import PartitionSpec as P

DRAFT = 4
NEG_BIG = -3e38
LOG2E = 1.4426950408889634
MESH = pl.DeviceIdType.MESH

GROUP = 16
KEYS = 10
VALUES = 11
PITCH = GROUP + 4
RING = 8
KEEP = 16
ASK = 2
GIVE, MERGE, HALVE, FINAL = 2, 4, 7, 10
SPARE = 10


def attend(q_ref, len_ref, k_hbm, v_hbm, o_ref,
           kbuf, vbuf, q_all, q_wide, pos_rel, s_buf, p_buf, i_buf, part_o, part_l,
           pair_so, pair_ro, near_so, near_ro, far_so, far_ro, keep_o, keep_l, last_o, last_l,
           k_sem, v_sem, qs_sem, qr_sem, pair_sem, near_sem, far_sem):
    own, num_batch, head_dim = q_ref.shape
    span = k_hbm.shape[1]
    rows = 8 * own
    half = 4 * own
    data = own * GROUP
    steps = num_batch // GROUP
    asks = steps // ASK
    scale = (head_dim ** -0.5) * LOG2E

    me = lax.axis_index("dup")
    chip = me // 2
    core = me % 2
    turn = (1 - 2 * core) * (1 - 2 * (chip % 2))
    partner = chip * 2 + (1 - core)
    ahead = ((chip + turn + 4) % 4) * 2 + core
    behind = ((chip - turn + 4) % 4) * 2 + core

    def key_copy(g):
        return pltpu.make_async_copy(k_hbm.at[pl.ds(g * GROUP, GROUP)], kbuf.at[g % KEYS], k_sem.at[g % KEYS])

    def value_copy(g):
        return pltpu.make_async_copy(v_hbm.at[pl.ds(g * GROUP, GROUP)], vbuf.at[g % VALUES], v_sem.at[g % VALUES])

    key_copy(0).start()
    key_copy(1).start()

    def start_cache(g, carry):
        key_copy(g + 2).start()
        value_copy(g).start()
        return carry

    lax.fori_loop(0, KEYS - 2, start_cache, 0)
    for g in range(KEYS - 2, VALUES):
        value_copy(g).start()

    barrier = pltpu.get_barrier_semaphore()
    for peer in (partner, ahead, behind):
        pl.semaphore_signal(barrier, inc=1, device_id={"dup": peer}, device_id_type=MESH)

    def q_copy(kind, c):
        part = pl.ds(pl.multiple_of(c * ASK * GROUP, ASK * GROUP), ASK * GROUP)
        src, dst, peer = (
            (q_ref.at[:, part], q_all.at[1, :, part], behind),
            (q_ref.at[:, part], q_all.at[2, :, part], ahead),
            (q_ref.at[:, part], q_all.at[4, :, part], partner),
            (q_all.at[1, :, part], q_all.at[3, :, part], ahead),
            (q_all.at[1:4, :, part], q_all.at[5:8, :, part], partner),
        )[kind]
        return pltpu.make_async_remote_copy(
            src_ref=src, dst_ref=dst, send_sem=qs_sem.at[kind, c], recv_sem=qr_sem.at[kind, c],
            device_id={"dup": peer}, device_id_type=MESH)

    def q_own(c):
        for kind in (0, 1, 2):
            q_copy(kind, c).start()

    def q_pass_near(c):
        q_copy(0, c).wait_recv()
        q_copy(3, c).start()

    def q_pass_far(c):
        q_copy(1, c).wait_recv()
        q_copy(3, c).wait_recv()
        q_copy(4, c).start()

    span_start = me * span
    chip_disp = (0, 4 - turn, 4 + turn, 2)
    pair_disp = (0, 4 + turn, 4 - turn, 2)
    row_id = lax.broadcasted_iota(jnp.int32, (rows, span), 0)
    token = jnp.zeros((rows, span), jnp.int32)
    for h in range(2):
        for s in range(4):
            disp = (chip_disp, pair_disp)[h][s]
            device = ((chip + disp) % 4) * 2 + (core if h == 0 else 1 - core)
            for i in range(own):
                token = jnp.where(row_id == h * half + s * own + i, (own * device + i) % DRAFT, token)
    pos_rel[...] = lax.broadcasted_iota(jnp.int32, (rows, span), 1) + span_start - token

    pl.semaphore_wait(barrier, 3)
    q_own(0)
    q_own(1)
    q_pass_near(0)
    q_pass_far(0)
    q_pass_near(1)
    q_own(2)
    q_own(3)

    def q_arrive(c):
        for kind in (2, 4):
            q_copy(kind, c).wait_recv()

    lane = lax.broadcasted_iota(jnp.int32, (GROUP, head_dim), 1)
    seq = lax.broadcasted_iota(jnp.int32, (GROUP, head_dim), 0)

    def score(g):
        part = pl.ds(pl.multiple_of(g * GROUP, GROUP), GROUP)
        for s in range(8):
            for i in range(own):
                block = q_ref[i, part, :] if s == 0 else q_all[s, i, part, :]
                q_wide[pl.ds((s * own + i) * PITCH, GROUP), :] = block.astype(jnp.float32)
        slot = g % KEYS
        zeros = jnp.zeros((rows, head_dim), jnp.float32)
        for j in range(0, GROUP, 2):
            q0 = q_wide[pl.ds(j, rows, stride=PITCH), :]
            q1 = q_wide[pl.ds(j + 1, rows, stride=PITCH), :]
            q2 = jnp.concatenate([jnp.concatenate([q0, zeros], 1), jnp.concatenate([zeros, q1], 1)], 0).astype(jnp.bfloat16)
            k2 = jnp.concatenate([kbuf[slot, j], kbuf[slot, j + 1]], 1)
            s_buf[j // 2] = lax.dot_general(q2, k2, (((1,), (1,)), ((), ())), preferred_element_type=jnp.float32)

    def soften(g):
        slab_l = part_l.at[g % RING]
        for j in range(0, GROUP, 2):
            s = s_buf[j // 2]
            rel = pos_rel[...]
            base = g * GROUP + j
            s = jnp.concatenate([
                jnp.where(rel <= len_ref[base] - DRAFT, s[:rows], NEG_BIG),
                jnp.where(rel <= len_ref[base + 1] - DRAFT, s[rows:], NEG_BIG)], 0)
            peak = jnp.max(s, axis=1, keepdims=True)
            p = jnp.exp2((s - peak) * scale)
            mass = jnp.sum(p, axis=1, keepdims=True)
            p_buf[j // 2] = p.astype(jnp.bfloat16)
            i_buf[j // 2] = jnp.broadcast_to(1.0 / mass, (2 * rows, head_dim))
            log_mass = jnp.broadcast_to(peak * scale + jnp.log2(mass), (2 * rows, head_dim))
            for n in range(2):
                slab_l[pl.ds(j + n, rows, stride=PITCH), :] = log_mass[n * rows:(n + 1) * rows]

    def mix(g):
        slot = g % VALUES
        slab_o = part_o.at[g % RING]
        for j in range(0, GROUP, 2):
            v2 = jnp.concatenate([vbuf[slot, j], vbuf[slot, j + 1]], 1)
            o2 = jnp.dot(p_buf[j // 2], v2, preferred_element_type=jnp.float32)
            inv = i_buf[j // 2]
            for n in range(2):
                o = o2[n * rows:(n + 1) * rows, n * head_dim:(n + 1) * head_dim] * inv[n * rows:(n + 1) * rows]
                slab_o[pl.ds(j + n, rows, stride=PITCH), :] = o

    def to_lanes(values):
        total = jnp.zeros((GROUP, head_dim), jnp.float32)
        for i, value in enumerate(values):
            total = jnp.where(lane == seq + i * GROUP, value, total)
        line = jnp.sum(total, axis=0, keepdims=True)
        high = line.astype(jnp.bfloat16).astype(jnp.float32)
        mid = (line - high).astype(jnp.bfloat16).astype(jnp.float32)
        low = line - high - mid
        part = seq[:8]
        return jnp.where(part == 0, high, jnp.where(part == 1, mid, jnp.where(part == 2, low, 0.0))).astype(jnp.bfloat16)

    def put(ref, values, logs):
        for i, value in enumerate(values):
            ref[i * GROUP:(i + 1) * GROUP, :] = value.astype(jnp.bfloat16)
        ref[data:data + 8, :] = to_lanes(logs)

    def take(ref):
        line = jnp.sum(ref[data:data + 8, :].astype(jnp.float32), axis=0, keepdims=True)
        return [(ref[i * GROUP:(i + 1) * GROUP, :].astype(jnp.float32),
                 jnp.sum(jnp.where(lane == seq + i * GROUP, line, 0.0), axis=1, keepdims=True)) for i in range(own)]

    def joined(mine, log_mine, theirs, log_theirs):
        top = jnp.maximum(log_mine, log_theirs)
        w_mine, w_theirs = jnp.exp2(log_mine - top), jnp.exp2(log_theirs - top)
        total = w_mine + w_theirs
        return (w_mine * mine + w_theirs * theirs) / total, top + jnp.log2(total)

    def copy_of(src, dst, sems, c, peer):
        return pltpu.make_async_remote_copy(
            src_ref=src.at[c], dst_ref=dst.at[c], send_sem=sems.at[0, c], recv_sem=sems.at[1, c],
            device_id={"dup": peer}, device_id_type=MESH)

    def pair_copy(c):
        return copy_of(pair_so, pair_ro, pair_sem, c, partner)

    def near_copy(c):
        return copy_of(near_so, near_ro, near_sem, c, behind)

    def far_copy(c):
        return copy_of(far_so, far_ro, far_sem, c, ahead)

    def slab(ref, g, row):
        return ref.at[g % RING][pl.ds(row * PITCH, GROUP), :]

    def place(g):
        return (g + steps + SPARE) % (steps + SPARE)

    def give(g):
        c, r = place(g), g + KEEP
        for s in range(4):
            at = [half + s * own + i for i in range(own)]
            put(pair_so.at[c, s], [slab(part_o, r, n) for n in at], [slab(part_l, r, n) for n in at])

    def merge(g):
        c, r = place(g), g + KEEP
        for s in (1, 3, 0, 2):
            both = [joined(slab(part_o, r, s * own + i), slab(part_l, r, s * own + i), *theirs)
                    for i, theirs in enumerate(take(pair_ro.at[c, s]))]
            if s % 2:
                put(near_so.at[c, s // 2], [o for o, _ in both], [log for _, log in both])
            else:
                for i, (o, log) in enumerate(both):
                    keep_o[r % KEEP, s // 2, i] = o
                    keep_l[r % KEEP, s // 2, i] = log

    def halve(g):
        c, r = place(g), g + KEEP
        for s in (1, 0):
            both = [joined(keep_o[r % KEEP, s, i], keep_l[r % KEEP, s, i], *theirs)
                    for i, theirs in enumerate(take(near_ro.at[c, s]))]
            if s:
                put(far_so.at[c], [o for o, _ in both], [log for _, log in both])
            else:
                for i, (o, log) in enumerate(both):
                    last_o[r % KEEP, i] = o
                    last_l[r % KEEP, i] = log

    def final(g):
        c, r = place(g), g + KEEP
        to = pl.ds(pl.multiple_of(((g + steps) % steps) * GROUP, GROUP), GROUP)
        for i, theirs in enumerate(take(far_ro.at[c])):
            o_ref[i, to, :] = joined(last_o[r % KEEP, i], last_l[r % KEEP, i], *theirs)[0].astype(jnp.bfloat16)

    q_arrive(0)
    key_copy(0).wait()
    score(0)
    key_copy(KEYS).start()
    key_copy(1).wait()
    soften(0)
    score(1)
    key_copy(KEYS + 1).start()
    q_pass_far(1)
    q_pass_near(2)

    def step(t, carry):
        c = t // ASK

        @pl.when(t % ASK == 0)
        def _():
            @pl.when(c + 3 < asks)
            def _():
                q_own(c + 3)

            @pl.when(c + 2 < asks)
            def _():
                q_pass_near(c + 2)

            @pl.when(c + 1 < asks)
            def _():
                q_pass_far(c + 1)

            q_arrive(c)

        key_copy(t).wait()
        value_copy(t - 2).wait()

        @pl.when(t >= MERGE)
        def _():
            pair_copy(t - MERGE).wait_recv()

        @pl.when(t >= HALVE)
        def _():
            near_copy(t - HALVE).wait_recv()

        @pl.when(t >= FINAL)
        def _():
            far_copy(t - FINAL).wait_recv()

        final(t - FINAL)
        halve(t - HALVE)
        merge(t - MERGE)
        mix(t - 2)
        give(t - GIVE)
        soften(t - 1)
        score(t)

        pair_copy(t - GIVE).start()

        @pl.when(t >= MERGE)
        def _():
            near_copy(t - MERGE).start()

        @pl.when(t >= HALVE)
        def _():
            far_copy(t - HALVE).start()

        @pl.when(t + KEYS < steps)
        def _():
            key_copy(t + KEYS).start()

        @pl.when(t - 2 + VALUES < steps)
        def _():
            value_copy(t - 2 + VALUES).start()
        return carry

    lax.fori_loop(2, steps, step, 0)

    def late_merge(g):
        pair_copy(g).wait_recv()
        merge(g)
        near_copy(g).start()

    def late_halve(g):
        near_copy(g).wait_recv()
        halve(g)
        far_copy(g).start()

    def late_final(g, carry):
        far_copy(g).wait_recv()
        final(g)
        return carry

    value_copy(steps - 2).wait()
    mix(steps - 2)
    give(steps - 2)
    soften(steps - 1)
    pair_copy(steps - 2).start()
    value_copy(steps - 1).wait()
    mix(steps - 1)
    give(steps - 1)
    pair_copy(steps - 1).start()

    def late_step(j, carry):
        late_merge(steps - MERGE + j)
        late_halve(steps - HALVE + j)
        return carry

    lax.fori_loop(0, MERGE, late_step, 0)
    lax.fori_loop(steps - FINAL, steps - HALVE, late_final, 0)

    def later_step(j, carry):
        late_halve(steps - 3 + j)
        return late_final(steps - HALVE + j, carry)

    lax.fori_loop(0, 3, later_step, 0)
    lax.fori_loop(steps - HALVE + 3, steps, late_final, 0)

    def drain_asks(c, carry):
        for kind in range(5):
            q_copy(kind, c).wait_send()
        return carry

    lax.fori_loop(0, asks, drain_asks, 0)

    def drain(c, carry):
        for copy in (pair_copy(c), near_copy(c), far_copy(c)):
            copy.wait_send()
        return carry

    lax.fori_loop(0, steps, drain, 0)


def solution(mesh):
    def group_step(q_local, k_span, v_span, len_local):
        num_batch, own, head_dim = q_local.shape
        span = k_span.shape[1]
        steps = num_batch // GROUP
        asks = steps // ASK
        places = steps + SPARE
        block = own * GROUP + 8
        rows = 8 * own
        vmem = functools.partial(pl.BlockSpec, memory_space=pltpu.VMEM)
        hbm = functools.partial(pl.BlockSpec, memory_space=pl.ANY)
        bf16, f32 = jnp.bfloat16, jnp.float32
        dma = pltpu.SemaphoreType.DMA
        out = pl.pallas_call(
            attend,
            out_shape=jax.ShapeDtypeStruct((own, num_batch, head_dim), bf16),
            in_specs=[vmem(), pl.BlockSpec(memory_space=pltpu.SMEM), hbm(), hbm()],
            out_specs=vmem(),
            scratch_shapes=[
                pltpu.VMEM((KEYS, GROUP, span, head_dim), bf16),
                pltpu.VMEM((VALUES, GROUP, span, head_dim), bf16),
                pltpu.VMEM((8, own, num_batch, head_dim), bf16),
                pltpu.VMEM((rows * PITCH, head_dim), f32),
                pltpu.VMEM((rows, span), jnp.int32),
                pltpu.VMEM((GROUP // 2, 2 * rows, span), f32),
                pltpu.VMEM((GROUP // 2, 2 * rows, span), bf16),
                pltpu.VMEM((GROUP // 2, 2 * rows, head_dim), f32),
                pltpu.VMEM((RING, rows * PITCH, head_dim), f32),
                pltpu.VMEM((RING, rows * PITCH, head_dim), f32),
                pltpu.VMEM((places, 4, block, head_dim), bf16),
                pltpu.VMEM((places, 4, block, head_dim), bf16),
                pltpu.VMEM((places, 2, block, head_dim), bf16),
                pltpu.VMEM((places, 2, block, head_dim), bf16),
                pltpu.VMEM((places, block, head_dim), bf16),
                pltpu.VMEM((places, block, head_dim), bf16),
                pltpu.VMEM((KEEP, 2, own, GROUP, head_dim), f32),
                pltpu.VMEM((KEEP, 2, own, GROUP, head_dim), f32),
                pltpu.VMEM((KEEP, own, GROUP, head_dim), f32),
                pltpu.VMEM((KEEP, own, GROUP, head_dim), f32),
                dma((KEYS,)), dma((VALUES,)),
                dma((5, asks)), dma((5, asks)),
                dma((2, steps)), dma((2, steps)), dma((2, steps)),
            ],
            compiler_params=pltpu.CompilerParams(
                collective_id=0, has_side_effects=True, vmem_limit_bytes=60 * 1024 * 1024),
            cost_estimate=pl.CostEstimate(
                flops=4 * num_batch * rows * span * head_dim,
                bytes_accessed=4 * num_batch * span * head_dim,
                transcendentals=num_batch * rows * span),
        )(q_local.transpose(1, 0, 2), len_local, k_span, v_span)
        return out.transpose(1, 0, 2)

    return jax.shard_map(
        group_step, mesh=mesh,
        in_specs=(P("kv", "dup", None), P("kv", "dup", None), P("kv", "dup", None), P("kv")),
        out_specs=P("kv", "dup", None), check_vma=False)
```

```python
import functools

import jax
import jax.numpy as jnp
from jax import lax
from jax.experimental import pallas as pl
from jax.experimental.pallas import tpu as pltpu
from jax.sharding import PartitionSpec as P

DRAFT = 4
NEG_BIG = -3e38
LOG2E = 1.4426950408889634
MESH = pl.DeviceIdType.MESH

GROUP = 16
KEYS = 10
VALUES = 11
PITCH = GROUP + 4
RING = 8
KEEP = 16
ASK = 2
GIVE, MERGE, FINAL = 2, 4, 9
SPARE = 9


def attend(q_ref, len_ref, k_hbm, v_hbm, o_ref,
           kbuf, vbuf, q_all, q_wide, pos_rel, s_buf, p_buf, i_buf, part_o, part_l,
           pair_so, pair_ro, chip_so, chip_ro, keep_o, keep_l,
           k_sem, v_sem, qs_sem, qr_sem, pair_sem, chip_sem):
    own, num_batch, head_dim = q_ref.shape
    span = k_hbm.shape[1]
    rows = 8 * own
    half = 4 * own
    data = own * GROUP
    steps = num_batch // GROUP
    asks = steps // ASK
    scale = (head_dim ** -0.5) * LOG2E

    me = lax.axis_index("dup")
    chip = me // 2
    core = me % 2
    turn = (1 - 2 * core) * (1 - 2 * (chip % 2))
    partner = chip * 2 + (1 - core)
    ahead = ((chip + turn + 4) % 4) * 2 + core
    behind = ((chip - turn + 4) % 4) * 2 + core
    across = ((chip + 2) % 4) * 2 + core

    def key_copy(g):
        return pltpu.make_async_copy(k_hbm.at[pl.ds(g * GROUP, GROUP)], kbuf.at[g % KEYS], k_sem.at[g % KEYS])

    def value_copy(g):
        return pltpu.make_async_copy(v_hbm.at[pl.ds(g * GROUP, GROUP)], vbuf.at[g % VALUES], v_sem.at[g % VALUES])

    key_copy(0).start()
    key_copy(1).start()

    def start_cache(g, carry):
        key_copy(g + 2).start()
        value_copy(g).start()
        return carry

    lax.fori_loop(0, KEYS - 2, start_cache, 0)
    for g in range(KEYS - 2, VALUES):
        value_copy(g).start()

    barrier = pltpu.get_barrier_semaphore()
    for peer in (partner, ahead, behind, across):
        pl.semaphore_signal(barrier, inc=1, device_id={"dup": peer}, device_id_type=MESH)

    def q_copy(kind, c, direct=False):
        part = pl.ds(pl.multiple_of(c * ASK * GROUP, ASK * GROUP), ASK * GROUP)
        src, dst, peer = (
            (q_ref.at[:, part], q_all.at[1, :, part], behind),
            (q_ref.at[:, part], q_all.at[2, :, part], ahead),
            (q_ref.at[:, part], q_all.at[4, :, part], partner),
            (q_all.at[1, :, part], q_all.at[3, :, part], ahead),
            (q_all.at[1:4, :, part], q_all.at[5:8, :, part], partner),
        )[kind]
        if direct:
            src, peer = q_ref.at[:, part], across
        return pltpu.make_async_remote_copy(
            src_ref=src, dst_ref=dst, send_sem=qs_sem.at[kind, c], recv_sem=qr_sem.at[kind, c],
            device_id={"dup": peer}, device_id_type=MESH)

    def q_own(c):
        for kind in (0, 1, 2):
            q_copy(kind, c).start()

    def q_pass_near(c):
        q_copy(0, c).wait_recv()
        q_copy(3, c).start()

    def q_pass_far(c):
        q_copy(1, c).wait_recv()
        q_copy(3, c).wait_recv()
        q_copy(4, c).start()

    span_start = me * span
    chip_disp = (0, 4 - turn, 4 + turn, 2)
    pair_disp = (0, 4 + turn, 4 - turn, 2)
    row_id = lax.broadcasted_iota(jnp.int32, (rows, span), 0)
    token = jnp.zeros((rows, span), jnp.int32)
    for h in range(2):
        for s in range(4):
            disp = (chip_disp, pair_disp)[h][s]
            device = ((chip + disp) % 4) * 2 + (core if h == 0 else 1 - core)
            for i in range(own):
                token = jnp.where(row_id == h * half + s * own + i, (own * device + i) % DRAFT, token)
    pos_rel[...] = lax.broadcasted_iota(jnp.int32, (rows, span), 1) + span_start - token

    pl.semaphore_wait(barrier, 4)
    q_copy(3, 0, direct=True).start()
    q_own(0)
    for c in range(1, 6):
        q_own(c)
    q_copy(0, 0).wait_recv()
    q_pass_far(0)
    q_pass_near(1)
    q_pass_near(2)

    def q_arrive(c):
        for kind in (2, 4):
            q_copy(kind, c).wait_recv()

    lane = lax.broadcasted_iota(jnp.int32, (GROUP, head_dim), 1)
    seq = lax.broadcasted_iota(jnp.int32, (GROUP, head_dim), 0)

    def score(g):
        part = pl.ds(pl.multiple_of(g * GROUP, GROUP), GROUP)
        for s in range(8):
            for i in range(own):
                block = q_ref[i, part, :] if s == 0 else q_all[s, i, part, :]
                q_wide[pl.ds((s * own + i) * PITCH, GROUP), :] = block.astype(jnp.float32)
        slot = g % KEYS
        zeros = jnp.zeros((rows, head_dim), jnp.float32)
        for j in range(0, GROUP, 2):
            q0 = q_wide[pl.ds(j, rows, stride=PITCH), :]
            q1 = q_wide[pl.ds(j + 1, rows, stride=PITCH), :]
            q2 = jnp.concatenate([jnp.concatenate([q0, zeros], 1), jnp.concatenate([zeros, q1], 1)], 0).astype(jnp.bfloat16)
            k2 = jnp.concatenate([kbuf[slot, j], kbuf[slot, j + 1]], 1)
            s_buf[j // 2] = lax.dot_general(q2, k2, (((1,), (1,)), ((), ())), preferred_element_type=jnp.float32)

    def soften(g):
        slab_l = part_l.at[g % RING]
        for j in range(0, GROUP, 2):
            s = s_buf[j // 2]
            rel = pos_rel[...]
            base = g * GROUP + j
            s = jnp.concatenate([
                jnp.where(rel <= len_ref[base] - DRAFT, s[:rows], NEG_BIG),
                jnp.where(rel <= len_ref[base + 1] - DRAFT, s[rows:], NEG_BIG)], 0)
            peak = jnp.max(s, axis=1, keepdims=True)
            p = jnp.exp2((s - peak) * scale)
            mass = jnp.sum(p, axis=1, keepdims=True)
            p_buf[j // 2] = p.astype(jnp.bfloat16)
            i_buf[j // 2] = jnp.broadcast_to(1.0 / mass, (2 * rows, head_dim))
            log_mass = jnp.broadcast_to(peak * scale + jnp.log2(mass), (2 * rows, head_dim))
            for n in range(2):
                slab_l[pl.ds(j + n, rows, stride=PITCH), :] = log_mass[n * rows:(n + 1) * rows]

    def mix(g):
        slot = g % VALUES
        slab_o = part_o.at[g % RING]
        for j in range(0, GROUP, 2):
            v2 = jnp.concatenate([vbuf[slot, j], vbuf[slot, j + 1]], 1)
            o2 = jnp.dot(p_buf[j // 2], v2, preferred_element_type=jnp.float32)
            inv = i_buf[j // 2]
            for n in range(2):
                o = o2[n * rows:(n + 1) * rows, n * head_dim:(n + 1) * head_dim] * inv[n * rows:(n + 1) * rows]
                slab_o[pl.ds(j + n, rows, stride=PITCH), :] = o

    def to_lanes(values):
        total = jnp.zeros((GROUP, head_dim), jnp.float32)
        for i, value in enumerate(values):
            total = jnp.where(lane == seq + i * GROUP, value, total)
        line = jnp.sum(total, axis=0, keepdims=True)
        high = line.astype(jnp.bfloat16).astype(jnp.float32)
        mid = (line - high).astype(jnp.bfloat16).astype(jnp.float32)
        low = line - high - mid
        part = seq[:8]
        return jnp.where(part == 0, high, jnp.where(part == 1, mid, jnp.where(part == 2, low, 0.0))).astype(jnp.bfloat16)

    def put(ref, values, logs):
        for i, value in enumerate(values):
            ref[i * GROUP:(i + 1) * GROUP, :] = value.astype(jnp.bfloat16)
        ref[data:data + 8, :] = to_lanes(logs)

    def take(ref):
        line = jnp.sum(ref[data:data + 8, :].astype(jnp.float32), axis=0, keepdims=True)
        return [(ref[i * GROUP:(i + 1) * GROUP, :].astype(jnp.float32),
                 jnp.sum(jnp.where(lane == seq + i * GROUP, line, 0.0), axis=1, keepdims=True)) for i in range(own)]

    def joined(mine, log_mine, theirs, log_theirs):
        top = jnp.maximum(log_mine, log_theirs)
        w_mine, w_theirs = jnp.exp2(log_mine - top), jnp.exp2(log_theirs - top)
        total = w_mine + w_theirs
        return (w_mine * mine + w_theirs * theirs) / total, top + jnp.log2(total)

    def copy_of(src, dst, sems, c, peer):
        return pltpu.make_async_remote_copy(
            src_ref=src.at[c], dst_ref=dst.at[c], send_sem=sems.at[0, c], recv_sem=sems.at[1, c],
            device_id={"dup": peer}, device_id_type=MESH)

    def pair_copy(c):
        return copy_of(pair_so, pair_ro, pair_sem, c, partner)

    def chip_copies(c):
        return [pltpu.make_async_remote_copy(
            src_ref=chip_so.at[c, n], dst_ref=chip_ro.at[c, n], send_sem=chip_sem.at[0, n, c], recv_sem=chip_sem.at[1, n, c],
            device_id={"dup": peer}, device_id_type=MESH) for n, peer in ((2, across), (0, behind), (1, ahead))]

    def chip_start(c):
        for copy in chip_copies(c):
            copy.start()

    def chip_arrive(c):
        for copy in chip_copies(c):
            copy.wait_recv()

    def slab(ref, g, row):
        return ref.at[g % RING][pl.ds(row * PITCH, GROUP), :]

    def place(g):
        return (g + steps + SPARE) % (steps + SPARE)

    def give(g):
        c, r = place(g), g + KEEP
        for s in range(4):
            at = [half + s * own + i for i in range(own)]
            put(pair_so.at[c, s], [slab(part_o, r, n) for n in at], [slab(part_l, r, n) for n in at])

    def merge(g):
        c, r = place(g), g + KEEP
        for s in (3, 1, 2, 0):
            both = [joined(slab(part_o, r, s * own + i), slab(part_l, r, s * own + i), *theirs)
                    for i, theirs in enumerate(take(pair_ro.at[c, s]))]
            if s:
                put(chip_so.at[c, s - 1], [o for o, _ in both], [log for _, log in both])
            else:
                for i, (o, log) in enumerate(both):
                    keep_o[r % KEEP, i] = o
                    keep_l[r % KEEP, i] = log

    def final(g):
        c, r = place(g), g + KEEP
        to = pl.ds(pl.multiple_of(((g + steps) % steps) * GROUP, GROUP), GROUP)
        others = [take(chip_ro.at[c, n]) for n in range(3)]
        for i in range(own):
            logs = [keep_l[r % KEEP, i]] + [other[i][1] for other in others]
            top = functools.reduce(jnp.maximum, logs)
            weights = [jnp.exp2(log - top) for log in logs]
            total = functools.reduce(jnp.add, weights)
            merged = weights[0] * keep_o[r % KEEP, i]
            for weight, other in zip(weights[1:], others):
                merged = merged + weight * other[i][0]
            o_ref[i, to, :] = (merged / total).astype(jnp.bfloat16)

    q_arrive(0)
    key_copy(0).wait()
    score(0)
    key_copy(KEYS).start()
    key_copy(1).wait()
    soften(0)
    score(1)
    key_copy(KEYS + 1).start()
    q_pass_far(1)
    q_pass_near(3)

    def step(t, carry):
        c = t // ASK

        @pl.when(t % ASK == 0)
        def _():
            @pl.when(c + 5 < asks)
            def _():
                q_own(c + 5)

            @pl.when(c + 3 < asks)
            def _():
                q_pass_near(c + 3)

            @pl.when(c + 1 < asks)
            def _():
                q_pass_far(c + 1)

            q_arrive(c)

        key_copy(t).wait()
        value_copy(t - 2).wait()

        @pl.when(t >= MERGE)
        def _():
            pair_copy(t - MERGE).wait_recv()

        @pl.when(t >= FINAL)
        def _():
            chip_arrive(t - FINAL)

        final(t - FINAL)
        merge(t - MERGE)
        mix(t - 2)
        give(t - GIVE)
        soften(t - 1)
        score(t)

        pair_copy(t - GIVE).start()

        @pl.when(t >= MERGE)
        def _():
            chip_start(t - MERGE)

        @pl.when(t + KEYS < steps)
        def _():
            key_copy(t + KEYS).start()

        @pl.when(t - 2 + VALUES < steps)
        def _():
            value_copy(t - 2 + VALUES).start()
        return carry

    lax.fori_loop(2, steps, step, 0)

    def late_merge(g, carry):
        pair_copy(g).wait_recv()
        merge(g)
        chip_start(g)
        return carry

    def late_final(g, carry):
        chip_arrive(g)
        final(g)
        return carry

    value_copy(steps - 2).wait()
    mix(steps - 2)
    give(steps - 2)
    soften(steps - 1)
    pair_copy(steps - 2).start()
    value_copy(steps - 1).wait()
    mix(steps - 1)
    give(steps - 1)
    pair_copy(steps - 1).start()

    lax.fori_loop(steps - MERGE, steps, late_merge, 0)
    lax.fori_loop(steps - FINAL, steps, late_final, 0)

    def drain_asks(c, carry):
        for kind in range(5):
            q_copy(kind, c).wait_send()
        return carry

    lax.fori_loop(0, asks, drain_asks, 0)

    def drain(c, carry):
        for copy in [pair_copy(c)] + chip_copies(c):
            copy.wait_send()
        return carry

    lax.fori_loop(0, steps, drain, 0)


def solution(mesh):
    def group_step(q_local, k_span, v_span, len_local):
        num_batch, own, head_dim = q_local.shape
        span = k_span.shape[1]
        steps = num_batch // GROUP
        asks = steps // ASK
        places = steps + SPARE
        block = own * GROUP + 8
        rows = 8 * own
        vmem = functools.partial(pl.BlockSpec, memory_space=pltpu.VMEM)
        hbm = functools.partial(pl.BlockSpec, memory_space=pl.ANY)
        bf16, f32 = jnp.bfloat16, jnp.float32
        dma = pltpu.SemaphoreType.DMA
        out = pl.pallas_call(
            attend,
            out_shape=jax.ShapeDtypeStruct((own, num_batch, head_dim), bf16),
            in_specs=[vmem(), pl.BlockSpec(memory_space=pltpu.SMEM), hbm(), hbm()],
            out_specs=vmem(),
            scratch_shapes=[
                pltpu.VMEM((KEYS, GROUP, span, head_dim), bf16),
                pltpu.VMEM((VALUES, GROUP, span, head_dim), bf16),
                pltpu.VMEM((8, own, num_batch, head_dim), bf16),
                pltpu.VMEM((rows * PITCH, head_dim), f32),
                pltpu.VMEM((rows, span), jnp.int32),
                pltpu.VMEM((GROUP // 2, 2 * rows, span), f32),
                pltpu.VMEM((GROUP // 2, 2 * rows, span), bf16),
                pltpu.VMEM((GROUP // 2, 2 * rows, head_dim), f32),
                pltpu.VMEM((RING, rows * PITCH, head_dim), f32),
                pltpu.VMEM((RING, rows * PITCH, head_dim), f32),
                pltpu.VMEM((places, 4, block, head_dim), bf16),
                pltpu.VMEM((places, 4, block, head_dim), bf16),
                pltpu.VMEM((places, 3, block, head_dim), bf16),
                pltpu.VMEM((places, 3, block, head_dim), bf16),
                pltpu.VMEM((KEEP, own, GROUP, head_dim), f32),
                pltpu.VMEM((KEEP, own, GROUP, head_dim), f32),
                dma((KEYS,)), dma((VALUES,)),
                dma((5, asks)), dma((5, asks)),
                dma((2, steps)), dma((2, 3, steps)),
            ],
            compiler_params=pltpu.CompilerParams(
                collective_id=0, has_side_effects=True, vmem_limit_bytes=60 * 1024 * 1024),
            cost_estimate=pl.CostEstimate(
                flops=4 * num_batch * rows * span * head_dim,
                bytes_accessed=4 * num_batch * span * head_dim,
                transcendentals=num_batch * rows * span),
        )(q_local.transpose(1, 0, 2), len_local, k_span, v_span)
        return out.transpose(1, 0, 2)

    return jax.shard_map(
        group_step, mesh=mesh,
        in_specs=(P("kv", "dup", None), P("kv", "dup", None), P("kv", "dup", None), P("kv")),
        out_specs=P("kv", "dup", None), check_vma=False)
```

```python
import functools

import jax
import jax.numpy as jnp
from jax import lax
from jax.experimental import pallas as pl
from jax.experimental.pallas import tpu as pltpu
from jax.sharding import PartitionSpec as P

DRAFT = 4
NEG_BIG = -3e38
LOG2E = 1.4426950408889634
MESH = pl.DeviceIdType.MESH

GROUP = 16
KEYS = 10
VALUES = 11
PITCH = GROUP + 4
RING = 8
KEEP = 16
ASK = 2
GIVE, MERGE, FINAL = 2, 4, 9
SPARE = 9


def attend(q_ref, len_ref, k_hbm, v_hbm, o_ref,
           kbuf, vbuf, q_all, q_wide, pos_rel, s_buf, p_buf, i_buf, part_o, part_l,
           pair_so, pair_ro, chip_so, chip_ro, keep_o, keep_l,
           k_sem, v_sem, qs_sem, qr_sem, sent_sem, pair_sem, chip_sem):
    own, num_batch, head_dim = q_ref.shape
    span = k_hbm.shape[1]
    rows = 8 * own
    half = 4 * own
    data = own * GROUP
    steps = num_batch // GROUP
    asks = steps // ASK
    scale = (head_dim ** -0.5) * LOG2E

    me = lax.axis_index("dup")
    chip = me // 2
    core = me % 2
    turn = (1 - 2 * core) * (1 - 2 * (chip % 2))
    partner = chip * 2 + (1 - core)
    ahead = ((chip + turn + 4) % 4) * 2 + core
    behind = ((chip - turn + 4) % 4) * 2 + core
    across = ((chip + 2) % 4) * 2 + core

    def key_copy(g):
        return pltpu.make_async_copy(k_hbm.at[pl.ds(g * GROUP, GROUP)], kbuf.at[g % KEYS], k_sem.at[g % KEYS])

    def value_copy(g):
        return pltpu.make_async_copy(v_hbm.at[pl.ds(g * GROUP, GROUP)], vbuf.at[g % VALUES], v_sem.at[g % VALUES])

    key_copy(0).start()
    key_copy(1).start()

    def start_cache(g, carry):
        key_copy(g + 2).start()
        value_copy(g).start()
        return carry

    lax.fori_loop(0, KEYS - 2, start_cache, 0)
    for g in range(KEYS - 2, VALUES):
        value_copy(g).start()

    barrier = pltpu.get_barrier_semaphore()
    for peer in (partner, ahead, behind, across):
        pl.semaphore_signal(barrier, inc=1, device_id={"dup": peer}, device_id_type=MESH)

    def q_copy(kind, c, direct=False):
        part = pl.ds(pl.multiple_of(c * ASK * GROUP, ASK * GROUP), ASK * GROUP)
        src, dst, peer = (
            (q_ref.at[:, part], q_all.at[1, :, part], behind),
            (q_ref.at[:, part], q_all.at[2, :, part], ahead),
            (q_ref.at[:, part], q_all.at[4, :, part], partner),
            (q_all.at[1, :, part], q_all.at[3, :, part], ahead),
            (q_all.at[1:4, :, part], q_all.at[5:8, :, part], partner),
        )[kind]
        if direct:
            src, peer = q_ref.at[:, part], across
        return pltpu.make_async_remote_copy(
            src_ref=src, dst_ref=dst, send_sem=qs_sem.at[kind], recv_sem=qr_sem.at[kind, c],
            device_id={"dup": peer}, device_id_type=MESH)

    def q_own(c):
        for kind in (0, 1, 2):
            q_copy(kind, c).start()

    def q_pass_near(c):
        q_copy(0, c).wait_recv()
        q_copy(3, c).start()

    def q_pass_far(c):
        q_copy(1, c).wait_recv()
        q_copy(3, c).wait_recv()
        q_copy(4, c).start()

    span_start = me * span
    chip_disp = (0, 4 - turn, 4 + turn, 2)
    pair_disp = (0, 4 + turn, 4 - turn, 2)
    row_id = lax.broadcasted_iota(jnp.int32, (rows, span), 0)
    token = jnp.zeros((rows, span), jnp.int32)
    for h in range(2):
        for s in range(4):
            disp = (chip_disp, pair_disp)[h][s]
            device = ((chip + disp) % 4) * 2 + (core if h == 0 else 1 - core)
            for i in range(own):
                token = jnp.where(row_id == h * half + s * own + i, (own * device + i) % DRAFT, token)
    pos_rel[...] = lax.broadcasted_iota(jnp.int32, (rows, span), 1) + span_start - token

    pl.semaphore_wait(barrier, 4)
    q_copy(3, 0, direct=True).start()
    q_own(0)
    for c in range(1, 6):
        q_own(c)
    q_copy(0, 0).wait_recv()
    q_pass_far(0)
    q_pass_near(1)
    q_pass_near(2)

    def q_arrive(c):
        for kind in (2, 4):
            q_copy(kind, c).wait_recv()

    lane = lax.broadcasted_iota(jnp.int32, (GROUP, head_dim), 1)
    seq = lax.broadcasted_iota(jnp.int32, (GROUP, head_dim), 0)

    def score(g):
        part = pl.ds(pl.multiple_of(g * GROUP, GROUP), GROUP)
        for s in range(8):
            for i in range(own):
                block = q_ref[i, part, :] if s == 0 else q_all[s, i, part, :]
                q_wide[pl.ds((s * own + i) * PITCH, GROUP), :] = block.astype(jnp.float32)
        slot = g % KEYS
        zeros = jnp.zeros((rows, head_dim), jnp.float32)
        for j in range(0, GROUP, 2):
            q0 = q_wide[pl.ds(j, rows, stride=PITCH), :]
            q1 = q_wide[pl.ds(j + 1, rows, stride=PITCH), :]
            q2 = jnp.concatenate([jnp.concatenate([q0, zeros], 1), jnp.concatenate([zeros, q1], 1)], 0).astype(jnp.bfloat16)
            k2 = jnp.concatenate([kbuf[slot, j], kbuf[slot, j + 1]], 1)
            s_buf[j // 2] = lax.dot_general(q2, k2, (((1,), (1,)), ((), ())), preferred_element_type=jnp.float32)

    def soften(g):
        slab_l = part_l.at[g % RING]
        for j in range(0, GROUP, 2):
            s = s_buf[j // 2]
            rel = pos_rel[...]
            base = g * GROUP + j
            s = jnp.concatenate([
                jnp.where(rel <= len_ref[base] - DRAFT, s[:rows], NEG_BIG),
                jnp.where(rel <= len_ref[base + 1] - DRAFT, s[rows:], NEG_BIG)], 0)
            peak = jnp.max(s, axis=1, keepdims=True)
            p = jnp.exp2((s - peak) * scale)
            mass = jnp.sum(p, axis=1, keepdims=True)
            p_buf[j // 2] = p.astype(jnp.bfloat16)
            i_buf[j // 2] = jnp.broadcast_to(1.0 / mass, (2 * rows, head_dim))
            log_mass = jnp.broadcast_to(peak * scale + jnp.log2(mass), (2 * rows, head_dim))
            for n in range(2):
                slab_l[pl.ds(j + n, rows, stride=PITCH), :] = log_mass[n * rows:(n + 1) * rows]

    def mix(g):
        slot = g % VALUES
        slab_o = part_o.at[g % RING]
        for j in range(0, GROUP, 2):
            v2 = jnp.concatenate([vbuf[slot, j], vbuf[slot, j + 1]], 1)
            o2 = jnp.dot(p_buf[j // 2], v2, preferred_element_type=jnp.float32)
            inv = i_buf[j // 2]
            for n in range(2):
                o = o2[n * rows:(n + 1) * rows, n * head_dim:(n + 1) * head_dim] * inv[n * rows:(n + 1) * rows]
                slab_o[pl.ds(j + n, rows, stride=PITCH), :] = o

    def to_lanes(values):
        total = jnp.zeros((GROUP, head_dim), jnp.float32)
        for i, value in enumerate(values):
            total = jnp.where(lane == seq + i * GROUP, value, total)
        line = jnp.sum(total, axis=0, keepdims=True)
        high = line.astype(jnp.bfloat16).astype(jnp.float32)
        mid = (line - high).astype(jnp.bfloat16).astype(jnp.float32)
        low = line - high - mid
        part = seq[:8]
        return jnp.where(part == 0, high, jnp.where(part == 1, mid, jnp.where(part == 2, low, 0.0))).astype(jnp.bfloat16)

    def put(ref, values, logs):
        for i, value in enumerate(values):
            ref[i * GROUP:(i + 1) * GROUP, :] = value.astype(jnp.bfloat16)
        ref[data:data + 8, :] = to_lanes(logs)

    def take(ref):
        line = jnp.sum(ref[data:data + 8, :].astype(jnp.float32), axis=0, keepdims=True)
        return [(ref[i * GROUP:(i + 1) * GROUP, :].astype(jnp.float32),
                 jnp.sum(jnp.where(lane == seq + i * GROUP, line, 0.0), axis=1, keepdims=True)) for i in range(own)]

    def joined(mine, log_mine, theirs, log_theirs):
        top = jnp.maximum(log_mine, log_theirs)
        w_mine, w_theirs = jnp.exp2(log_mine - top), jnp.exp2(log_theirs - top)
        total = w_mine + w_theirs
        return (w_mine * mine + w_theirs * theirs) / total, top + jnp.log2(total)

    def pair_copy(c):
        return pltpu.make_async_remote_copy(
            src_ref=pair_so.at[c], dst_ref=pair_ro.at[c], send_sem=sent_sem.at[0], recv_sem=pair_sem.at[c],
            device_id={"dup": partner}, device_id_type=MESH)

    def chip_start(c):
        for n, peer in ((2, across), (0, behind), (1, ahead)):
            pltpu.make_async_remote_copy(
                src_ref=chip_so.at[c, n], dst_ref=chip_ro.at[c, n], send_sem=sent_sem.at[1], recv_sem=chip_sem.at[c],
                device_id={"dup": peer}, device_id_type=MESH).start()

    def chip_arrive(c):
        pltpu.make_async_remote_copy(
            src_ref=chip_so.at[c], dst_ref=chip_ro.at[c], send_sem=sent_sem.at[1], recv_sem=chip_sem.at[c],
            device_id={"dup": partner}, device_id_type=MESH).wait_recv()

    def slab(ref, g, row):
        return ref.at[g % RING][pl.ds(row * PITCH, GROUP), :]

    def place(g):
        return (g + steps + SPARE) % (steps + SPARE)

    def give(g):
        c, r = place(g), g + KEEP
        for s in range(4):
            at = [half + s * own + i for i in range(own)]
            put(pair_so.at[c, s], [slab(part_o, r, n) for n in at], [slab(part_l, r, n) for n in at])

    def merge(g):
        c, r = place(g), g + KEEP
        for s in (3, 1, 2, 0):
            both = [joined(slab(part_o, r, s * own + i), slab(part_l, r, s * own + i), *theirs)
                    for i, theirs in enumerate(take(pair_ro.at[c, s]))]
            if s:
                put(chip_so.at[c, s - 1], [o for o, _ in both], [log for _, log in both])
            else:
                for i, (o, log) in enumerate(both):
                    keep_o[r % KEEP, i] = o
                    keep_l[r % KEEP, i] = log

    def final(g):
        c, r = place(g), g + KEEP
        to = pl.ds(pl.multiple_of(((g + steps) % steps) * GROUP, GROUP), GROUP)
        others = [take(chip_ro.at[c, n]) for n in range(3)]
        for i in range(own):
            logs = [keep_l[r % KEEP, i]] + [other[i][1] for other in others]
            top = functools.reduce(jnp.maximum, logs)
            weights = [jnp.exp2(log - top) for log in logs]
            total = functools.reduce(jnp.add, weights)
            merged = weights[0] * keep_o[r % KEEP, i]
            for weight, other in zip(weights[1:], others):
                merged = merged + weight * other[i][0]
            o_ref[i, to, :] = (merged / total).astype(jnp.bfloat16)

    q_arrive(0)
    key_copy(0).wait()
    score(0)
    key_copy(KEYS).start()
    key_copy(1).wait()
    soften(0)
    score(1)
    key_copy(KEYS + 1).start()
    q_pass_far(1)
    q_pass_near(3)

    def step(t, carry, full):
        c = t // ASK

        @pl.when(t % ASK == 0)
        def _():
            if not full:
                @pl.when(c + 5 < asks)
                def _():
                    q_own(c + 5)

            @pl.when(c + 3 < asks)
            def _():
                q_pass_near(c + 3)

            @pl.when(c + 1 < asks)
            def _():
                q_pass_far(c + 1)

            q_arrive(c)

        key_copy(t).wait()
        value_copy(t - 2).wait()
        if full:
            pair_copy(t - MERGE).wait_recv()
            chip_arrive(t - FINAL)
            final(t - FINAL)
        else:
            @pl.when(t >= MERGE)
            def _():
                pair_copy(t - MERGE).wait_recv()

        merge(t - MERGE)
        mix(t - 2)
        give(t - GIVE)
        soften(t - 1)
        score(t)

        pair_copy(t - GIVE).start()
        if full:
            chip_start(t - MERGE)
        else:
            @pl.when(t >= MERGE)
            def _():
                chip_start(t - MERGE)

            @pl.when(t + KEYS < steps)
            def _():
                key_copy(t + KEYS).start()

            @pl.when(t - 2 + VALUES < steps)
            def _():
                value_copy(t - 2 + VALUES).start()
        return carry

    lax.fori_loop(2, FINAL, functools.partial(step, full=False), 0)
    lax.fori_loop(FINAL, steps, functools.partial(step, full=True), 0)

    def late_merge(g, carry):
        pair_copy(g).wait_recv()
        merge(g)
        chip_start(g)
        return carry

    def late_final(g, carry):
        chip_arrive(g)
        final(g)
        return carry

    value_copy(steps - 2).wait()
    pair_copy(steps - 4).wait_recv()
    merge(steps - 4)
    mix(steps - 2)
    give(steps - 2)
    soften(steps - 1)
    pair_copy(steps - 2).start()
    chip_start(steps - 4)
    value_copy(steps - 1).wait()
    mix(steps - 1)
    give(steps - 1)
    pair_copy(steps - 1).start()
    lax.fori_loop(steps - MERGE + 1, steps, late_merge, 0)
    lax.fori_loop(steps - FINAL, steps, late_final, 0)

    def drain(src, sem):
        pltpu.make_async_remote_copy(
            src_ref=src, dst_ref=src, send_sem=sem, recv_sem=pair_sem.at[0],
            device_id={"dup": partner}, device_id_type=MESH).wait_send()

    for kind, src in enumerate((q_ref, q_ref, q_ref, q_all.at[1], q_all.at[1:4])):
        drain(src, qs_sem.at[kind])
    drain(pair_so.at[pl.ds(0, steps)], sent_sem.at[0])
    drain(chip_so.at[pl.ds(0, steps)], sent_sem.at[1])


def solution(mesh):
    def group_step(q_local, k_span, v_span, len_local):
        num_batch, own, head_dim = q_local.shape
        span = k_span.shape[1]
        steps = num_batch // GROUP
        asks = steps // ASK
        places = steps + SPARE
        block = own * GROUP + 8
        rows = 8 * own
        vmem = functools.partial(pl.BlockSpec, memory_space=pltpu.VMEM)
        hbm = functools.partial(pl.BlockSpec, memory_space=pl.ANY)
        bf16, f32 = jnp.bfloat16, jnp.float32
        dma = pltpu.SemaphoreType.DMA
        out = pl.pallas_call(
            attend,
            out_shape=jax.ShapeDtypeStruct((own, num_batch, head_dim), bf16),
            in_specs=[vmem(), pl.BlockSpec(memory_space=pltpu.SMEM), hbm(), hbm()],
            out_specs=vmem(),
            scratch_shapes=[
                pltpu.VMEM((KEYS, GROUP, span, head_dim), bf16),
                pltpu.VMEM((VALUES, GROUP, span, head_dim), bf16),
                pltpu.VMEM((8, own, num_batch, head_dim), bf16),
                pltpu.VMEM((rows * PITCH, head_dim), f32),
                pltpu.VMEM((rows, span), jnp.int32),
                pltpu.VMEM((GROUP // 2, 2 * rows, span), f32),
                pltpu.VMEM((GROUP // 2, 2 * rows, span), bf16),
                pltpu.VMEM((GROUP // 2, 2 * rows, head_dim), f32),
                pltpu.VMEM((RING, rows * PITCH, head_dim), f32),
                pltpu.VMEM((RING, rows * PITCH, head_dim), f32),
                pltpu.VMEM((places, 4, block, head_dim), bf16),
                pltpu.VMEM((places, 4, block, head_dim), bf16),
                pltpu.VMEM((places, 3, block, head_dim), bf16),
                pltpu.VMEM((places, 3, block, head_dim), bf16),
                pltpu.VMEM((KEEP, own, GROUP, head_dim), f32),
                pltpu.VMEM((KEEP, own, GROUP, head_dim), f32),
                dma((KEYS,)), dma((VALUES,)),
                dma((5,)), dma((5, asks)),
                dma((2,)), dma((steps,)), dma((steps,)),
            ],
            compiler_params=pltpu.CompilerParams(
                collective_id=0, has_side_effects=True, vmem_limit_bytes=60 * 1024 * 1024),
            cost_estimate=pl.CostEstimate(
                flops=4 * num_batch * rows * span * head_dim,
                bytes_accessed=4 * num_batch * span * head_dim,
                transcendentals=num_batch * rows * span),
        )(q_local.transpose(1, 0, 2), len_local, k_span, v_span)
        return out.transpose(1, 0, 2)

    return jax.shard_map(
        group_step, mesh=mesh,
        in_specs=(P("kv", "dup", None), P("kv", "dup", None), P("kv", "dup", None), P("kv")),
        out_specs=P("kv", "dup", None), check_vma=False)
```

```python
import functools

import jax
import jax.numpy as jnp
from jax import lax
from jax.experimental import pallas as pl
from jax.experimental.pallas import tpu as pltpu
from jax.sharding import PartitionSpec as P

DRAFT = 4
NEG_BIG = -3e38
LOG2E = 1.4426950408889634
MESH = pl.DeviceIdType.MESH

GROUP = 16
KEYS = 10
VALUES = 11
PITCH = GROUP + 4
RING = 8
KEEP = 16
ASK = 2
GIVE, MERGE, FINAL = 2, 4, 9
SPARE = 9


def attend(q_ref, len_ref, k_hbm, v_hbm, o_ref,
           kbuf, vbuf, q_all, q_wide, pos_rel, s_buf, p_buf, i_buf, part_o, part_l,
           pair_so, pair_ro, chip_so, chip_ro, keep_o, keep_l,
           k_sem, v_sem, qs_sem, qr_sem, sent_sem, pair_sem, chip_sem):
    own, num_batch, head_dim = q_ref.shape
    span = k_hbm.shape[1]
    rows = 8 * own
    half = 4 * own
    data = own * GROUP
    steps = num_batch // GROUP
    asks = steps // ASK + 1
    scale = (head_dim ** -0.5) * LOG2E

    me = lax.axis_index("dup")
    chip = me // 2
    core = me % 2
    turn = (1 - 2 * core) * (1 - 2 * (chip % 2))
    partner = chip * 2 + (1 - core)
    ahead = ((chip + turn + 4) % 4) * 2 + core
    behind = ((chip - turn + 4) % 4) * 2 + core
    across = ((chip + 2) % 4) * 2 + core

    def key_copy(g):
        return pltpu.make_async_copy(k_hbm.at[pl.ds(g * GROUP, GROUP)], kbuf.at[g % KEYS], k_sem.at[g % KEYS])

    def value_copy(g):
        return pltpu.make_async_copy(v_hbm.at[pl.ds(g * GROUP, GROUP)], vbuf.at[g % VALUES], v_sem.at[g % VALUES])

    key_copy(0).start()
    key_copy(1).start()

    def start_cache(g, carry):
        key_copy(g + 2).start()
        value_copy(g).start()
        return carry

    lax.fori_loop(0, KEYS - 2, start_cache, 0)
    for g in range(KEYS - 2, VALUES):
        value_copy(g).start()

    barrier = pltpu.get_barrier_semaphore()
    for peer in (partner, ahead, behind, across):
        pl.semaphore_signal(barrier, inc=1, device_id={"dup": peer}, device_id_type=MESH)

    def q_copy(kind, c, direct=False):
        if isinstance(c, int) and c < 2:
            part = pl.ds(c * GROUP, GROUP)
        else:
            part = pl.ds(pl.multiple_of((c - 1) * ASK * GROUP, ASK * GROUP), ASK * GROUP)
        src, dst, peer = (
            (q_ref.at[:, part], q_all.at[1, :, part], behind),
            (q_ref.at[:, part], q_all.at[2, :, part], ahead),
            (q_ref.at[:, part], q_all.at[4, :, part], partner),
            (q_all.at[1, :, part], q_all.at[3, :, part], ahead),
            (q_all.at[1:4, :, part], q_all.at[5:8, :, part], partner),
        )[kind]
        if direct:
            src, peer = q_ref.at[:, part], across
        return pltpu.make_async_remote_copy(
            src_ref=src, dst_ref=dst, send_sem=qs_sem.at[kind], recv_sem=qr_sem.at[kind, c],
            device_id={"dup": peer}, device_id_type=MESH)

    def q_own(c):
        for kind in (0, 1, 2):
            q_copy(kind, c).start()

    def q_pass_near(c):
        q_copy(0, c).wait_recv()
        q_copy(3, c).start()

    def q_pass_far(c):
        q_copy(1, c).wait_recv()
        q_copy(3, c).wait_recv()
        q_copy(4, c).start()

    span_start = me * span
    chip_disp = (0, 4 - turn, 4 + turn, 2)
    pair_disp = (0, 4 + turn, 4 - turn, 2)
    row_id = lax.broadcasted_iota(jnp.int32, (rows, span), 0)
    token = jnp.zeros((rows, span), jnp.int32)
    for h in range(2):
        for s in range(4):
            disp = (chip_disp, pair_disp)[h][s]
            device = ((chip + disp) % 4) * 2 + (core if h == 0 else 1 - core)
            for i in range(own):
                token = jnp.where(row_id == h * half + s * own + i, (own * device + i) % DRAFT, token)
    pos_rel[...] = lax.broadcasted_iota(jnp.int32, (rows, span), 1) + span_start - token

    pl.semaphore_wait(barrier, 4)
    for c in range(2):
        q_copy(3, c, direct=True).start()
        q_own(c)
    for c in range(2, 7):
        q_own(c)
    for c in range(2):
        q_copy(0, c).wait_recv()
        q_pass_far(c)
    q_pass_near(2)
    q_pass_near(3)

    def q_arrive(c):
        for kind in (2, 4):
            q_copy(kind, c).wait_recv()

    lane = lax.broadcasted_iota(jnp.int32, (GROUP, head_dim), 1)
    seq = lax.broadcasted_iota(jnp.int32, (GROUP, head_dim), 0)

    def widen(g):
        part = pl.ds(pl.multiple_of(g * GROUP, GROUP), GROUP)
        for s in range(8):
            for i in range(own):
                block = q_ref[i, part, :] if s == 0 else q_all[s, i, part, :]
                q_wide[pl.ds((s * own + i) * PITCH, GROUP), :] = block.astype(jnp.float32)

    def score(g, n):
        slot, j = g % KEYS, 2 * n
        zeros = jnp.zeros((rows, head_dim), jnp.float32)
        q0 = q_wide[pl.ds(j, rows, stride=PITCH), :]
        q1 = q_wide[pl.ds(j + 1, rows, stride=PITCH), :]
        q2 = jnp.concatenate([jnp.concatenate([q0, zeros], 1), jnp.concatenate([zeros, q1], 1)], 0).astype(jnp.bfloat16)
        k2 = jnp.concatenate([kbuf[slot, j], kbuf[slot, j + 1]], 1)
        s_buf[n] = lax.dot_general(q2, k2, (((1,), (1,)), ((), ())), preferred_element_type=jnp.float32)

    def soften(g, n):
        slab_l = part_l.at[g % RING]
        j = 2 * n
        s = s_buf[n]
        rel = pos_rel[...]
        base = g * GROUP + j
        s = jnp.concatenate([
            jnp.where(rel <= len_ref[base] - DRAFT, s[:rows], NEG_BIG),
            jnp.where(rel <= len_ref[base + 1] - DRAFT, s[rows:], NEG_BIG)], 0)
        peak = jnp.max(s, axis=1, keepdims=True)
        p = jnp.exp2((s - peak) * scale)
        mass = jnp.sum(p, axis=1, keepdims=True)
        p_buf[n] = p.astype(jnp.bfloat16)
        i_buf[n] = jnp.broadcast_to(1.0 / mass, (2 * rows, head_dim))
        log_mass = jnp.broadcast_to(peak * scale + jnp.log2(mass), (2 * rows, head_dim))
        for m in range(2):
            slab_l[pl.ds(j + m, rows, stride=PITCH), :] = log_mass[m * rows:(m + 1) * rows]

    def mix(g, n):
        slot, j = g % VALUES, 2 * n
        slab_o = part_o.at[g % RING]
        v2 = jnp.concatenate([vbuf[slot, j], vbuf[slot, j + 1]], 1)
        o2 = jnp.dot(p_buf[n], v2, preferred_element_type=jnp.float32)
        inv = i_buf[n]
        for m in range(2):
            o = o2[m * rows:(m + 1) * rows, m * head_dim:(m + 1) * head_dim] * inv[m * rows:(m + 1) * rows]
            slab_o[pl.ds(j + m, rows, stride=PITCH), :] = o

    pairs = range(GROUP // 2)

    def to_lanes(values):
        total = jnp.zeros((GROUP, head_dim), jnp.float32)
        for i, value in enumerate(values):
            total = jnp.where(lane == seq + i * GROUP, value, total)
        line = jnp.sum(total, axis=0, keepdims=True)
        high = line.astype(jnp.bfloat16).astype(jnp.float32)
        mid = (line - high).astype(jnp.bfloat16).astype(jnp.float32)
        low = line - high - mid
        part = seq[:8]
        return jnp.where(part == 0, high, jnp.where(part == 1, mid, jnp.where(part == 2, low, 0.0))).astype(jnp.bfloat16)

    def put(ref, values, logs):
        for i, value in enumerate(values):
            ref[i * GROUP:(i + 1) * GROUP, :] = value.astype(jnp.bfloat16)
        ref[data:data + 8, :] = to_lanes(logs)

    def take(ref):
        line = jnp.sum(ref[data:data + 8, :].astype(jnp.float32), axis=0, keepdims=True)
        return [(ref[i * GROUP:(i + 1) * GROUP, :].astype(jnp.float32),
                 jnp.sum(jnp.where(lane == seq + i * GROUP, line, 0.0), axis=1, keepdims=True)) for i in range(own)]

    def joined(mine, log_mine, theirs, log_theirs):
        top = jnp.maximum(log_mine, log_theirs)
        w_mine, w_theirs = jnp.exp2(log_mine - top), jnp.exp2(log_theirs - top)
        total = w_mine + w_theirs
        return (w_mine * mine + w_theirs * theirs) / total, top + jnp.log2(total)

    def pair_copy(c):
        return pltpu.make_async_remote_copy(
            src_ref=pair_so.at[c], dst_ref=pair_ro.at[c], send_sem=sent_sem.at[0], recv_sem=pair_sem.at[c],
            device_id={"dup": partner}, device_id_type=MESH)

    def chip_start(c):
        for n, peer in ((2, across), (0, behind), (1, ahead)):
            pltpu.make_async_remote_copy(
                src_ref=chip_so.at[c, n], dst_ref=chip_ro.at[c, n], send_sem=sent_sem.at[1], recv_sem=chip_sem.at[c],
                device_id={"dup": peer}, device_id_type=MESH).start()

    def chip_arrive(c):
        pltpu.make_async_remote_copy(
            src_ref=chip_so.at[c], dst_ref=chip_ro.at[c], send_sem=sent_sem.at[1], recv_sem=chip_sem.at[c],
            device_id={"dup": partner}, device_id_type=MESH).wait_recv()

    def slab(ref, g, row):
        return ref.at[g % RING][pl.ds(row * PITCH, GROUP), :]

    def place(g):
        return (g + steps + SPARE) % (steps + SPARE)

    def give(g):
        c, r = place(g), g + KEEP
        for s in range(4):
            at = [half + s * own + i for i in range(own)]
            put(pair_so.at[c, s], [slab(part_o, r, n) for n in at], [slab(part_l, r, n) for n in at])

    def merge(g):
        c, r = place(g), g + KEEP
        for s in (3, 1, 2, 0):
            both = [joined(slab(part_o, r, s * own + i), slab(part_l, r, s * own + i), *theirs)
                    for i, theirs in enumerate(take(pair_ro.at[c, s]))]
            if s:
                put(chip_so.at[c, s - 1], [o for o, _ in both], [log for _, log in both])
            else:
                for i, (o, log) in enumerate(both):
                    keep_o[r % KEEP, i] = o
                    keep_l[r % KEEP, i] = log

    def final(g):
        c, r = place(g), g + KEEP
        to = pl.ds(pl.multiple_of(((g + steps) % steps) * GROUP, GROUP), GROUP)
        others = [take(chip_ro.at[c, n]) for n in range(3)]
        for i in range(own):
            logs = [keep_l[r % KEEP, i]] + [other[i][1] for other in others]
            top = functools.reduce(jnp.maximum, logs)
            weights = [jnp.exp2(log - top) for log in logs]
            total = functools.reduce(jnp.add, weights)
            merged = weights[0] * keep_o[r % KEEP, i]
            for weight, other in zip(weights[1:], others):
                merged = merged + weight * other[i][0]
            o_ref[i, to, :] = (merged / total).astype(jnp.bfloat16)

    q_arrive(0)
    key_copy(0).wait()
    widen(0)
    for n in pairs:
        score(0, n)
    key_copy(KEYS).start()
    key_copy(1).wait()
    q_arrive(1)
    widen(1)
    for n in pairs:
        soften(0, n)
        score(1, n)
    key_copy(KEYS + 1).start()
    q_pass_far(2)
    q_pass_near(4)

    def step(t, carry, full):
        c = t // ASK + 1

        @pl.when(t % ASK == 0)
        def _():
            if not full:
                @pl.when(c + 5 < asks)
                def _():
                    q_own(c + 5)

            @pl.when(c + 3 < asks)
            def _():
                q_pass_near(c + 3)

            @pl.when(c + 1 < asks)
            def _():
                q_pass_far(c + 1)

            q_arrive(c)

        key_copy(t).wait()
        value_copy(t - 2).wait()
        if full:
            pair_copy(t - MERGE).wait_recv()
            chip_arrive(t - FINAL)
            final(t - FINAL)
        else:
            @pl.when(t >= MERGE)
            def _():
                pair_copy(t - MERGE).wait_recv()

        widen(t)
        for n in pairs:
            mix(t - 2, n)
            soften(t - 1, n)
            score(t, n)
        give(t - GIVE)
        merge(t - MERGE)

        pair_copy(t - GIVE).start()
        if full:
            chip_start(t - MERGE)
        else:
            @pl.when(t >= MERGE)
            def _():
                chip_start(t - MERGE)

            @pl.when(t + KEYS < steps)
            def _():
                key_copy(t + KEYS).start()

            @pl.when(t - 2 + VALUES < steps)
            def _():
                value_copy(t - 2 + VALUES).start()
        return carry

    lax.fori_loop(2, FINAL, functools.partial(step, full=False), 0)
    lax.fori_loop(FINAL, steps, functools.partial(step, full=True), 0)

    def late_merge(g, carry):
        pair_copy(g).wait_recv()
        merge(g)
        chip_start(g)
        return carry

    def late_final(g, carry):
        chip_arrive(g)
        final(g)
        return carry

    value_copy(steps - 2).wait()
    pair_copy(steps - 4).wait_recv()
    merge(steps - 4)
    for n in pairs:
        mix(steps - 2, n)
        soften(steps - 1, n)
    give(steps - 2)
    pair_copy(steps - 2).start()
    chip_start(steps - 4)
    value_copy(steps - 1).wait()
    for n in pairs:
        mix(steps - 1, n)
    give(steps - 1)
    pair_copy(steps - 1).start()
    lax.fori_loop(steps - MERGE + 1, steps, late_merge, 0)
    lax.fori_loop(steps - FINAL, steps, late_final, 0)

    def drain(src, sem):
        pltpu.make_async_remote_copy(
            src_ref=src, dst_ref=src, send_sem=sem, recv_sem=pair_sem.at[0],
            device_id={"dup": partner}, device_id_type=MESH).wait_send()

    for kind, src in enumerate((q_ref, q_ref, q_ref, q_all.at[1], q_all.at[1:4])):
        drain(src, qs_sem.at[kind])
    drain(pair_so.at[pl.ds(0, steps)], sent_sem.at[0])
    drain(chip_so.at[pl.ds(0, steps)], sent_sem.at[1])


def solution(mesh):
    def group_step(q_local, k_span, v_span, len_local):
        num_batch, own, head_dim = q_local.shape
        span = k_span.shape[1]
        steps = num_batch // GROUP
        asks = steps // ASK + 1
        places = steps + SPARE
        block = own * GROUP + 8
        rows = 8 * own
        vmem = functools.partial(pl.BlockSpec, memory_space=pltpu.VMEM)
        hbm = functools.partial(pl.BlockSpec, memory_space=pl.ANY)
        bf16, f32 = jnp.bfloat16, jnp.float32
        dma = pltpu.SemaphoreType.DMA
        out = pl.pallas_call(
            attend,
            out_shape=jax.ShapeDtypeStruct((own, num_batch, head_dim), bf16),
            in_specs=[vmem(), pl.BlockSpec(memory_space=pltpu.SMEM), hbm(), hbm()],
            out_specs=vmem(),
            scratch_shapes=[
                pltpu.VMEM((KEYS, GROUP, span, head_dim), bf16),
                pltpu.VMEM((VALUES, GROUP, span, head_dim), bf16),
                pltpu.VMEM((8, own, num_batch, head_dim), bf16),
                pltpu.VMEM((rows * PITCH, head_dim), f32),
                pltpu.VMEM((rows, span), jnp.int32),
                pltpu.VMEM((GROUP // 2, 2 * rows, span), f32),
                pltpu.VMEM((GROUP // 2, 2 * rows, span), bf16),
                pltpu.VMEM((GROUP // 2, 2 * rows, head_dim), f32),
                pltpu.VMEM((RING, rows * PITCH, head_dim), f32),
                pltpu.VMEM((RING, rows * PITCH, head_dim), f32),
                pltpu.VMEM((places, 4, block, head_dim), bf16),
                pltpu.VMEM((places, 4, block, head_dim), bf16),
                pltpu.VMEM((places, 3, block, head_dim), bf16),
                pltpu.VMEM((places, 3, block, head_dim), bf16),
                pltpu.VMEM((KEEP, own, GROUP, head_dim), f32),
                pltpu.VMEM((KEEP, own, GROUP, head_dim), f32),
                dma((KEYS,)), dma((VALUES,)),
                dma((5,)), dma((5, asks)),
                dma((2,)), dma((steps,)), dma((steps,)),
            ],
            compiler_params=pltpu.CompilerParams(
                collective_id=0, has_side_effects=True, vmem_limit_bytes=60 * 1024 * 1024),
            cost_estimate=pl.CostEstimate(
                flops=4 * num_batch * rows * span * head_dim,
                bytes_accessed=4 * num_batch * span * head_dim,
                transcendentals=num_batch * rows * span),
        )(q_local.transpose(1, 0, 2), len_local, k_span, v_span)
        return out.transpose(1, 0, 2)

    return jax.shard_map(
        group_step, mesh=mesh,
        in_specs=(P("kv", "dup", None), P("kv", "dup", None), P("kv", "dup", None), P("kv")),
        out_specs=P("kv", "dup", None), check_vma=False)
```

```python
import functools

import jax
import jax.numpy as jnp
from jax import lax
from jax.experimental import pallas as pl
from jax.experimental.pallas import tpu as pltpu
from jax.sharding import PartitionSpec as P

DRAFT = 4
NEG_BIG = -3e38
LOG2E = 1.4426950408889634
MESH = pl.DeviceIdType.MESH

GROUP = 16
KEYS = 10
VALUES = 11
PITCH = GROUP + 4
RING = 8
KEEP = 16
ASK = 2
GIVE, MERGE, FINAL = 2, 4, 9
SPARE = 9


def attend(q_ref, len_ref, k_hbm, v_hbm, o_ref,
           kbuf, vbuf, q_all, q_wide, pos_rel, s_buf, p_buf, i_buf, part_o, part_l,
           pair_so, pair_ro, chip_so, chip_ro, keep_o, keep_l,
           k_sem, v_sem, qs_sem, qr_sem, sent_sem, pair_sem, chip_sem):
    own, num_batch, head_dim = q_ref.shape
    span = k_hbm.shape[1]
    rows = 8 * own
    half = 4 * own
    data = own * GROUP
    steps = num_batch // GROUP
    asks = steps // ASK + 1
    scale = (head_dim ** -0.5) * LOG2E

    me = lax.axis_index("dup")
    chip = me // 2
    core = me % 2
    turn = (1 - 2 * core) * (1 - 2 * (chip % 2))
    partner = chip * 2 + (1 - core)
    ahead = ((chip + turn + 4) % 4) * 2 + core
    behind = ((chip - turn + 4) % 4) * 2 + core
    across = ((chip + 2) % 4) * 2 + core

    def key_copy(g):
        return pltpu.make_async_copy(k_hbm.at[pl.ds(g * GROUP, GROUP)], kbuf.at[g % KEYS], k_sem.at[g % KEYS])

    def value_copy(g):
        return pltpu.make_async_copy(v_hbm.at[pl.ds(g * GROUP, GROUP)], vbuf.at[g % VALUES], v_sem.at[g % VALUES])

    key_copy(0).start()
    key_copy(1).start()

    def start_cache(g, carry):
        key_copy(g + 2).start()
        value_copy(g).start()
        return carry

    lax.fori_loop(0, KEYS - 2, start_cache, 0)
    for g in range(KEYS - 2, VALUES):
        value_copy(g).start()

    barrier = pltpu.get_barrier_semaphore()
    for peer in (partner, ahead, behind, across):
        pl.semaphore_signal(barrier, inc=1, device_id={"dup": peer}, device_id_type=MESH)

    def q_copy(kind, c, direct=False):
        if isinstance(c, int) and c < 2:
            part = pl.ds(c * GROUP, GROUP)
        else:
            part = pl.ds(pl.multiple_of((c - 1) * ASK * GROUP, ASK * GROUP), ASK * GROUP)
        src, dst, peer = (
            (q_ref.at[:, part], q_all.at[1, :, part], behind),
            (q_ref.at[:, part], q_all.at[2, :, part], ahead),
            (q_ref.at[:, part], q_all.at[4, :, part], partner),
            (q_all.at[1, :, part], q_all.at[3, :, part], ahead),
            (q_all.at[1:4, :, part], q_all.at[5:8, :, part], partner),
        )[kind]
        if direct:
            src, peer = q_ref.at[:, part], across
        return pltpu.make_async_remote_copy(
            src_ref=src, dst_ref=dst, send_sem=qs_sem.at[kind], recv_sem=qr_sem.at[kind, c],
            device_id={"dup": peer}, device_id_type=MESH)

    def q_own(c):
        for kind in (0, 1, 2):
            q_copy(kind, c).start()

    def q_pass_near(c):
        q_copy(0, c).wait_recv()
        q_copy(3, c).start()

    def q_pass_far(c):
        q_copy(1, c).wait_recv()
        q_copy(3, c).wait_recv()
        q_copy(4, c).start()

    span_start = me * span
    chip_disp = (0, 4 - turn, 4 + turn, 2)
    pair_disp = (0, 4 + turn, 4 - turn, 2)
    row_id = lax.broadcasted_iota(jnp.int32, (rows, span), 0)
    token = jnp.zeros((rows, span), jnp.int32)
    for h in range(2):
        for s in range(4):
            disp = (chip_disp, pair_disp)[h][s]
            device = ((chip + disp) % 4) * 2 + (core if h == 0 else 1 - core)
            for i in range(own):
                token = jnp.where(row_id == h * half + s * own + i, (own * device + i) % DRAFT, token)
    pos_rel[...] = lax.broadcasted_iota(jnp.int32, (rows, span), 1) + span_start - token

    pl.semaphore_wait(barrier, 4)
    for c in range(2):
        q_copy(3, c, direct=True).start()
        q_own(c)
    q_own(2)
    q_pass_near(2)
    q_own(3)
    for c in range(2):
        q_copy(0, c).wait_recv()
        q_pass_far(c)
    q_own(4)
    q_pass_near(3)
    q_own(5)

    def q_arrive(c):
        for kind in (2, 4):
            q_copy(kind, c).wait_recv()

    lane = lax.broadcasted_iota(jnp.int32, (GROUP, head_dim), 1)
    seq = lax.broadcasted_iota(jnp.int32, (GROUP, head_dim), 0)

    def widen(g):
        part = pl.ds(pl.multiple_of(g * GROUP, GROUP), GROUP)
        for s in range(8):
            for i in range(own):
                block = q_ref[i, part, :] if s == 0 else q_all[s, i, part, :]
                q_wide[pl.ds((s * own + i) * PITCH, GROUP), :] = block.astype(jnp.float32)

    def score(g, n):
        slot, j = g % KEYS, 2 * n
        zeros = jnp.zeros((rows, head_dim), jnp.float32)
        q0 = q_wide[pl.ds(j, rows, stride=PITCH), :]
        q1 = q_wide[pl.ds(j + 1, rows, stride=PITCH), :]
        q2 = jnp.concatenate([jnp.concatenate([q0, zeros], 1), jnp.concatenate([zeros, q1], 1)], 0).astype(jnp.bfloat16)
        k2 = jnp.concatenate([kbuf[slot, j], kbuf[slot, j + 1]], 1)
        s_buf[n] = lax.dot_general(q2, k2, (((1,), (1,)), ((), ())), preferred_element_type=jnp.float32)

    def soften(g, n):
        slab_l = part_l.at[g % RING]
        j = 2 * n
        s = s_buf[n]
        rel = pos_rel[...]
        base = g * GROUP + j
        s = jnp.concatenate([
            jnp.where(rel <= len_ref[base] - DRAFT, s[:rows], NEG_BIG),
            jnp.where(rel <= len_ref[base + 1] - DRAFT, s[rows:], NEG_BIG)], 0)
        peak = jnp.max(s, axis=1, keepdims=True)
        p = jnp.exp2((s - peak) * scale)
        mass = jnp.sum(p, axis=1, keepdims=True)
        p_buf[n] = p.astype(jnp.bfloat16)
        i_buf[n] = jnp.broadcast_to(1.0 / mass, (2 * rows, head_dim))
        log_mass = jnp.broadcast_to(peak * scale + jnp.log2(mass), (2 * rows, head_dim))
        for m in range(2):
            slab_l[pl.ds(j + m, rows, stride=PITCH), :] = log_mass[m * rows:(m + 1) * rows]

    def mix(g, n):
        slot, j = g % VALUES, 2 * n
        slab_o = part_o.at[g % RING]
        v2 = jnp.concatenate([vbuf[slot, j], vbuf[slot, j + 1]], 1)
        o2 = jnp.dot(p_buf[n], v2, preferred_element_type=jnp.float32)
        inv = i_buf[n]
        for m in range(2):
            o = o2[m * rows:(m + 1) * rows, m * head_dim:(m + 1) * head_dim] * inv[m * rows:(m + 1) * rows]
            slab_o[pl.ds(j + m, rows, stride=PITCH), :] = o

    pairs = range(GROUP // 2)

    def to_lanes(values):
        total = jnp.zeros((GROUP, head_dim), jnp.float32)
        for i, value in enumerate(values):
            total = jnp.where(lane == seq + i * GROUP, value, total)
        line = jnp.sum(total, axis=0, keepdims=True)
        high = line.astype(jnp.bfloat16).astype(jnp.float32)
        mid = (line - high).astype(jnp.bfloat16).astype(jnp.float32)
        low = line - high - mid
        part = seq[:8]
        return jnp.where(part == 0, high, jnp.where(part == 1, mid, jnp.where(part == 2, low, 0.0))).astype(jnp.bfloat16)

    def put(ref, values, logs):
        for i, value in enumerate(values):
            ref[i * GROUP:(i + 1) * GROUP, :] = value.astype(jnp.bfloat16)
        ref[data:data + 8, :] = to_lanes(logs)

    def take(ref):
        line = jnp.sum(ref[data:data + 8, :].astype(jnp.float32), axis=0, keepdims=True)
        return [(ref[i * GROUP:(i + 1) * GROUP, :].astype(jnp.float32),
                 jnp.sum(jnp.where(lane == seq + i * GROUP, line, 0.0), axis=1, keepdims=True)) for i in range(own)]

    def joined(mine, log_mine, theirs, log_theirs):
        top = jnp.maximum(log_mine, log_theirs)
        w_mine, w_theirs = jnp.exp2(log_mine - top), jnp.exp2(log_theirs - top)
        total = w_mine + w_theirs
        return (w_mine * mine + w_theirs * theirs) / total, top + jnp.log2(total)

    def pair_copy(c):
        return pltpu.make_async_remote_copy(
            src_ref=pair_so.at[c], dst_ref=pair_ro.at[c], send_sem=sent_sem.at[0], recv_sem=pair_sem.at[c],
            device_id={"dup": partner}, device_id_type=MESH)

    def chip_start(c):
        for n, peer in ((2, across), (0, behind), (1, ahead)):
            pltpu.make_async_remote_copy(
                src_ref=chip_so.at[c, n], dst_ref=chip_ro.at[c, n], send_sem=sent_sem.at[1], recv_sem=chip_sem.at[c],
                device_id={"dup": peer}, device_id_type=MESH).start()

    def chip_arrive(c):
        pltpu.make_async_remote_copy(
            src_ref=chip_so.at[c], dst_ref=chip_ro.at[c], send_sem=sent_sem.at[1], recv_sem=chip_sem.at[c],
            device_id={"dup": partner}, device_id_type=MESH).wait_recv()

    def slab(ref, g, row):
        return ref.at[g % RING][pl.ds(row * PITCH, GROUP), :]

    def place(g):
        return (g + steps + SPARE) % (steps + SPARE)

    def give(g):
        c, r = place(g), g + KEEP
        for s in range(4):
            at = [half + s * own + i for i in range(own)]
            put(pair_so.at[c, s], [slab(part_o, r, n) for n in at], [slab(part_l, r, n) for n in at])

    def merge(g):
        c, r = place(g), g + KEEP
        for s in (3, 1, 2, 0):
            both = [joined(slab(part_o, r, s * own + i), slab(part_l, r, s * own + i), *theirs)
                    for i, theirs in enumerate(take(pair_ro.at[c, s]))]
            if s:
                put(chip_so.at[c, s - 1], [o for o, _ in both], [log for _, log in both])
            else:
                for i, (o, log) in enumerate(both):
                    keep_o[r % KEEP, i] = o
                    keep_l[r % KEEP, i] = log

    def final(g):
        c, r = place(g), g + KEEP
        to = pl.ds(pl.multiple_of(((g + steps) % steps) * GROUP, GROUP), GROUP)
        others = [take(chip_ro.at[c, n]) for n in range(3)]
        for i in range(own):
            logs = [keep_l[r % KEEP, i]] + [other[i][1] for other in others]
            top = functools.reduce(jnp.maximum, logs)
            weights = [jnp.exp2(log - top) for log in logs]
            total = functools.reduce(jnp.add, weights)
            merged = weights[0] * keep_o[r % KEEP, i]
            for weight, other in zip(weights[1:], others):
                merged = merged + weight * other[i][0]
            o_ref[i, to, :] = (merged / total).astype(jnp.bfloat16)

    q_arrive(0)
    key_copy(0).wait()
    widen(0)
    for n in pairs:
        score(0, n)
    key_copy(KEYS).start()
    q_pass_far(2)
    key_copy(1).wait()
    q_arrive(1)
    widen(1)
    for n in pairs:
        soften(0, n)
        score(1, n)
    key_copy(KEYS + 1).start()
    q_own(6)
    q_pass_near(4)

    def step(t, carry, full):
        c = t // ASK + 1

        @pl.when(t % ASK == 0)
        def _():
            if not full:
                @pl.when(c + 5 < asks)
                def _():
                    q_own(c + 5)

            @pl.when(c + 3 < asks)
            def _():
                q_pass_near(c + 3)

            @pl.when(c + 1 < asks)
            def _():
                q_pass_far(c + 1)

            q_arrive(c)

        key_copy(t).wait()
        value_copy(t - 2).wait()
        if full:
            pair_copy(t - MERGE).wait_recv()
            chip_arrive(t - FINAL)
            final(t - FINAL)
        else:
            @pl.when(t >= MERGE)
            def _():
                pair_copy(t - MERGE).wait_recv()

        widen(t)
        for n in pairs:
            mix(t - 2, n)
            soften(t - 1, n)
            score(t, n)
        give(t - GIVE)
        merge(t - MERGE)

        pair_copy(t - GIVE).start()
        if full:
            chip_start(t - MERGE)
        else:
            @pl.when(t >= MERGE)
            def _():
                chip_start(t - MERGE)

            @pl.when(t + KEYS < steps)
            def _():
                key_copy(t + KEYS).start()

            @pl.when(t - 2 + VALUES < steps)
            def _():
                value_copy(t - 2 + VALUES).start()
        return carry

    lax.fori_loop(2, FINAL, functools.partial(step, full=False), 0)
    lax.fori_loop(FINAL, steps, functools.partial(step, full=True), 0)

    def late_merge(g, carry):
        pair_copy(g).wait_recv()
        merge(g)
        chip_start(g)
        return carry

    def late_final(g, carry):
        chip_arrive(g)
        final(g)
        return carry

    value_copy(steps - 2).wait()
    pair_copy(steps - 4).wait_recv()
    merge(steps - 4)
    for n in pairs:
        mix(steps - 2, n)
        soften(steps - 1, n)
    give(steps - 2)
    pair_copy(steps - 2).start()
    chip_start(steps - 4)
    value_copy(steps - 1).wait()
    for n in pairs:
        mix(steps - 1, n)
    give(steps - 1)
    pair_copy(steps - 1).start()
    lax.fori_loop(steps - MERGE + 1, steps, late_merge, 0)
    lax.fori_loop(steps - FINAL, steps, late_final, 0)

    def drain(src, sem):
        pltpu.make_async_remote_copy(
            src_ref=src, dst_ref=src, send_sem=sem, recv_sem=pair_sem.at[0],
            device_id={"dup": partner}, device_id_type=MESH).wait_send()

    for kind, src in enumerate((q_ref, q_ref, q_ref, q_all.at[1], q_all.at[1:4])):
        drain(src, qs_sem.at[kind])
    drain(pair_so.at[pl.ds(0, steps)], sent_sem.at[0])
    drain(chip_so.at[pl.ds(0, steps)], sent_sem.at[1])


def solution(mesh):
    def group_step(q_local, k_span, v_span, len_local):
        num_batch, own, head_dim = q_local.shape
        span = k_span.shape[1]
        steps = num_batch // GROUP
        asks = steps // ASK + 1
        places = steps + SPARE
        block = own * GROUP + 8
        rows = 8 * own
        vmem = functools.partial(pl.BlockSpec, memory_space=pltpu.VMEM)
        hbm = functools.partial(pl.BlockSpec, memory_space=pl.ANY)
        bf16, f32 = jnp.bfloat16, jnp.float32
        dma = pltpu.SemaphoreType.DMA
        out = pl.pallas_call(
            attend,
            out_shape=jax.ShapeDtypeStruct((own, num_batch, head_dim), bf16),
            in_specs=[vmem(), pl.BlockSpec(memory_space=pltpu.SMEM), hbm(), hbm()],
            out_specs=vmem(),
            scratch_shapes=[
                pltpu.VMEM((KEYS, GROUP, span, head_dim), bf16),
                pltpu.VMEM((VALUES, GROUP, span, head_dim), bf16),
                pltpu.VMEM((8, own, num_batch, head_dim), bf16),
                pltpu.VMEM((rows * PITCH, head_dim), f32),
                pltpu.VMEM((rows, span), jnp.int32),
                pltpu.VMEM((GROUP // 2, 2 * rows, span), f32),
                pltpu.VMEM((GROUP // 2, 2 * rows, span), bf16),
                pltpu.VMEM((GROUP // 2, 2 * rows, head_dim), f32),
                pltpu.VMEM((RING, rows * PITCH, head_dim), f32),
                pltpu.VMEM((RING, rows * PITCH, head_dim), f32),
                pltpu.VMEM((places, 4, block, head_dim), bf16),
                pltpu.VMEM((places, 4, block, head_dim), bf16),
                pltpu.VMEM((places, 3, block, head_dim), bf16),
                pltpu.VMEM((places, 3, block, head_dim), bf16),
                pltpu.VMEM((KEEP, own, GROUP, head_dim), f32),
                pltpu.VMEM((KEEP, own, GROUP, head_dim), f32),
                dma((KEYS,)), dma((VALUES,)),
                dma((5,)), dma((5, asks)),
                dma((2,)), dma((steps,)), dma((steps,)),
            ],
            compiler_params=pltpu.CompilerParams(
                collective_id=0, has_side_effects=True, vmem_limit_bytes=60 * 1024 * 1024),
            cost_estimate=pl.CostEstimate(
                flops=4 * num_batch * rows * span * head_dim,
                bytes_accessed=4 * num_batch * span * head_dim,
                transcendentals=num_batch * rows * span),
        )(q_local.transpose(1, 0, 2), len_local, k_span, v_span)
        return out.transpose(1, 0, 2)

    return jax.shard_map(
        group_step, mesh=mesh,
        in_specs=(P("kv", "dup", None), P("kv", "dup", None), P("kv", "dup", None), P("kv")),
        out_specs=P("kv", "dup", None), check_vma=False)
```

```python
import functools

import jax
import jax.numpy as jnp
from jax import lax
from jax.experimental import pallas as pl
from jax.experimental.pallas import tpu as pltpu
from jax.sharding import PartitionSpec as P

DRAFT = 4
NEG_BIG = -3e38
LOG2E = 1.4426950408889634
MESH = pl.DeviceIdType.MESH

GROUP = 16
KEYS = 10
VALUES = 11
PITCH = GROUP + 4
RING = 8
KEEP = 16
ASK = 2
GIVE, MERGE, FINAL = 2, 4, 9
SPARE = 9


def attend(q_ref, len_ref, k_hbm, v_hbm, o_ref,
           kbuf, vbuf, q_all, q_wide, pos_rel, s_buf, p_buf, i_buf, part_o, part_l,
           pair_so, pair_ro, chip_so, chip_ro, keep_o, keep_l,
           k_sem, v_sem, qs_sem, qr_sem, sent_sem, pair_sem, chip_sem):
    own, num_batch, head_dim = q_ref.shape
    span = k_hbm.shape[1]
    rows = 8 * own
    half = 4 * own
    data = own * GROUP
    steps = num_batch // GROUP
    asks = steps // ASK + 1
    scale = (head_dim ** -0.5) * LOG2E

    me = lax.axis_index("dup")
    chip = me // 2
    core = me % 2
    turn = (1 - 2 * core) * (1 - 2 * (chip % 2))
    partner = chip * 2 + (1 - core)
    ahead = ((chip + turn + 4) % 4) * 2 + core
    behind = ((chip - turn + 4) % 4) * 2 + core
    across = ((chip + 2) % 4) * 2 + core

    def key_copy(g):
        return pltpu.make_async_copy(k_hbm.at[pl.ds(g * GROUP, GROUP)], kbuf.at[g % KEYS], k_sem.at[g % KEYS])

    def value_copy(g):
        return pltpu.make_async_copy(v_hbm.at[pl.ds(g * GROUP, GROUP)], vbuf.at[g % VALUES], v_sem.at[g % VALUES])

    key_copy(0).start()
    key_copy(1).start()

    def start_cache(g, carry):
        key_copy(g + 2).start()
        value_copy(g).start()
        return carry

    lax.fori_loop(0, KEYS - 2, start_cache, 0)
    for g in range(KEYS - 2, VALUES):
        value_copy(g).start()

    barrier = pltpu.get_barrier_semaphore()
    for peer in (partner, ahead, behind, across):
        pl.semaphore_signal(barrier, inc=1, device_id={"dup": peer}, device_id_type=MESH)

    def q_copy(kind, c, direct=False):
        if isinstance(c, int) and c < 2:
            part = pl.ds(c * GROUP, GROUP)
        else:
            part = pl.ds(pl.multiple_of((c - 1) * ASK * GROUP, ASK * GROUP), ASK * GROUP)
        src, dst, peer = (
            (q_ref.at[:, part], q_all.at[1, :, part], behind),
            (q_ref.at[:, part], q_all.at[2, :, part], ahead),
            (q_ref.at[:, part], q_all.at[4, :, part], partner),
            (q_all.at[1, :, part], q_all.at[3, :, part], ahead),
            (q_all.at[1:4, :, part], q_all.at[5:8, :, part], partner),
        )[kind]
        if direct:
            src, peer = q_ref.at[:, part], across
        return pltpu.make_async_remote_copy(
            src_ref=src, dst_ref=dst, send_sem=qs_sem.at[kind], recv_sem=qr_sem.at[kind, c],
            device_id={"dup": peer}, device_id_type=MESH)

    def q_own(c):
        q_copy(0, c).start()
        q_copy(2, c).start()

    def q_pass_near(c):
        q_copy(0, c).wait_recv()
        q_copy(3, c).start()
        q_copy(1, c).start()

    def q_pass_far(c):
        q_copy(1, c).wait_recv()
        q_copy(3, c).wait_recv()
        q_copy(4, c).start()

    span_start = me * span
    chip_disp = (0, 4 - turn, 4 + turn, 2)
    pair_disp = (0, 4 + turn, 4 - turn, 2)
    row_id = lax.broadcasted_iota(jnp.int32, (rows, span), 0)
    token = jnp.zeros((rows, span), jnp.int32)
    for h in range(2):
        for s in range(4):
            disp = (chip_disp, pair_disp)[h][s]
            device = ((chip + disp) % 4) * 2 + (core if h == 0 else 1 - core)
            for i in range(own):
                token = jnp.where(row_id == h * half + s * own + i, (own * device + i) % DRAFT, token)
    pos_rel[...] = lax.broadcasted_iota(jnp.int32, (rows, span), 1) + span_start - token

    pl.semaphore_wait(barrier, 4)
    for c in range(2):
        q_copy(3, c, direct=True).start()
        q_own(c)
        q_copy(1, c).start()
    for c in range(2, 7):
        q_own(c)
    q_pass_near(2)
    for c in range(2):
        q_copy(0, c).wait_recv()
        q_pass_far(c)
    q_pass_near(3)

    def q_arrive(c):
        for kind in (2, 4):
            q_copy(kind, c).wait_recv()

    lane = lax.broadcasted_iota(jnp.int32, (GROUP, head_dim), 1)
    seq = lax.broadcasted_iota(jnp.int32, (GROUP, head_dim), 0)

    def widen(g):
        part = pl.ds(pl.multiple_of(g * GROUP, GROUP), GROUP)
        for s in range(8):
            for i in range(own):
                block = q_ref[i, part, :] if s == 0 else q_all[s, i, part, :]
                q_wide[pl.ds((s * own + i) * PITCH, GROUP), :] = block.astype(jnp.float32)

    def score(g, n):
        slot, j = g % KEYS, 2 * n
        zeros = jnp.zeros((rows, head_dim), jnp.float32)
        q0 = q_wide[pl.ds(j, rows, stride=PITCH), :]
        q1 = q_wide[pl.ds(j + 1, rows, stride=PITCH), :]
        q2 = jnp.concatenate([jnp.concatenate([q0, zeros], 1), jnp.concatenate([zeros, q1], 1)], 0).astype(jnp.bfloat16)
        k2 = jnp.concatenate([kbuf[slot, j], kbuf[slot, j + 1]], 1)
        s_buf[n] = lax.dot_general(q2, k2, (((1,), (1,)), ((), ())), preferred_element_type=jnp.float32)

    def soften(g, n):
        slab_l = part_l.at[g % RING]
        j = 2 * n
        s = s_buf[n]
        rel = pos_rel[...]
        base = g * GROUP + j
        s = jnp.concatenate([
            jnp.where(rel <= len_ref[base] - DRAFT, s[:rows], NEG_BIG),
            jnp.where(rel <= len_ref[base + 1] - DRAFT, s[rows:], NEG_BIG)], 0)
        peak = jnp.max(s, axis=1, keepdims=True)
        p = jnp.exp2((s - peak) * scale)
        mass = jnp.sum(p, axis=1, keepdims=True)
        p_buf[n] = p.astype(jnp.bfloat16)
        i_buf[n] = jnp.broadcast_to(1.0 / mass, (2 * rows, head_dim))
        log_mass = jnp.broadcast_to(peak * scale + jnp.log2(mass), (2 * rows, head_dim))
        for m in range(2):
            slab_l[pl.ds(j + m, rows, stride=PITCH), :] = log_mass[m * rows:(m + 1) * rows]

    def mix(g, n):
        slot, j = g % VALUES, 2 * n
        slab_o = part_o.at[g % RING]
        v2 = jnp.concatenate([vbuf[slot, j], vbuf[slot, j + 1]], 1)
        o2 = jnp.dot(p_buf[n], v2, preferred_element_type=jnp.float32)
        inv = i_buf[n]
        for m in range(2):
            o = o2[m * rows:(m + 1) * rows, m * head_dim:(m + 1) * head_dim] * inv[m * rows:(m + 1) * rows]
            slab_o[pl.ds(j + m, rows, stride=PITCH), :] = o

    pairs = range(GROUP // 2)

    def to_lanes(values):
        total = jnp.zeros((GROUP, head_dim), jnp.float32)
        for i, value in enumerate(values):
            total = jnp.where(lane == seq + i * GROUP, value, total)
        line = jnp.sum(total, axis=0, keepdims=True)
        high = line.astype(jnp.bfloat16).astype(jnp.float32)
        mid = (line - high).astype(jnp.bfloat16).astype(jnp.float32)
        low = line - high - mid
        part = seq[:8]
        return jnp.where(part == 0, high, jnp.where(part == 1, mid, jnp.where(part == 2, low, 0.0))).astype(jnp.bfloat16)

    def put(ref, values, logs):
        for i, value in enumerate(values):
            ref[i * GROUP:(i + 1) * GROUP, :] = value.astype(jnp.bfloat16)
        ref[data:data + 8, :] = to_lanes(logs)

    def take(ref):
        line = jnp.sum(ref[data:data + 8, :].astype(jnp.float32), axis=0, keepdims=True)
        return [(ref[i * GROUP:(i + 1) * GROUP, :].astype(jnp.float32),
                 jnp.sum(jnp.where(lane == seq + i * GROUP, line, 0.0), axis=1, keepdims=True)) for i in range(own)]

    def joined(mine, log_mine, theirs, log_theirs):
        top = jnp.maximum(log_mine, log_theirs)
        w_mine, w_theirs = jnp.exp2(log_mine - top), jnp.exp2(log_theirs - top)
        total = w_mine + w_theirs
        return (w_mine * mine + w_theirs * theirs) / total, top + jnp.log2(total)

    def pair_copy(c):
        return pltpu.make_async_remote_copy(
            src_ref=pair_so.at[c], dst_ref=pair_ro.at[c], send_sem=sent_sem.at[0], recv_sem=pair_sem.at[c],
            device_id={"dup": partner}, device_id_type=MESH)

    def chip_start(c):
        for n, peer in ((2, across), (0, behind), (1, ahead)):
            pltpu.make_async_remote_copy(
                src_ref=chip_so.at[c, n], dst_ref=chip_ro.at[c, n], send_sem=sent_sem.at[1], recv_sem=chip_sem.at[c],
                device_id={"dup": peer}, device_id_type=MESH).start()

    def chip_arrive(c):
        pltpu.make_async_remote_copy(
            src_ref=chip_so.at[c], dst_ref=chip_ro.at[c], send_sem=sent_sem.at[1], recv_sem=chip_sem.at[c],
            device_id={"dup": partner}, device_id_type=MESH).wait_recv()

    def slab(ref, g, row):
        return ref.at[g % RING][pl.ds(row * PITCH, GROUP), :]

    def place(g):
        return (g + steps + SPARE) % (steps + SPARE)

    def give(g):
        c, r = place(g), g + KEEP
        for s in range(4):
            at = [half + s * own + i for i in range(own)]
            put(pair_so.at[c, s], [slab(part_o, r, n) for n in at], [slab(part_l, r, n) for n in at])

    def merge(g):
        c, r = place(g), g + KEEP
        for s in (3, 1, 2, 0):
            both = [joined(slab(part_o, r, s * own + i), slab(part_l, r, s * own + i), *theirs)
                    for i, theirs in enumerate(take(pair_ro.at[c, s]))]
            if s:
                put(chip_so.at[c, s - 1], [o for o, _ in both], [log for _, log in both])
            else:
                for i, (o, log) in enumerate(both):
                    keep_o[r % KEEP, i] = o
                    keep_l[r % KEEP, i] = log

    def final(g):
        c, r = place(g), g + KEEP
        to = pl.ds(pl.multiple_of(((g + steps) % steps) * GROUP, GROUP), GROUP)
        others = [take(chip_ro.at[c, n]) for n in range(3)]
        for i in range(own):
            logs = [keep_l[r % KEEP, i]] + [other[i][1] for other in others]
            top = functools.reduce(jnp.maximum, logs)
            weights = [jnp.exp2(log - top) for log in logs]
            total = functools.reduce(jnp.add, weights)
            merged = weights[0] * keep_o[r % KEEP, i]
            for weight, other in zip(weights[1:], others):
                merged = merged + weight * other[i][0]
            o_ref[i, to, :] = (merged / total).astype(jnp.bfloat16)

    q_arrive(0)
    key_copy(0).wait()
    widen(0)
    for n in pairs:
        score(0, n)
    key_copy(KEYS).start()
    q_pass_far(2)
    key_copy(1).wait()
    q_arrive(1)
    widen(1)
    for n in pairs:
        soften(0, n)
        score(1, n)
    key_copy(KEYS + 1).start()
    q_pass_near(4)

    def step(t, carry, full):
        c = t // ASK + 1

        @pl.when(t % ASK == 0)
        def _():
            if not full:
                @pl.when(c + 5 < asks)
                def _():
                    q_own(c + 5)

            @pl.when(c + 3 < asks)
            def _():
                q_pass_near(c + 3)

            @pl.when(c + 1 < asks)
            def _():
                q_pass_far(c + 1)

            q_arrive(c)

        key_copy(t).wait()
        value_copy(t - 2).wait()
        if full:
            pair_copy(t - MERGE).wait_recv()
            chip_arrive(t - FINAL)
            final(t - FINAL)
        else:
            @pl.when(t >= MERGE)
            def _():
                pair_copy(t - MERGE).wait_recv()

        widen(t)
        for n in pairs:
            mix(t - 2, n)
            soften(t - 1, n)
            score(t, n)
        give(t - GIVE)
        merge(t - MERGE)

        pair_copy(t - GIVE).start()
        if full:
            chip_start(t - MERGE)
        else:
            @pl.when(t >= MERGE)
            def _():
                chip_start(t - MERGE)

            @pl.when(t + KEYS < steps)
            def _():
                key_copy(t + KEYS).start()

            @pl.when(t - 2 + VALUES < steps)
            def _():
                value_copy(t - 2 + VALUES).start()
        return carry

    lax.fori_loop(2, FINAL, functools.partial(step, full=False), 0)
    lax.fori_loop(FINAL, steps, functools.partial(step, full=True), 0)

    def late_merge(g, carry):
        pair_copy(g).wait_recv()
        merge(g)
        chip_start(g)
        return carry

    def late_final(g, carry):
        chip_arrive(g)
        final(g)
        return carry

    value_copy(steps - 2).wait()
    pair_copy(steps - 4).wait_recv()
    merge(steps - 4)
    for n in pairs:
        mix(steps - 2, n)
        soften(steps - 1, n)
    give(steps - 2)
    pair_copy(steps - 2).start()
    chip_start(steps - 4)
    value_copy(steps - 1).wait()
    for n in pairs:
        mix(steps - 1, n)
    give(steps - 1)
    pair_copy(steps - 1).start()
    lax.fori_loop(steps - MERGE + 1, steps, late_merge, 0)
    lax.fori_loop(steps - FINAL, steps, late_final, 0)

    def drain(src, sem):
        pltpu.make_async_remote_copy(
            src_ref=src, dst_ref=src, send_sem=sem, recv_sem=pair_sem.at[0],
            device_id={"dup": partner}, device_id_type=MESH).wait_send()

    for kind, src in enumerate((q_ref, q_ref, q_ref, q_all.at[1], q_all.at[1:4])):
        drain(src, qs_sem.at[kind])
    drain(pair_so.at[pl.ds(0, steps)], sent_sem.at[0])
    drain(chip_so.at[pl.ds(0, steps)], sent_sem.at[1])


def solution(mesh):
    def group_step(q_local, k_span, v_span, len_local):
        num_batch, own, head_dim = q_local.shape
        span = k_span.shape[1]
        steps = num_batch // GROUP
        asks = steps // ASK + 1
        places = steps + SPARE
        block = own * GROUP + 8
        rows = 8 * own
        vmem = functools.partial(pl.BlockSpec, memory_space=pltpu.VMEM)
        hbm = functools.partial(pl.BlockSpec, memory_space=pl.ANY)
        bf16, f32 = jnp.bfloat16, jnp.float32
        dma = pltpu.SemaphoreType.DMA
        out = pl.pallas_call(
            attend,
            out_shape=jax.ShapeDtypeStruct((own, num_batch, head_dim), bf16),
            in_specs=[vmem(), pl.BlockSpec(memory_space=pltpu.SMEM), hbm(), hbm()],
            out_specs=vmem(),
            scratch_shapes=[
                pltpu.VMEM((KEYS, GROUP, span, head_dim), bf16),
                pltpu.VMEM((VALUES, GROUP, span, head_dim), bf16),
                pltpu.VMEM((8, own, num_batch, head_dim), bf16),
                pltpu.VMEM((rows * PITCH, head_dim), f32),
                pltpu.VMEM((rows, span), jnp.int32),
                pltpu.VMEM((GROUP // 2, 2 * rows, span), f32),
                pltpu.VMEM((GROUP // 2, 2 * rows, span), bf16),
                pltpu.VMEM((GROUP // 2, 2 * rows, head_dim), f32),
                pltpu.VMEM((RING, rows * PITCH, head_dim), f32),
                pltpu.VMEM((RING, rows * PITCH, head_dim), f32),
                pltpu.VMEM((places, 4, block, head_dim), bf16),
                pltpu.VMEM((places, 4, block, head_dim), bf16),
                pltpu.VMEM((places, 3, block, head_dim), bf16),
                pltpu.VMEM((places, 3, block, head_dim), bf16),
                pltpu.VMEM((KEEP, own, GROUP, head_dim), f32),
                pltpu.VMEM((KEEP, own, GROUP, head_dim), f32),
                dma((KEYS,)), dma((VALUES,)),
                dma((5,)), dma((5, asks)),
                dma((2,)), dma((steps,)), dma((steps,)),
            ],
            compiler_params=pltpu.CompilerParams(
                collective_id=0, has_side_effects=True, vmem_limit_bytes=60 * 1024 * 1024),
            cost_estimate=pl.CostEstimate(
                flops=4 * num_batch * rows * span * head_dim,
                bytes_accessed=4 * num_batch * span * head_dim,
                transcendentals=num_batch * rows * span),
        )(q_local.transpose(1, 0, 2), len_local, k_span, v_span)
        return out.transpose(1, 0, 2)

    return jax.shard_map(
        group_step, mesh=mesh,
        in_specs=(P("kv", "dup", None), P("kv", "dup", None), P("kv", "dup", None), P("kv")),
        out_specs=P("kv", "dup", None), check_vma=False)
```

```python
import functools

import jax
import jax.numpy as jnp
from jax import lax
from jax.experimental import pallas as pl
from jax.experimental.pallas import tpu as pltpu
from jax.sharding import PartitionSpec as P

DRAFT = 4
NEG_BIG = -3e38
LOG2E = 1.4426950408889634
MESH = pl.DeviceIdType.MESH

GROUP = 16
KEYS = 10
VALUES = 11
PITCH = GROUP + 4
RING = 8
KEEP = 16
ASK = 2
GIVE, MERGE = 2, 4
SPARE = 4


def attend(q_ref, len_ref, k_hbm, v_hbm, o_ref,
           kbuf, vbuf, q_all, q_wide, pos_rel, s_buf, p_buf, i_buf, part_o, part_l,
           pair_so, pair_ro, chip_so, chip_ro, keep_o, keep_l,
           k_sem, v_sem, qs_sem, qr_sem, sent_sem, pair_sem, chip_sem):
    own, num_batch, head_dim = q_ref.shape
    span = k_hbm.shape[1]
    rows = 8 * own
    half = 4 * own
    data = own * GROUP
    steps = num_batch // GROUP
    asks = steps // ASK + 1
    scale = (head_dim ** -0.5) * LOG2E

    me = lax.axis_index("dup")
    chip = me // 2
    core = me % 2
    turn = (1 - 2 * core) * (1 - 2 * (chip % 2))
    partner = chip * 2 + (1 - core)
    ahead = ((chip + turn + 4) % 4) * 2 + core
    behind = ((chip - turn + 4) % 4) * 2 + core
    across = ((chip + 2) % 4) * 2 + core

    def key_copy(g):
        return pltpu.make_async_copy(k_hbm.at[pl.ds(g * GROUP, GROUP)], kbuf.at[g % KEYS], k_sem.at[g % KEYS])

    def value_copy(g):
        return pltpu.make_async_copy(v_hbm.at[pl.ds(g * GROUP, GROUP)], vbuf.at[g % VALUES], v_sem.at[g % VALUES])

    key_copy(0).start()
    key_copy(1).start()

    def start_cache(g, carry):
        key_copy(g + 2).start()
        value_copy(g).start()
        return carry

    lax.fori_loop(0, KEYS - 2, start_cache, 0)
    for g in range(KEYS - 2, VALUES):
        value_copy(g).start()

    barrier = pltpu.get_barrier_semaphore()
    for peer in (partner, ahead, behind, across):
        pl.semaphore_signal(barrier, inc=1, device_id={"dup": peer}, device_id_type=MESH)

    def q_copy(kind, c, direct=False):
        if isinstance(c, int) and c < 2:
            part = pl.ds(c * GROUP, GROUP)
        else:
            part = pl.ds(pl.multiple_of((c - 1) * ASK * GROUP, ASK * GROUP), ASK * GROUP)
        src, dst, peer = (
            (q_ref.at[:, part], q_all.at[1, :, part], behind),
            (q_ref.at[:, part], q_all.at[2, :, part], ahead),
            (q_ref.at[:, part], q_all.at[4, :, part], partner),
            (q_all.at[1, :, part], q_all.at[3, :, part], ahead),
            (q_all.at[1:4, :, part], q_all.at[5:8, :, part], partner),
        )[kind]
        if direct:
            src, peer = q_ref.at[:, part], across
        return pltpu.make_async_remote_copy(
            src_ref=src, dst_ref=dst, send_sem=qs_sem.at[kind], recv_sem=qr_sem.at[kind, c],
            device_id={"dup": peer}, device_id_type=MESH)

    def q_own(c):
        q_copy(0, c).start()
        q_copy(2, c).start()

    def q_pass_near(c):
        q_copy(0, c).wait_recv()
        q_copy(3, c).start()
        q_copy(1, c).start()

    def q_pass_far(c):
        q_copy(1, c).wait_recv()
        q_copy(3, c).wait_recv()
        q_copy(4, c).start()

    span_start = me * span
    chip_disp = (0, 4 - turn, 4 + turn, 2)
    pair_disp = (0, 4 + turn, 4 - turn, 2)
    row_id = lax.broadcasted_iota(jnp.int32, (rows, span), 0)
    token = jnp.zeros((rows, span), jnp.int32)
    for h in range(2):
        for s in range(4):
            disp = (chip_disp, pair_disp)[h][s]
            device = ((chip + disp) % 4) * 2 + (core if h == 0 else 1 - core)
            for i in range(own):
                token = jnp.where(row_id == h * half + s * own + i, (own * device + i) % DRAFT, token)
    pos_rel[...] = lax.broadcasted_iota(jnp.int32, (rows, span), 1) + span_start - token

    pl.semaphore_wait(barrier, 4)
    for c in range(2):
        q_copy(3, c, direct=True).start()
        q_own(c)
        q_copy(1, c).start()
    for c in range(2, 7):
        q_own(c)
    q_pass_near(2)
    for c in range(2):
        q_copy(0, c).wait_recv()
        q_pass_far(c)
    q_pass_near(3)

    def q_arrive(c):
        for kind in (2, 4):
            q_copy(kind, c).wait_recv()

    lane = lax.broadcasted_iota(jnp.int32, (GROUP, head_dim), 1)
    seq = lax.broadcasted_iota(jnp.int32, (GROUP, head_dim), 0)

    def widen(g):
        part = pl.ds(pl.multiple_of(g * GROUP, GROUP), GROUP)
        for s in range(8):
            for i in range(own):
                block = q_ref[i, part, :] if s == 0 else q_all[s, i, part, :]
                q_wide[pl.ds((s * own + i) * PITCH, GROUP), :] = block.astype(jnp.float32)

    def score(g, n):
        slot, j = g % KEYS, 2 * n
        zeros = jnp.zeros((rows, head_dim), jnp.float32)
        q0 = q_wide[pl.ds(j, rows, stride=PITCH), :]
        q1 = q_wide[pl.ds(j + 1, rows, stride=PITCH), :]
        q2 = jnp.concatenate([jnp.concatenate([q0, zeros], 1), jnp.concatenate([zeros, q1], 1)], 0).astype(jnp.bfloat16)
        k2 = jnp.concatenate([kbuf[slot, j], kbuf[slot, j + 1]], 1)
        s_buf[n] = lax.dot_general(q2, k2, (((1,), (1,)), ((), ())), preferred_element_type=jnp.float32)

    def soften(g, n):
        slab_l = part_l.at[g % RING]
        j = 2 * n
        s = s_buf[n]
        rel = pos_rel[...]
        base = g * GROUP + j
        s = jnp.concatenate([
            jnp.where(rel <= len_ref[base] - DRAFT, s[:rows], NEG_BIG),
            jnp.where(rel <= len_ref[base + 1] - DRAFT, s[rows:], NEG_BIG)], 0)
        peak = jnp.max(s, axis=1, keepdims=True)
        p = jnp.exp2((s - peak) * scale)
        mass = jnp.sum(p, axis=1, keepdims=True)
        p_buf[n] = p.astype(jnp.bfloat16)
        i_buf[n] = jnp.broadcast_to(1.0 / mass, (2 * rows, head_dim))
        log_mass = jnp.broadcast_to(peak * scale + jnp.log2(mass), (2 * rows, head_dim))
        for m in range(2):
            slab_l[pl.ds(j + m, rows, stride=PITCH), :] = log_mass[m * rows:(m + 1) * rows]

    def mix(g, n):
        slot, j = g % VALUES, 2 * n
        slab_o = part_o.at[g % RING]
        v2 = jnp.concatenate([vbuf[slot, j], vbuf[slot, j + 1]], 1)
        o2 = jnp.dot(p_buf[n], v2, preferred_element_type=jnp.float32)
        inv = i_buf[n]
        for m in range(2):
            o = o2[m * rows:(m + 1) * rows, m * head_dim:(m + 1) * head_dim] * inv[m * rows:(m + 1) * rows]
            slab_o[pl.ds(j + m, rows, stride=PITCH), :] = o

    pairs = range(GROUP // 2)

    def to_lanes(values):
        total = jnp.zeros((GROUP, head_dim), jnp.float32)
        for i, value in enumerate(values):
            total = jnp.where(lane == seq + i * GROUP, value, total)
        line = jnp.sum(total, axis=0, keepdims=True)
        high = line.astype(jnp.bfloat16).astype(jnp.float32)
        mid = (line - high).astype(jnp.bfloat16).astype(jnp.float32)
        low = line - high - mid
        part = seq[:8]
        return jnp.where(part == 0, high, jnp.where(part == 1, mid, jnp.where(part == 2, low, 0.0))).astype(jnp.bfloat16)

    def put(ref, values, logs):
        for i, value in enumerate(values):
            ref[i * GROUP:(i + 1) * GROUP, :] = value.astype(jnp.bfloat16)
        ref[data:data + 8, :] = to_lanes(logs)

    def take(ref):
        line = jnp.sum(ref[data:data + 8, :].astype(jnp.float32), axis=0, keepdims=True)
        return [(ref[i * GROUP:(i + 1) * GROUP, :].astype(jnp.float32),
                 jnp.sum(jnp.where(lane == seq + i * GROUP, line, 0.0), axis=1, keepdims=True)) for i in range(own)]

    def joined(mine, log_mine, theirs, log_theirs):
        top = jnp.maximum(log_mine, log_theirs)
        w_mine, w_theirs = jnp.exp2(log_mine - top), jnp.exp2(log_theirs - top)
        total = w_mine + w_theirs
        return (w_mine * mine + w_theirs * theirs) / total, top + jnp.log2(total)

    def pair_copy(c):
        return pltpu.make_async_remote_copy(
            src_ref=pair_so.at[c], dst_ref=pair_ro.at[c], send_sem=sent_sem.at[0], recv_sem=pair_sem.at[c],
            device_id={"dup": partner}, device_id_type=MESH)

    def chip_start(c):
        for n, peer in ((2, across), (0, behind), (1, ahead)):
            pltpu.make_async_remote_copy(
                src_ref=chip_so.at[c, n], dst_ref=chip_ro.at[c, n], send_sem=sent_sem.at[1], recv_sem=chip_sem.at[c],
                device_id={"dup": peer}, device_id_type=MESH).start()

    def chip_arrive(c):
        pltpu.make_async_remote_copy(
            src_ref=chip_so.at[c], dst_ref=chip_ro.at[c], send_sem=sent_sem.at[1], recv_sem=chip_sem.at[c],
            device_id={"dup": partner}, device_id_type=MESH).wait_recv()

    def slab(ref, g, row):
        return ref.at[g % RING][pl.ds(row * PITCH, GROUP), :]

    def place(g):
        return (g + steps + SPARE) % (steps + SPARE)

    def give(g):
        c, r = place(g), g + KEEP
        for s in range(4):
            at = [half + s * own + i for i in range(own)]
            put(pair_so.at[c, s], [slab(part_o, r, n) for n in at], [slab(part_l, r, n) for n in at])

    def merge(g):
        c, r = place(g), g + KEEP
        for s in (3, 1, 2, 0):
            both = [joined(slab(part_o, r, s * own + i), slab(part_l, r, s * own + i), *theirs)
                    for i, theirs in enumerate(take(pair_ro.at[c, s]))]
            if s:
                put(chip_so.at[c, s - 1], [o for o, _ in both], [log for _, log in both])
            else:
                for i, (o, log) in enumerate(both):
                    keep_o[r % KEEP, i] = o
                    keep_l[r % KEEP, i] = log

    def final(g):
        c, r = place(g), g + KEEP
        to = pl.ds(pl.multiple_of(((g + steps) % steps) * GROUP, GROUP), GROUP)
        others = [take(chip_ro.at[c, n]) for n in range(3)]
        for i in range(own):
            logs = [keep_l[r % KEEP, i]] + [other[i][1] for other in others]
            top = functools.reduce(jnp.maximum, logs)
            weights = [jnp.exp2(log - top) for log in logs]
            total = functools.reduce(jnp.add, weights)
            merged = weights[0] * keep_o[r % KEEP, i]
            for weight, other in zip(weights[1:], others):
                merged = merged + weight * other[i][0]
            o_ref[i, to, :] = (merged / total).astype(jnp.bfloat16)

    q_arrive(0)
    key_copy(0).wait()
    widen(0)
    for n in pairs:
        score(0, n)
    key_copy(KEYS).start()
    q_pass_far(2)
    key_copy(1).wait()
    q_arrive(1)
    widen(1)
    for n in pairs:
        soften(0, n)
        score(1, n)
    key_copy(KEYS + 1).start()
    q_pass_near(4)

    def step(t, carry, full):
        c = t // ASK + 1

        @pl.when(t % ASK == 0)
        def _():
            if not full:
                @pl.when(c + 5 < asks)
                def _():
                    q_own(c + 5)

            @pl.when(c + 3 < asks)
            def _():
                q_pass_near(c + 3)

            @pl.when(c + 1 < asks)
            def _():
                q_pass_far(c + 1)

            q_arrive(c)

        key_copy(t).wait()
        value_copy(t - 2).wait()
        if full:
            pair_copy(t - MERGE).wait_recv()
        else:
            @pl.when(t >= MERGE)
            def _():
                pair_copy(t - MERGE).wait_recv()

        widen(t)
        for n in pairs:
            mix(t - 2, n)
            soften(t - 1, n)
            score(t, n)
        give(t - GIVE)
        merge(t - MERGE)

        pair_copy(t - GIVE).start()
        if full:
            chip_start(t - MERGE)
        else:
            @pl.when(t >= MERGE)
            def _():
                chip_start(t - MERGE)

            @pl.when(t + KEYS < steps)
            def _():
                key_copy(t + KEYS).start()

            @pl.when(t - 2 + VALUES < steps)
            def _():
                value_copy(t - 2 + VALUES).start()
        return carry

    lax.fori_loop(2, steps // 2, functools.partial(step, full=False), 0)
    lax.fori_loop(steps // 2, steps, functools.partial(step, full=True), 0)

    def late_merge(g, carry):
        pair_copy(g).wait_recv()
        merge(g)
        chip_start(g)
        return carry

    def late_final(g, carry):
        chip_arrive(g)
        final(g)
        return carry

    value_copy(steps - 2).wait()
    pair_copy(steps - 4).wait_recv()
    merge(steps - 4)
    for n in pairs:
        mix(steps - 2, n)
        soften(steps - 1, n)
    give(steps - 2)
    pair_copy(steps - 2).start()
    chip_start(steps - 4)
    value_copy(steps - 1).wait()
    for n in pairs:
        mix(steps - 1, n)
    give(steps - 1)
    pair_copy(steps - 1).start()
    lax.fori_loop(steps - MERGE + 1, steps, late_merge, 0)
    lax.fori_loop(0, steps, late_final, 0)

    def drain(src, sem):
        pltpu.make_async_remote_copy(
            src_ref=src, dst_ref=src, send_sem=sem, recv_sem=pair_sem.at[0],
            device_id={"dup": partner}, device_id_type=MESH).wait_send()

    for kind, src in enumerate((q_ref, q_ref, q_ref, q_all.at[1], q_all.at[1:4])):
        drain(src, qs_sem.at[kind])
    drain(pair_so.at[pl.ds(0, steps)], sent_sem.at[0])
    drain(chip_so.at[pl.ds(0, steps)], sent_sem.at[1])


def solution(mesh):
    def group_step(q_local, k_span, v_span, len_local):
        num_batch, own, head_dim = q_local.shape
        span = k_span.shape[1]
        steps = num_batch // GROUP
        asks = steps // ASK + 1
        places = steps + SPARE
        block = own * GROUP + 8
        rows = 8 * own
        vmem = functools.partial(pl.BlockSpec, memory_space=pltpu.VMEM)
        hbm = functools.partial(pl.BlockSpec, memory_space=pl.ANY)
        bf16, f32 = jnp.bfloat16, jnp.float32
        dma = pltpu.SemaphoreType.DMA
        out = pl.pallas_call(
            attend,
            out_shape=jax.ShapeDtypeStruct((own, num_batch, head_dim), bf16),
            in_specs=[vmem(), pl.BlockSpec(memory_space=pltpu.SMEM), hbm(), hbm()],
            out_specs=vmem(),
            scratch_shapes=[
                pltpu.VMEM((KEYS, GROUP, span, head_dim), bf16),
                pltpu.VMEM((VALUES, GROUP, span, head_dim), bf16),
                pltpu.VMEM((8, own, num_batch, head_dim), bf16),
                pltpu.VMEM((rows * PITCH, head_dim), f32),
                pltpu.VMEM((rows, span), jnp.int32),
                pltpu.VMEM((GROUP // 2, 2 * rows, span), f32),
                pltpu.VMEM((GROUP // 2, 2 * rows, span), bf16),
                pltpu.VMEM((GROUP // 2, 2 * rows, head_dim), f32),
                pltpu.VMEM((RING, rows * PITCH, head_dim), f32),
                pltpu.VMEM((RING, rows * PITCH, head_dim), f32),
                pltpu.VMEM((places, 4, block, head_dim), bf16),
                pltpu.VMEM((places, 4, block, head_dim), bf16),
                pltpu.VMEM((places, 3, block, head_dim), bf16),
                pltpu.VMEM((places, 3, block, head_dim), bf16),
                pltpu.VMEM((KEEP, own, GROUP, head_dim), f32),
                pltpu.VMEM((KEEP, own, GROUP, head_dim), f32),
                dma((KEYS,)), dma((VALUES,)),
                dma((5,)), dma((5, asks)),
                dma((2,)), dma((steps,)), dma((steps,)),
            ],
            compiler_params=pltpu.CompilerParams(
                collective_id=0, has_side_effects=True, vmem_limit_bytes=60 * 1024 * 1024),
            cost_estimate=pl.CostEstimate(
                flops=4 * num_batch * rows * span * head_dim,
                bytes_accessed=4 * num_batch * span * head_dim,
                transcendentals=num_batch * rows * span),
        )(q_local.transpose(1, 0, 2), len_local, k_span, v_span)
        return out.transpose(1, 0, 2)

    return jax.shard_map(
        group_step, mesh=mesh,
        in_specs=(P("kv", "dup", None), P("kv", "dup", None), P("kv", "dup", None), P("kv")),
        out_specs=P("kv", "dup", None), check_vma=False)
```

```python
import functools

import jax
import jax.numpy as jnp
from jax import lax
from jax.experimental import pallas as pl
from jax.experimental.pallas import tpu as pltpu
from jax.sharding import PartitionSpec as P

DRAFT = 4
NEG_BIG = -3e38
LOG2E = 1.4426950408889634
MESH = pl.DeviceIdType.MESH

GROUP = 16
KEYS = 10
VALUES = 11
PITCH = GROUP + 4
RING = 8
KEEP = 16
ASK = 2
GIVE, MERGE = 2, 5
SPARE = 5


def attend(q_ref, len_ref, k_hbm, v_hbm, o_ref,
           kbuf, vbuf, q_all, q_wide, pos_rel, s_buf, p_buf, i_buf, part_o, part_l,
           pair_so, pair_ro, chip_so, chip_ro, keep_o, keep_l,
           k_sem, v_sem, qs_sem, qr_sem, sent_sem, pair_sem, chip_sem):
    own, num_batch, head_dim = q_ref.shape
    span = k_hbm.shape[1]
    rows = 8 * own
    half = 4 * own
    data = own * GROUP
    steps = num_batch // GROUP
    asks = steps // ASK + 1
    scale = (head_dim ** -0.5) * LOG2E

    me = lax.axis_index("dup")
    chip = me // 2
    core = me % 2
    turn = (1 - 2 * core) * (1 - 2 * (chip % 2))
    partner = chip * 2 + (1 - core)
    ahead = ((chip + turn + 4) % 4) * 2 + core
    behind = ((chip - turn + 4) % 4) * 2 + core
    across = ((chip + 2) % 4) * 2 + core

    def key_copy(g):
        return pltpu.make_async_copy(k_hbm.at[pl.ds(g * GROUP, GROUP)], kbuf.at[g % KEYS], k_sem.at[g % KEYS])

    def value_copy(g):
        return pltpu.make_async_copy(v_hbm.at[pl.ds(g * GROUP, GROUP)], vbuf.at[g % VALUES], v_sem.at[g % VALUES])

    key_copy(0).start()
    key_copy(1).start()

    def start_cache(g, carry):
        key_copy(g + 2).start()
        value_copy(g).start()
        return carry

    lax.fori_loop(0, KEYS - 2, start_cache, 0)
    for g in range(KEYS - 2, VALUES):
        value_copy(g).start()

    barrier = pltpu.get_barrier_semaphore()
    for peer in (partner, ahead, behind, across):
        pl.semaphore_signal(barrier, inc=1, device_id={"dup": peer}, device_id_type=MESH)

    def q_copy(kind, c, direct=False):
        if isinstance(c, int) and c < 2:
            part = pl.ds(c * GROUP, GROUP)
        else:
            part = pl.ds(pl.multiple_of((c - 1) * ASK * GROUP, ASK * GROUP), ASK * GROUP)
        src, dst, peer = (
            (q_ref.at[:, part], q_all.at[1, :, part], behind),
            (q_ref.at[:, part], q_all.at[2, :, part], ahead),
            (q_ref.at[:, part], q_all.at[4, :, part], partner),
            (q_all.at[1, :, part], q_all.at[3, :, part], ahead),
            (q_all.at[1:4, :, part], q_all.at[5:8, :, part], partner),
        )[kind]
        if direct:
            src, peer = q_ref.at[:, part], across
        return pltpu.make_async_remote_copy(
            src_ref=src, dst_ref=dst, send_sem=qs_sem.at[kind], recv_sem=qr_sem.at[kind, c],
            device_id={"dup": peer}, device_id_type=MESH)

    def q_own(c):
        q_copy(0, c).start()
        q_copy(2, c).start()

    def q_pass_near(c):
        q_copy(0, c).wait_recv()
        q_copy(3, c).start()
        q_copy(1, c).start()

    def q_pass_far(c):
        q_copy(1, c).wait_recv()
        q_copy(3, c).wait_recv()
        q_copy(4, c).start()

    span_start = me * span
    chip_disp = (0, 4 - turn, 4 + turn, 2)
    pair_disp = (0, 4 + turn, 4 - turn, 2)
    row_id = lax.broadcasted_iota(jnp.int32, (rows, span), 0)
    token = jnp.zeros((rows, span), jnp.int32)
    for h in range(2):
        for s in range(4):
            disp = (chip_disp, pair_disp)[h][s]
            device = ((chip + disp) % 4) * 2 + (core if h == 0 else 1 - core)
            for i in range(own):
                token = jnp.where(row_id == h * half + s * own + i, (own * device + i) % DRAFT, token)
    pos_rel[...] = lax.broadcasted_iota(jnp.int32, (rows, span), 1) + span_start - token

    pl.semaphore_wait(barrier, 4)
    for c in range(2):
        q_copy(3, c, direct=True).start()
        q_own(c)
        q_copy(1, c).start()
    for c in range(2, 7):
        q_own(c)
    q_pass_near(2)
    for c in range(2):
        q_copy(0, c).wait_recv()
        q_pass_far(c)
    q_pass_near(3)

    def q_arrive(c):
        for kind in (2, 4):
            q_copy(kind, c).wait_recv()

    lane = lax.broadcasted_iota(jnp.int32, (GROUP, head_dim), 1)
    seq = lax.broadcasted_iota(jnp.int32, (GROUP, head_dim), 0)

    def widen(g):
        part = pl.ds(pl.multiple_of(g * GROUP, GROUP), GROUP)
        for s in range(8):
            for i in range(own):
                block = q_ref[i, part, :] if s == 0 else q_all[s, i, part, :]
                q_wide[pl.ds((s * own + i) * PITCH, GROUP), :] = block.astype(jnp.float32)

    def score(g, n):
        slot, j = g % KEYS, 2 * n
        zeros = jnp.zeros((rows, head_dim), jnp.float32)
        q0 = q_wide[pl.ds(j, rows, stride=PITCH), :]
        q1 = q_wide[pl.ds(j + 1, rows, stride=PITCH), :]
        q2 = jnp.concatenate([jnp.concatenate([q0, zeros], 1), jnp.concatenate([zeros, q1], 1)], 0).astype(jnp.bfloat16)
        k2 = jnp.concatenate([kbuf[slot, j], kbuf[slot, j + 1]], 1)
        s_buf[n] = lax.dot_general(q2, k2, (((1,), (1,)), ((), ())), preferred_element_type=jnp.float32)

    def soften(g, n):
        slab_l = part_l.at[g % RING]
        j = 2 * n
        s = s_buf[n]
        rel = pos_rel[...]
        base = g * GROUP + j
        s = jnp.concatenate([
            jnp.where(rel <= len_ref[base] - DRAFT, s[:rows], NEG_BIG),
            jnp.where(rel <= len_ref[base + 1] - DRAFT, s[rows:], NEG_BIG)], 0)
        peak = jnp.max(s, axis=1, keepdims=True)
        p = jnp.exp2((s - peak) * scale)
        mass = jnp.sum(p, axis=1, keepdims=True)
        p_buf[n] = p.astype(jnp.bfloat16)
        i_buf[n] = jnp.broadcast_to(1.0 / mass, (2 * rows, head_dim))
        log_mass = jnp.broadcast_to(peak * scale + jnp.log2(mass), (2 * rows, head_dim))
        for m in range(2):
            slab_l[pl.ds(j + m, rows, stride=PITCH), :] = log_mass[m * rows:(m + 1) * rows]

    def mix(g, n):
        slot, j = g % VALUES, 2 * n
        slab_o = part_o.at[g % RING]
        v2 = jnp.concatenate([vbuf[slot, j], vbuf[slot, j + 1]], 1)
        o2 = jnp.dot(p_buf[n], v2, preferred_element_type=jnp.float32)
        inv = i_buf[n]
        for m in range(2):
            o = o2[m * rows:(m + 1) * rows, m * head_dim:(m + 1) * head_dim] * inv[m * rows:(m + 1) * rows]
            slab_o[pl.ds(j + m, rows, stride=PITCH), :] = o

    pairs = range(GROUP // 2)

    def to_lanes(values):
        total = jnp.zeros((GROUP, head_dim), jnp.float32)
        for i, value in enumerate(values):
            total = jnp.where(lane == seq + i * GROUP, value, total)
        line = jnp.sum(total, axis=0, keepdims=True)
        high = line.astype(jnp.bfloat16).astype(jnp.float32)
        mid = (line - high).astype(jnp.bfloat16).astype(jnp.float32)
        low = line - high - mid
        part = seq[:8]
        return jnp.where(part == 0, high, jnp.where(part == 1, mid, jnp.where(part == 2, low, 0.0))).astype(jnp.bfloat16)

    def put(ref, values, logs):
        for i, value in enumerate(values):
            ref[i * GROUP:(i + 1) * GROUP, :] = value.astype(jnp.bfloat16)
        ref[data:data + 8, :] = to_lanes(logs)

    def take(ref):
        line = jnp.sum(ref[data:data + 8, :].astype(jnp.float32), axis=0, keepdims=True)
        return [(ref[i * GROUP:(i + 1) * GROUP, :].astype(jnp.float32),
                 jnp.sum(jnp.where(lane == seq + i * GROUP, line, 0.0), axis=1, keepdims=True)) for i in range(own)]

    def joined(mine, log_mine, theirs, log_theirs):
        top = jnp.maximum(log_mine, log_theirs)
        w_mine, w_theirs = jnp.exp2(log_mine - top), jnp.exp2(log_theirs - top)
        total = w_mine + w_theirs
        return (w_mine * mine + w_theirs * theirs) / total, top + jnp.log2(total)

    def pair_copy(c):
        return pltpu.make_async_remote_copy(
            src_ref=pair_so.at[c], dst_ref=pair_ro.at[c], send_sem=sent_sem.at[0], recv_sem=pair_sem.at[c],
            device_id={"dup": partner}, device_id_type=MESH)

    def chip_start(c):
        for n, peer in ((2, across), (0, behind), (1, ahead)):
            pltpu.make_async_remote_copy(
                src_ref=chip_so.at[c, n], dst_ref=chip_ro.at[c, n], send_sem=sent_sem.at[1], recv_sem=chip_sem.at[c],
                device_id={"dup": peer}, device_id_type=MESH).start()

    def chip_arrive(c):
        pltpu.make_async_remote_copy(
            src_ref=chip_so.at[c], dst_ref=chip_ro.at[c], send_sem=sent_sem.at[1], recv_sem=chip_sem.at[c],
            device_id={"dup": partner}, device_id_type=MESH).wait_recv()

    def slab(ref, g, row):
        return ref.at[g % RING][pl.ds(row * PITCH, GROUP), :]

    def place(g):
        return (g + steps + SPARE) % (steps + SPARE)

    def give(g):
        c, r = place(g), g + KEEP
        for s in range(4):
            at = [half + s * own + i for i in range(own)]
            put(pair_so.at[c, s], [slab(part_o, r, n) for n in at], [slab(part_l, r, n) for n in at])

    def merge(g):
        c, r = place(g), g + KEEP
        for s in (3, 1, 2, 0):
            both = [joined(slab(part_o, r, s * own + i), slab(part_l, r, s * own + i), *theirs)
                    for i, theirs in enumerate(take(pair_ro.at[c, s]))]
            if s:
                put(chip_so.at[c, s - 1], [o for o, _ in both], [log for _, log in both])
            else:
                for i, (o, log) in enumerate(both):
                    keep_o[r % KEEP, i] = o
                    keep_l[r % KEEP, i] = log

    def final(g):
        c, r = place(g), g + KEEP
        to = pl.ds(pl.multiple_of(((g + steps) % steps) * GROUP, GROUP), GROUP)
        others = [take(chip_ro.at[c, n]) for n in range(3)]
        for i in range(own):
            logs = [keep_l[r % KEEP, i]] + [other[i][1] for other in others]
            top = functools.reduce(jnp.maximum, logs)
            weights = [jnp.exp2(log - top) for log in logs]
            total = functools.reduce(jnp.add, weights)
            merged = weights[0] * keep_o[r % KEEP, i]
            for weight, other in zip(weights[1:], others):
                merged = merged + weight * other[i][0]
            o_ref[i, to, :] = (merged / total).astype(jnp.bfloat16)

    q_arrive(0)
    key_copy(0).wait()
    widen(0)
    for n in pairs:
        score(0, n)
    key_copy(KEYS).start()
    q_pass_far(2)
    key_copy(1).wait()
    q_arrive(1)
    widen(1)
    for n in pairs:
        soften(0, n)
        score(1, n)
    key_copy(KEYS + 1).start()
    q_pass_near(4)

    def step(t, carry, full):
        c = t // ASK + 1

        @pl.when(t % ASK == 0)
        def _():
            if not full:
                @pl.when(c + 5 < asks)
                def _():
                    q_own(c + 5)

            @pl.when(c + 3 < asks)
            def _():
                q_pass_near(c + 3)

            @pl.when(c + 1 < asks)
            def _():
                q_pass_far(c + 1)

            q_arrive(c)

        key_copy(t).wait()
        value_copy(t - 2).wait()
        if full:
            pair_copy(t - MERGE).wait_recv()
        else:
            @pl.when(t >= MERGE)
            def _():
                pair_copy(t - MERGE).wait_recv()

        widen(t)
        for n in pairs:
            mix(t - 2, n)
            soften(t - 1, n)
            score(t, n)
        give(t - GIVE)
        merge(t - MERGE)

        pair_copy(t - GIVE).start()
        if full:
            chip_start(t - MERGE)
        else:
            @pl.when(t >= MERGE)
            def _():
                chip_start(t - MERGE)

            @pl.when(t + KEYS < steps)
            def _():
                key_copy(t + KEYS).start()

            @pl.when(t - 2 + VALUES < steps)
            def _():
                value_copy(t - 2 + VALUES).start()
        return carry

    lax.fori_loop(2, steps // 2, functools.partial(step, full=False), 0)
    lax.fori_loop(steps // 2, steps, functools.partial(step, full=True), 0)

    def late_merge(g, carry):
        pair_copy(g).wait_recv()
        merge(g)
        chip_start(g)
        return carry

    def late_final(g, carry):
        chip_arrive(g)
        final(g)
        return carry

    value_copy(steps - 2).wait()
    pair_copy(steps - MERGE).wait_recv()
    merge(steps - MERGE)
    for n in pairs:
        mix(steps - 2, n)
        soften(steps - 1, n)
    give(steps - 2)
    pair_copy(steps - 2).start()
    chip_start(steps - MERGE)
    value_copy(steps - 1).wait()
    pair_copy(steps - MERGE + 1).wait_recv()
    merge(steps - MERGE + 1)
    for n in pairs:
        mix(steps - 1, n)
    give(steps - 1)
    pair_copy(steps - 1).start()
    chip_start(steps - MERGE + 1)
    lax.fori_loop(steps - MERGE + 2, steps, late_merge, 0)
    lax.fori_loop(0, steps, late_final, 0)

    def drain(src, sem):
        pltpu.make_async_remote_copy(
            src_ref=src, dst_ref=src, send_sem=sem, recv_sem=pair_sem.at[0],
            device_id={"dup": partner}, device_id_type=MESH).wait_send()

    for kind, src in enumerate((q_ref, q_ref, q_ref, q_all.at[1], q_all.at[1:4])):
        drain(src, qs_sem.at[kind])
    drain(pair_so.at[pl.ds(0, steps)], sent_sem.at[0])
    drain(chip_so.at[pl.ds(0, steps)], sent_sem.at[1])


def solution(mesh):
    def group_step(q_local, k_span, v_span, len_local):
        num_batch, own, head_dim = q_local.shape
        span = k_span.shape[1]
        steps = num_batch // GROUP
        asks = steps // ASK + 1
        places = steps + SPARE
        block = own * GROUP + 8
        rows = 8 * own
        vmem = functools.partial(pl.BlockSpec, memory_space=pltpu.VMEM)
        hbm = functools.partial(pl.BlockSpec, memory_space=pl.ANY)
        bf16, f32 = jnp.bfloat16, jnp.float32
        dma = pltpu.SemaphoreType.DMA
        out = pl.pallas_call(
            attend,
            out_shape=jax.ShapeDtypeStruct((own, num_batch, head_dim), bf16),
            in_specs=[vmem(), pl.BlockSpec(memory_space=pltpu.SMEM), hbm(), hbm()],
            out_specs=vmem(),
            scratch_shapes=[
                pltpu.VMEM((KEYS, GROUP, span, head_dim), bf16),
                pltpu.VMEM((VALUES, GROUP, span, head_dim), bf16),
                pltpu.VMEM((8, own, num_batch, head_dim), bf16),
                pltpu.VMEM((rows * PITCH, head_dim), f32),
                pltpu.VMEM((rows, span), jnp.int32),
                pltpu.VMEM((GROUP // 2, 2 * rows, span), f32),
                pltpu.VMEM((GROUP // 2, 2 * rows, span), bf16),
                pltpu.VMEM((GROUP // 2, 2 * rows, head_dim), f32),
                pltpu.VMEM((RING, rows * PITCH, head_dim), f32),
                pltpu.VMEM((RING, rows * PITCH, head_dim), f32),
                pltpu.VMEM((places, 4, block, head_dim), bf16),
                pltpu.VMEM((places, 4, block, head_dim), bf16),
                pltpu.VMEM((places, 3, block, head_dim), bf16),
                pltpu.VMEM((places, 3, block, head_dim), bf16),
                pltpu.VMEM((KEEP, own, GROUP, head_dim), f32),
                pltpu.VMEM((KEEP, own, GROUP, head_dim), f32),
                dma((KEYS,)), dma((VALUES,)),
                dma((5,)), dma((5, asks)),
                dma((2,)), dma((steps,)), dma((steps,)),
            ],
            compiler_params=pltpu.CompilerParams(
                collective_id=0, has_side_effects=True, vmem_limit_bytes=60 * 1024 * 1024),
            cost_estimate=pl.CostEstimate(
                flops=4 * num_batch * rows * span * head_dim,
                bytes_accessed=4 * num_batch * span * head_dim,
                transcendentals=num_batch * rows * span),
        )(q_local.transpose(1, 0, 2), len_local, k_span, v_span)
        return out.transpose(1, 0, 2)

    return jax.shard_map(
        group_step, mesh=mesh,
        in_specs=(P("kv", "dup", None), P("kv", "dup", None), P("kv", "dup", None), P("kv")),
        out_specs=P("kv", "dup", None), check_vma=False)
```

```python
import functools

import jax
import jax.numpy as jnp
from jax import lax
from jax.experimental import pallas as pl
from jax.experimental.pallas import tpu as pltpu
from jax.sharding import PartitionSpec as P

DRAFT = 4
NEG_BIG = -3e38
LOG2E = 1.4426950408889634
MESH = pl.DeviceIdType.MESH

GROUP = 16
KEYS = 10
VALUES = 11
PITCH = GROUP + 4
RING = 8
KEEP = 16
ASK = 2
GIVE, MERGE = 2, 4
SPARE = 4


def attend(q_ref, len_ref, k_hbm, v_hbm, o_ref,
           kbuf, vbuf, q_all, q_wide, pos_rel, s_buf, p_buf, i_buf, part_o, part_l,
           pair_so, pair_ro, chip_so, chip_ro, keep_o, keep_l,
           k_sem, v_sem, qs_sem, qr_sem, sent_sem, pair_sem, chip_sem):
    own, num_batch, head_dim = q_ref.shape
    span = k_hbm.shape[1]
    rows = 8 * own
    half = 4 * own
    data = own * GROUP
    steps = num_batch // GROUP
    asks = steps // ASK + 1
    scale = (head_dim ** -0.5) * LOG2E

    me = lax.axis_index("dup")
    chip = me // 2
    core = me % 2
    turn = (1 - 2 * core) * (1 - 2 * (chip % 2))
    partner = chip * 2 + (1 - core)
    ahead = ((chip + turn + 4) % 4) * 2 + core
    behind = ((chip - turn + 4) % 4) * 2 + core
    across = ((chip + 2) % 4) * 2 + core

    def key_copy(g):
        return pltpu.make_async_copy(k_hbm.at[pl.ds(g * GROUP, GROUP)], kbuf.at[g % KEYS], k_sem.at[g % KEYS])

    def value_copy(g):
        return pltpu.make_async_copy(v_hbm.at[pl.ds(g * GROUP, GROUP)], vbuf.at[g % VALUES], v_sem.at[g % VALUES])

    key_copy(0).start()
    key_copy(1).start()

    def start_cache(g, carry):
        key_copy(g + 2).start()
        value_copy(g).start()
        return carry

    lax.fori_loop(0, KEYS - 2, start_cache, 0)
    for g in range(KEYS - 2, VALUES):
        value_copy(g).start()

    barrier = pltpu.get_barrier_semaphore()
    for peer in (partner, ahead, behind, across):
        pl.semaphore_signal(barrier, inc=1, device_id={"dup": peer}, device_id_type=MESH)

    def q_copy(kind, c, direct=False):
        if isinstance(c, int) and c < 2:
            part = pl.ds(c * GROUP, GROUP)
        else:
            part = pl.ds(pl.multiple_of((c - 1) * ASK * GROUP, ASK * GROUP), ASK * GROUP)
        src, dst, peer = (
            (q_ref.at[:, part], q_all.at[1, :, part], behind),
            (q_ref.at[:, part], q_all.at[2, :, part], ahead),
            (q_ref.at[:, part], q_all.at[4, :, part], partner),
            (q_all.at[1, :, part], q_all.at[3, :, part], ahead),
            (q_all.at[1:4, :, part], q_all.at[5:8, :, part], partner),
        )[kind]
        if direct:
            src, peer = q_ref.at[:, part], across
        return pltpu.make_async_remote_copy(
            src_ref=src, dst_ref=dst, send_sem=qs_sem.at[kind], recv_sem=qr_sem.at[kind, c],
            device_id={"dup": peer}, device_id_type=MESH)

    def q_own(c):
        q_copy(0, c).start()
        q_copy(2, c).start()

    def q_pass_near(c):
        q_copy(0, c).wait_recv()
        q_copy(3, c).start()
        q_copy(1, c).start()

    def q_pass_far(c):
        q_copy(1, c).wait_recv()
        q_copy(3, c).wait_recv()
        q_copy(4, c).start()

    span_start = me * span
    chip_disp = (0, 4 - turn, 4 + turn, 2)
    pair_disp = (0, 4 + turn, 4 - turn, 2)
    row_id = lax.broadcasted_iota(jnp.int32, (rows, span), 0)
    token = jnp.zeros((rows, span), jnp.int32)
    for h in range(2):
        for s in range(4):
            disp = (chip_disp, pair_disp)[h][s]
            device = ((chip + disp) % 4) * 2 + (core if h == 0 else 1 - core)
            for i in range(own):
                token = jnp.where(row_id == h * half + s * own + i, (own * device + i) % DRAFT, token)
    pos_rel[...] = lax.broadcasted_iota(jnp.int32, (rows, span), 1) + span_start - token

    pl.semaphore_wait(barrier, 4)
    for c in range(2):
        q_copy(3, c, direct=True).start()
        q_own(c)
        q_copy(1, c).start()
    for c in range(2, 7):
        q_own(c)
    q_pass_near(2)
    q_copy(0, 0).wait_recv()
    q_pass_far(0)
    q_pass_near(3)
    q_copy(0, 1).wait_recv()
    q_pass_far(1)
    q_pass_near(4)

    def q_arrive(c):
        for kind in (2, 4):
            q_copy(kind, c).wait_recv()

    lane = lax.broadcasted_iota(jnp.int32, (GROUP, head_dim), 1)
    seq = lax.broadcasted_iota(jnp.int32, (GROUP, head_dim), 0)

    def widen(g):
        part = pl.ds(pl.multiple_of(g * GROUP, GROUP), GROUP)
        for s in range(8):
            for i in range(own):
                block = q_ref[i, part, :] if s == 0 else q_all[s, i, part, :]
                q_wide[pl.ds((s * own + i) * PITCH, GROUP), :] = block.astype(jnp.float32)

    def score(g, n):
        slot, j = g % KEYS, 2 * n
        zeros = jnp.zeros((rows, head_dim), jnp.float32)
        q0 = q_wide[pl.ds(j, rows, stride=PITCH), :]
        q1 = q_wide[pl.ds(j + 1, rows, stride=PITCH), :]
        q2 = jnp.concatenate([jnp.concatenate([q0, zeros], 1), jnp.concatenate([zeros, q1], 1)], 0).astype(jnp.bfloat16)
        k2 = jnp.concatenate([kbuf[slot, j], kbuf[slot, j + 1]], 1)
        s_buf[n] = lax.dot_general(q2, k2, (((1,), (1,)), ((), ())), preferred_element_type=jnp.float32)

    def soften(g, n):
        slab_l = part_l.at[g % RING]
        j = 2 * n
        s = s_buf[n]
        rel = pos_rel[...]
        base = g * GROUP + j
        s = jnp.concatenate([
            jnp.where(rel <= len_ref[base] - DRAFT, s[:rows], NEG_BIG),
            jnp.where(rel <= len_ref[base + 1] - DRAFT, s[rows:], NEG_BIG)], 0)
        peak = jnp.max(s, axis=1, keepdims=True)
        p = jnp.exp2((s - peak) * scale)
        mass = jnp.sum(p, axis=1, keepdims=True)
        p_buf[n] = p.astype(jnp.bfloat16)
        i_buf[n] = jnp.broadcast_to(1.0 / mass, (2 * rows, head_dim))
        log_mass = jnp.broadcast_to(peak * scale + jnp.log2(mass), (2 * rows, head_dim))
        for m in range(2):
            slab_l[pl.ds(j + m, rows, stride=PITCH), :] = log_mass[m * rows:(m + 1) * rows]

    def mix(g, n):
        slot, j = g % VALUES, 2 * n
        slab_o = part_o.at[g % RING]
        v2 = jnp.concatenate([vbuf[slot, j], vbuf[slot, j + 1]], 1)
        o2 = jnp.dot(p_buf[n], v2, preferred_element_type=jnp.float32)
        inv = i_buf[n]
        for m in range(2):
            o = o2[m * rows:(m + 1) * rows, m * head_dim:(m + 1) * head_dim] * inv[m * rows:(m + 1) * rows]
            slab_o[pl.ds(j + m, rows, stride=PITCH), :] = o

    pairs = range(GROUP // 2)

    def to_lanes(values):
        total = jnp.zeros((GROUP, head_dim), jnp.float32)
        for i, value in enumerate(values):
            total = jnp.where(lane == seq + i * GROUP, value, total)
        line = jnp.sum(total, axis=0, keepdims=True)
        high = line.astype(jnp.bfloat16).astype(jnp.float32)
        mid = (line - high).astype(jnp.bfloat16).astype(jnp.float32)
        low = line - high - mid
        part = seq[:8]
        return jnp.where(part == 0, high, jnp.where(part == 1, mid, jnp.where(part == 2, low, 0.0))).astype(jnp.bfloat16)

    def put(ref, values, logs):
        for i, value in enumerate(values):
            ref[i * GROUP:(i + 1) * GROUP, :] = value.astype(jnp.bfloat16)
        ref[data:data + 8, :] = to_lanes(logs)

    def take(ref):
        line = jnp.sum(ref[data:data + 8, :].astype(jnp.float32), axis=0, keepdims=True)
        return [(ref[i * GROUP:(i + 1) * GROUP, :].astype(jnp.float32),
                 jnp.sum(jnp.where(lane == seq + i * GROUP, line, 0.0), axis=1, keepdims=True)) for i in range(own)]

    def joined(mine, log_mine, theirs, log_theirs):
        top = jnp.maximum(log_mine, log_theirs)
        w_mine, w_theirs = jnp.exp2(log_mine - top), jnp.exp2(log_theirs - top)
        total = w_mine + w_theirs
        return (w_mine * mine + w_theirs * theirs) / total, top + jnp.log2(total)

    def pair_copy(c):
        return pltpu.make_async_remote_copy(
            src_ref=pair_so.at[c], dst_ref=pair_ro.at[c], send_sem=sent_sem.at[0], recv_sem=pair_sem.at[c],
            device_id={"dup": partner}, device_id_type=MESH)

    def chip_start(c):
        for n, peer in ((2, across), (0, behind), (1, ahead)):
            pltpu.make_async_remote_copy(
                src_ref=chip_so.at[c, n], dst_ref=chip_ro.at[c, n], send_sem=sent_sem.at[1], recv_sem=chip_sem.at[c],
                device_id={"dup": peer}, device_id_type=MESH).start()

    def chip_arrive(c):
        pltpu.make_async_remote_copy(
            src_ref=chip_so.at[c], dst_ref=chip_ro.at[c], send_sem=sent_sem.at[1], recv_sem=chip_sem.at[c],
            device_id={"dup": partner}, device_id_type=MESH).wait_recv()

    def slab(ref, g, row):
        return ref.at[g % RING][pl.ds(row * PITCH, GROUP), :]

    def place(g):
        return (g + steps + SPARE) % (steps + SPARE)

    def give(g):
        c, r = place(g), g + KEEP
        for s in range(4):
            at = [half + s * own + i for i in range(own)]
            put(pair_so.at[c, s], [slab(part_o, r, n) for n in at], [slab(part_l, r, n) for n in at])

    def merge(g):
        c, r = place(g), g + KEEP
        for s in (3, 1, 2, 0):
            both = [joined(slab(part_o, r, s * own + i), slab(part_l, r, s * own + i), *theirs)
                    for i, theirs in enumerate(take(pair_ro.at[c, s]))]
            if s:
                put(chip_so.at[c, s - 1], [o for o, _ in both], [log for _, log in both])
            else:
                for i, (o, log) in enumerate(both):
                    keep_o[r % KEEP, i] = o
                    keep_l[r % KEEP, i] = log

    def final(g):
        c, r = place(g), g + KEEP
        to = pl.ds(pl.multiple_of(((g + steps) % steps) * GROUP, GROUP), GROUP)
        others = [take(chip_ro.at[c, n]) for n in range(3)]
        for i in range(own):
            logs = [keep_l[r % KEEP, i]] + [other[i][1] for other in others]
            top = functools.reduce(jnp.maximum, logs)
            weights = [jnp.exp2(log - top) for log in logs]
            total = functools.reduce(jnp.add, weights)
            merged = weights[0] * keep_o[r % KEEP, i]
            for weight, other in zip(weights[1:], others):
                merged = merged + weight * other[i][0]
            o_ref[i, to, :] = (merged / total).astype(jnp.bfloat16)

    q_arrive(0)
    key_copy(0).wait()
    widen(0)
    for n in pairs:
        score(0, n)
    key_copy(KEYS).start()
    q_pass_far(2)
    key_copy(1).wait()
    q_arrive(1)
    widen(1)
    for n in pairs:
        soften(0, n)
        score(1, n)
    key_copy(KEYS + 1).start()
    def step(t, carry, full):
        c = t // ASK + 1

        @pl.when(t % ASK == 0)
        def _():
            if not full:
                @pl.when(c + 5 < asks)
                def _():
                    q_own(c + 5)

            @pl.when(c + 3 < asks)
            def _():
                q_pass_near(c + 3)

            @pl.when(c + 1 < asks)
            def _():
                q_pass_far(c + 1)

            q_arrive(c)

        key_copy(t).wait()
        value_copy(t - 2).wait()
        if full:
            pair_copy(t - MERGE).wait_recv()
        else:
            @pl.when(t >= MERGE)
            def _():
                pair_copy(t - MERGE).wait_recv()

        widen(t)
        for n in pairs:
            mix(t - 2, n)
            soften(t - 1, n)
            score(t, n)
        give(t - GIVE)
        merge(t - MERGE)

        pair_copy(t - GIVE).start()
        if full:
            chip_start(t - MERGE)
        else:
            @pl.when(t >= MERGE)
            def _():
                chip_start(t - MERGE)

            @pl.when(t + KEYS < steps)
            def _():
                key_copy(t + KEYS).start()

            @pl.when(t - 2 + VALUES < steps)
            def _():
                value_copy(t - 2 + VALUES).start()
        return carry

    lax.fori_loop(2, steps // 2, functools.partial(step, full=False), 0)
    lax.fori_loop(steps // 2, steps, functools.partial(step, full=True), 0)

    def late_merge(g, carry):
        pair_copy(g).wait_recv()
        merge(g)
        chip_start(g)
        return carry

    def late_final(g, carry):
        chip_arrive(g)
        final(g)
        return carry

    value_copy(steps - 2).wait()
    pair_copy(steps - 4).wait_recv()
    merge(steps - 4)
    for n in pairs:
        mix(steps - 2, n)
        soften(steps - 1, n)
    give(steps - 2)
    pair_copy(steps - 2).start()
    chip_start(steps - 4)
    value_copy(steps - 1).wait()
    for n in pairs:
        mix(steps - 1, n)
    give(steps - 1)
    pair_copy(steps - 1).start()
    lax.fori_loop(steps - MERGE + 1, steps, late_merge, 0)
    lax.fori_loop(0, steps, late_final, 0)

    def drain(src, sem):
        pltpu.make_async_remote_copy(
            src_ref=src, dst_ref=src, send_sem=sem, recv_sem=pair_sem.at[0],
            device_id={"dup": partner}, device_id_type=MESH).wait_send()

    for kind, src in enumerate((q_ref, q_ref, q_ref, q_all.at[1], q_all.at[1:4])):
        drain(src, qs_sem.at[kind])
    drain(pair_so.at[pl.ds(0, steps)], sent_sem.at[0])
    drain(chip_so.at[pl.ds(0, steps)], sent_sem.at[1])


def solution(mesh):
    def group_step(q_local, k_span, v_span, len_local):
        num_batch, own, head_dim = q_local.shape
        span = k_span.shape[1]
        steps = num_batch // GROUP
        asks = steps // ASK + 1
        places = steps + SPARE
        block = own * GROUP + 8
        rows = 8 * own
        vmem = functools.partial(pl.BlockSpec, memory_space=pltpu.VMEM)
        hbm = functools.partial(pl.BlockSpec, memory_space=pl.ANY)
        bf16, f32 = jnp.bfloat16, jnp.float32
        dma = pltpu.SemaphoreType.DMA
        out = pl.pallas_call(
            attend,
            out_shape=jax.ShapeDtypeStruct((own, num_batch, head_dim), bf16),
            in_specs=[vmem(), pl.BlockSpec(memory_space=pltpu.SMEM), hbm(), hbm()],
            out_specs=vmem(),
            scratch_shapes=[
                pltpu.VMEM((KEYS, GROUP, span, head_dim), bf16),
                pltpu.VMEM((VALUES, GROUP, span, head_dim), bf16),
                pltpu.VMEM((8, own, num_batch, head_dim), bf16),
                pltpu.VMEM((rows * PITCH, head_dim), f32),
                pltpu.VMEM((rows, span), jnp.int32),
                pltpu.VMEM((GROUP // 2, 2 * rows, span), f32),
                pltpu.VMEM((GROUP // 2, 2 * rows, span), bf16),
                pltpu.VMEM((GROUP // 2, 2 * rows, head_dim), f32),
                pltpu.VMEM((RING, rows * PITCH, head_dim), f32),
                pltpu.VMEM((RING, rows * PITCH, head_dim), f32),
                pltpu.VMEM((places, 4, block, head_dim), bf16),
                pltpu.VMEM((places, 4, block, head_dim), bf16),
                pltpu.VMEM((places, 3, block, head_dim), bf16),
                pltpu.VMEM((places, 3, block, head_dim), bf16),
                pltpu.VMEM((KEEP, own, GROUP, head_dim), f32),
                pltpu.VMEM((KEEP, own, GROUP, head_dim), f32),
                dma((KEYS,)), dma((VALUES,)),
                dma((5,)), dma((5, asks)),
                dma((2,)), dma((steps,)), dma((steps,)),
            ],
            compiler_params=pltpu.CompilerParams(
                collective_id=0, has_side_effects=True, vmem_limit_bytes=60 * 1024 * 1024),
            cost_estimate=pl.CostEstimate(
                flops=4 * num_batch * rows * span * head_dim,
                bytes_accessed=4 * num_batch * span * head_dim,
                transcendentals=num_batch * rows * span),
        )(q_local.transpose(1, 0, 2), len_local, k_span, v_span)
        return out.transpose(1, 0, 2)

    return jax.shard_map(
        group_step, mesh=mesh,
        in_specs=(P("kv", "dup", None), P("kv", "dup", None), P("kv", "dup", None), P("kv")),
        out_specs=P("kv", "dup", None), check_vma=False)
```
